32 devices in a mesh: dp: 1 (over z), cp: 32 (over y, x, core).
Axes of the slice: x: 4, y: 4, z: 1, core: 2. Of those that a mesh axis runs over, the one named last changes fastest.
The devices are a block of a 4x4x8 slice.
Arguments:
- x_a: bfloat16 [512, 4096], P(('dp', 'cp'))
- kc_a: bfloat16 [16384, 8, 128], P(('dp', 'cp'))
- vc_a: bfloat16 [16384, 8, 128], P(('dp', 'cp'))
- x_b: bfloat16 [8192, 4096], P(('dp', 'cp'))
- kc_b: bfloat16 [4096, 8, 128], P(('dp', 'cp'))
- vc_b: bfloat16 [4096, 8, 128], P(('dp', 'cp'))
- w_q: bfloat16 [4096, 4096], replicated
- w_k: bfloat16 [4096, 1024], replicated
- w_v: bfloat16 [4096, 1024], replicated
- w_o: bfloat16 [4096, 4096], replicated
Outputs:
- output 1: bfloat16 [512, 4096], P(('dp', 'cp'))
- output 2: bfloat16 [512, 8, 128], P(('dp', 'cp'))
- output 3: bfloat16 [512, 8, 128], P(('dp', 'cp'))
- output 4: bfloat16 [8192, 4096], P(('dp', 'cp'))
- output 5: bfloat16 [8192, 8, 128], P(('dp', 'cp'))
- output 6: bfloat16 [8192, 8, 128], P(('dp', 'cp'))
All inputs are finite; a program needn't handle non-finite values.
Results may differ from the reference program's by a relative error of at most 0.0175995.
Values are sent between devices in bfloat16 or wider.
A program may use at most 768 MiB of HBM per device.

```python
import math
import jax
import jax.numpy as jnp
from jax import lax

DMODEL = 4096
HEADS = 32
KV_HEADS = 8
HEAD = 128
GROUP = 32
TOKENS_A = 512
CACHE_A = 16384
TOKENS_B = 8192
CACHE_B = 4096
ROPE_BASE = 500000


def rms_rows(raw_draw):
    return raw_draw * lax.rsqrt(jnp.mean(raw_draw * raw_draw, axis=-1, keepdims=True))


def shard_scaled(rng_key, n_rows, low_bound, high_bound):
    key_scale, key_draw = jax.random.split(rng_key)
    scales = jax.random.uniform(key_scale, (GROUP,), jnp.float32, low_bound, high_bound)
    normal_draw = jax.random.normal(key_draw, (n_rows, KV_HEADS, HEAD), jnp.float32)
    return normal_draw * jnp.repeat(scales, n_rows // GROUP)[:, None, None]


def setup_inputs(seed: int = 0, part: int = 0) -> dict:
    root_key = jax.random.key(seed)
    part_keys = jax.random.split(jax.random.fold_in(root_key, part), 6)
    weight_keys = jax.random.split(jax.random.key(seed + 1), 4)
    out_gain = ((CACHE_A + TOKENS_A // 2) * (CACHE_B + TOKENS_B // 2)) ** 0.25
    q_width = HEADS * HEAD
    kv_width = KV_HEADS * HEAD
    in_scale = DMODEL ** -0.5
    return {
        "x_a": rms_rows(jax.random.normal(part_keys[0], (TOKENS_A, DMODEL), jnp.float32)).astype(jnp.bfloat16),
        "kc_a": shard_scaled(part_keys[1], CACHE_A, 0.3, 1.3).astype(jnp.bfloat16),
        "vc_a": shard_scaled(part_keys[2], CACHE_A, 0.5, 1.5).astype(jnp.bfloat16),
        "x_b": rms_rows(jax.random.normal(part_keys[3], (TOKENS_B, DMODEL), jnp.float32)).astype(jnp.bfloat16),
        "kc_b": shard_scaled(part_keys[4], CACHE_B, 0.3, 1.3).astype(jnp.bfloat16),
        "vc_b": shard_scaled(part_keys[5], CACHE_B, 0.5, 1.5).astype(jnp.bfloat16),
        "w_q": (jax.random.normal(weight_keys[0], (DMODEL, q_width), jnp.float32) * in_scale).astype(jnp.bfloat16),
        "w_k": (jax.random.normal(weight_keys[1], (DMODEL, kv_width), jnp.float32) * (1.25 * in_scale)).astype(jnp.bfloat16),
        "w_v": (jax.random.normal(weight_keys[2], (DMODEL, kv_width), jnp.float32) * in_scale).astype(jnp.bfloat16),
        "w_o": (jax.random.normal(weight_keys[3], (q_width, DMODEL), jnp.float32) * (out_gain * q_width ** -0.5)).astype(jnp.bfloat16),
    }


def rope_apply(heads_x, positions):
    half_dim = HEAD // 2
    inv_freq = jnp.power(jnp.float32(ROPE_BASE), jnp.arange(half_dim, dtype=jnp.float32) * (-2.0 / HEAD))
    angles = positions.astype(jnp.float32)[:, None] * inv_freq[None, :]
    cos_ang = jnp.cos(angles)[:, None, :]
    sin_ang = jnp.sin(angles)[:, None, :]
    x_f32 = heads_x.astype(jnp.float32)
    x_first = x_f32[..., :half_dim]
    x_second = x_f32[..., half_dim:]
    rotated = jnp.concatenate([x_first * cos_ang - x_second * sin_ang, x_second * cos_ang + x_first * sin_ang], axis=-1)
    return rotated.astype(jnp.bfloat16)


def request_layer(tok_rows, cache_k, cache_v, w_q, w_k, w_v, w_o):
    tokens = tok_rows.shape[0]
    cache_len = cache_k.shape[0]
    q_per_kv = HEADS // KV_HEADS
    key_count = cache_len + tokens
    positions = cache_len + jnp.arange(tokens)
    q_lin = jnp.dot(tok_rows, w_q, preferred_element_type=jnp.float32).astype(jnp.bfloat16).reshape(tokens, HEADS, HEAD)
    k_lin = jnp.dot(tok_rows, w_k, preferred_element_type=jnp.float32).astype(jnp.bfloat16).reshape(tokens, KV_HEADS, HEAD)
    v_new = jnp.dot(tok_rows, w_v, preferred_element_type=jnp.float32).astype(jnp.bfloat16).reshape(tokens, KV_HEADS, HEAD)
    q_rot = rope_apply(q_lin, positions).reshape(tokens, KV_HEADS, q_per_kv, HEAD)
    k_new = rope_apply(k_lin, positions)
    keys_f32 = jnp.concatenate([cache_k, k_new], axis=0).astype(jnp.float32)
    vals_f32 = jnp.concatenate([cache_v, v_new], axis=0).astype(jnp.float32)
    key_pos = jnp.arange(key_count)
    target = max(1, 2 ** 22 // (HEADS * key_count))
    block_rows = math.gcd(tokens, 1 << (target.bit_length() - 1))
    attn_scale = HEAD ** -0.5

    def query_block(blk_pair):
        q_blk, pos_blk = blk_pair
        scores = jnp.einsum("tkgd,skd->tkgs", q_blk.astype(jnp.float32), keys_f32) * attn_scale
        allowed = (key_pos[None, :] <= pos_blk[:, None])[:, None, None, :]
        scores = jnp.where(allowed, scores, -jnp.inf)
        exp_s = jnp.exp(scores - jnp.max(scores, axis=-1, keepdims=True))
        row_sum = jnp.sum(exp_s, axis=-1)
        pv_sum = jnp.einsum("tkgs,skd->tkgd", exp_s.astype(jnp.bfloat16).astype(jnp.float32), vals_f32)
        return pv_sum / row_sum[..., None]

    out_o = lax.map(query_block, (q_rot.reshape(tokens // block_rows, block_rows, KV_HEADS, q_per_kv, HEAD), positions.reshape(tokens // block_rows, block_rows)))
    attn_out = out_o.reshape(tokens, HEADS * HEAD).astype(jnp.bfloat16)
    y_out = jnp.dot(attn_out, w_o, preferred_element_type=jnp.float32).astype(jnp.bfloat16)
    return y_out, k_new, v_new


def reference(x_a, kc_a, vc_a, x_b, kc_b, vc_b, w_q, w_k, w_v, w_o):
    y_a, knew_a, vnew_a = request_layer(x_a, kc_a, vc_a, w_q, w_k, w_v, w_o)
    y_b, knew_b, vnew_b = request_layer(x_b, kc_b, vc_b, w_q, w_k, w_v, w_o)
    return (y_a, knew_a, vnew_a, y_b, knew_b, vnew_b)
```

```python
import functools

import jax
import jax.numpy as jnp
from jax import lax
from jax.experimental import pallas as pl
from jax.experimental.pallas import tpu as pltpu
from jax.sharding import PartitionSpec as P

ROPE_BASE = 500000
LOG2E = 1.4426950408889634
NEG = float(jnp.finfo(jnp.float32).min)
MESH = pl.DeviceIdType.MESH
CORES = 2
VMEM_LIMIT = 62 * 1024 * 1024


def rope_tables(positions, head_dim):
    half_dim = head_dim // 2
    inv_freq = jnp.power(jnp.float32(ROPE_BASE), jnp.arange(half_dim, dtype=jnp.float32) * (-2.0 / head_dim))
    angles = positions.astype(jnp.float32)[:, None] * inv_freq[None, :]
    return jnp.cos(angles), jnp.sin(angles)


def rotary(lin, cos_ang, sin_ang, head_dim):
    n_tok = lin.shape[0]
    half_dim = head_dim // 2
    x = lin.reshape(n_tok, -1, head_dim).astype(jnp.float32)
    a, b = x[..., :half_dim], x[..., half_dim:]
    c, s = cos_ang[:, None, :], sin_ang[:, None, :]
    out = jnp.concatenate([a * c - b * s, b * c + a * s], axis=-1)
    return out.astype(jnp.bfloat16).reshape(n_tok, -1)


def qk(keys, queries):
    return lax.dot_general(keys, queries, (((1,), (1,)), ((), ())), preferred_element_type=jnp.float32)


def soft_step(scale2, s, vt, m, l, acc_ref):
    m_new = jnp.maximum(m, jnp.max(s, axis=0, keepdims=True))
    alpha = jnp.exp2((m - m_new) * scale2)
    e = jnp.exp2((s - m_new) * scale2)
    l_new = l * alpha + jnp.sum(e, axis=0, keepdims=True)
    pv = jnp.dot(vt, e.astype(jnp.bfloat16), preferred_element_type=jnp.float32)
    acc_ref[...] = acc_ref[...] * alpha + pv
    return m_new, l_new


def kernel(dims, qb, kb, vb, kcb, vcb, qa, ka, va, kca, vca, ob, oa,
           qbuf, kc, vc, kn, vn, vtc, vtn, obuf, acc, m_all, l_all, q_s, s0, s1,
           qabuf, kac, vac, kan, van, vtac, vtan, oastage, ststage, oarecv, strecv,
           send_sem, recv_sem):
    ny, nx, kv, grp, dim = dims
    cp = ny * nx * CORES
    tb = qb.shape[0]
    tq = tb // 2
    rows = grp * tq
    width = grp * dim
    cb = kcb.shape[0]
    ta = qa.shape[0]
    ca = kca.shape[0]
    scale2 = dim ** -0.5 * LOG2E

    me = lax.axis_index("cp")
    c = lax.rem(me, CORES)
    x = lax.rem(me // CORES, nx)
    y = me // (CORES * nx)
    hb = y * CORES + c
    ha = x * CORES + c

    def dev(yy, xx, cc):
        return (yy * nx + xx) * CORES + cc

    def peer_y(h):
        return dev(h // CORES, x, lax.rem(h, CORES))

    def peer_x(h):
        return dev(y, h // CORES, lax.rem(h, CORES))

    def put(item, src, dst, target):
        pltpu.make_async_remote_copy(
            src_ref=src, dst_ref=dst, send_sem=send_sem.at[item], recv_sem=recv_sem.at[item],
            device_id={"cp": target}, device_id_type=MESH,
        ).start()

    def local(item, src, dst):
        pltpu.make_async_copy(src, dst, recv_sem.at[item]).start()

    def wait_in(item, ref):
        pltpu.make_async_copy(ref, ref, recv_sem.at[item]).wait()

    def wait_out(item, ref):
        pltpu.make_async_copy(ref, ref, send_sem.at[item]).wait()

    KC, VC, Q, KN, VN, KAC, VAC, KAN, VAN, QA, OB, OA, ST = range(13)
    AG = 13

    barrier = pltpu.get_barrier_semaphore()

    def greet(d, _):
        pl.semaphore_signal(barrier, inc=1, device_id={"cp": d}, device_id_type=MESH)
        return 0

    lax.fori_loop(0, cp, greet, 0)
    pl.semaphore_wait(barrier, cp)

    def head_cols(ref, h, w):
        return ref.at[:, pl.ds(pl.multiple_of(h * w, w), w)]

    def scatter(item, src, w, dst, mine, peer):
        def one(k, _):
            h = lax.rem(mine + k, kv)
            put(item, head_cols(src, h, w), dst, peer(h))
            return 0

        lax.fori_loop(1, kv, one, 0)
        local(item, head_cols(src, mine, w), dst)

    def scatter_qa(k, _):
        d = lax.rem(me + k, cp)
        h = lax.rem(d, CORES * nx)
        put(QA, head_cols(qa, h, width), qabuf.at[pl.ds(pl.multiple_of(me * ta, ta), ta), :], d)
        return 0

    lax.fori_loop(1, cp, scatter_qa, 0)
    local(QA, head_cols(qa, ha, width), qabuf.at[pl.ds(pl.multiple_of(me * ta, ta), ta), :])
    a_rows = pl.ds(pl.multiple_of(ha * ta, ta), ta)
    scatter(KC, kcb, dim, kc.at[y, x, pl.ds(pl.multiple_of(c * cb, cb), cb), :], hb, peer_y)
    scatter(VC, vcb, dim, vc.at[y, x, pl.ds(pl.multiple_of(c * cb, cb), cb), :], hb, peer_y)
    scatter(KAN, ka, dim, kan.at[a_rows, :], ha, peer_x)
    scatter(VAN, va, dim, van.at[a_rows, :], ha, peer_x)
    scatter(KAC, kca, dim, kac.at[ha], ha, peer_x)
    scatter(VAC, vca, dim, vac.at[ha], ha, peer_x)
    scatter(Q, qb, width, qbuf.at[hb], hb, peer_y)
    scatter(KN, kb, dim, kn.at[y, x, pl.ds(pl.multiple_of(c * tb, tb), tb), :], hb, peer_y)
    scatter(VN, vb, dim, vn.at[y, x, pl.ds(pl.multiple_of(c * tb, tb), tb), :], hb, peer_y)

    right = dev(y, lax.rem(x + 1, nx), c)
    left = dev(y, lax.rem(x + nx - 1, nx), c)
    x_left = lax.rem(x + nx - 1, nx)
    x_right = lax.rem(x + 1, nx)
    x_far = lax.rem(x + nx // 2, nx)
    lo, hi = pl.ds(0, ny // 2), pl.ds(ny // 2, ny // 2)

    def ag_sem(i, step, direction):
        return AG + i * 4 + step * 2 + direction

    def ring_first(i, buf):
        put(ag_sem(i, 0, 0), buf.at[:, x], buf.at[:, x], right)
        put(ag_sem(i, 0, 1), buf.at[:, x], buf.at[:, x], left)

    def ring_second(i, buf):
        wait_in(ag_sem(i, 0, 0), buf.at[:, x_left])
        put(ag_sem(i, 1, 0), buf.at[lo, x_left], buf.at[lo, x_left], right)
        wait_in(ag_sem(i, 0, 1), buf.at[:, x_right])
        put(ag_sem(i, 1, 1), buf.at[hi, x_right], buf.at[hi, x_right], left)

    def ring_last(i, buf):
        wait_in(ag_sem(i, 1, 0), buf.at[lo, x_far])
        wait_in(ag_sem(i, 1, 1), buf.at[hi, x_far])

    def ring_drain(i, buf):
        wait_out(ag_sem(i, 0, 0), buf.at[:, x])
        wait_out(ag_sem(i, 0, 1), buf.at[:, x])
        wait_out(ag_sem(i, 1, 0), buf.at[lo, x])
        wait_out(ag_sem(i, 1, 1), buf.at[hi, x])

    wait_in(KC, kc.at[:, x])
    ring_first(0, kc)
    wait_in(VC, vc.at[:, x])
    ring_first(1, vc)

    def load_q(src, t0):
        for half in range(2):
            for g in range(grp):
                q_s[half, pl.ds(g * tq, tq), :] = src[pl.ds(t0 + half * tq, tq), pl.ds(g * dim, dim)]

    def two_tiles(n, k_at, v_at, acc0, acc1, state, masks):
        s0[...] = qk(k_at(0), q_s[0])

        def body(j, carry):
            m0, l0, m1, l1 = carry
            s1[...] = qk(k_at(j), q_s[1])
            m0, l0 = soft_step(scale2, s0[...], v_at(j), m0, l0, acc0)
            s0[...] = qk(k_at(j + 1), q_s[0])
            m1, l1 = soft_step(scale2, s1[...], v_at(j), m1, l1, acc1)
            return m0, l0, m1, l1

        m0, l0, m1, l1 = lax.fori_loop(0, n - 1, body, state)
        s1[...] = qk(k_at(n - 1), q_s[1])
        e0, e1 = s0[...], s1[...]
        if masks is not None:
            e0 = jnp.where(masks[0], e0, NEG)
            e1 = jnp.where(masks[1], e1, NEG)
        m0, l0 = soft_step(scale2, e0, v_at(n - 1), m0, l0, acc0)
        m1, l1 = soft_step(scale2, e1, v_at(n - 1), m1, l1, acc1)
        return m0, l0, m1, l1

    def fresh(acc0, acc1):
        acc0[...] = jnp.zeros_like(acc0)
        acc1[...] = jnp.zeros_like(acc1)
        neg = jnp.full((1, rows), NEG, jnp.float32)
        zero = jnp.zeros((1, rows), jnp.float32)
        return neg, zero, neg, zero

    def token_of_lane(shape):
        return lax.rem(lax.broadcasted_iota(jnp.int32, shape, 1), tq)

    wait_in(QA, qabuf)
    wait_in(KAC, kac)
    wait_in(VAC, vac)
    wait_in(KAN, kan)
    wait_in(VAN, van)

    def turn_a(j, _):
        vtac[j] = vac[j].T
        return 0

    lax.fori_loop(0, kv, turn_a, 0)
    vtan[...] = van[...].T
    new_a = kan.shape[0]

    def unit_a(u, _):
        t0 = pl.multiple_of(u * 2 * tq, 2 * tq)
        load_q(qabuf, t0)
        acc0, acc1 = acc.at[0], acc.at[1]
        state = fresh(acc0, acc1)
        m0, l0, m1, l1 = two_tiles(kv, lambda j: kac[j], lambda j: vtac[j], acc0, acc1, state, None)
        pos_k = y * new_a + lax.broadcasted_iota(jnp.int32, (new_a, rows), 0)
        pos_q = t0 + token_of_lane((new_a, rows))
        out = []
        for half, (m, l, a_ref) in enumerate(((m0, l0, acc0), (m1, l1, acc1))):
            s = jnp.where(pos_k <= pos_q + half * tq, qk(kan[...], q_s[half]), NEG)
            m, l = soft_step(scale2, s, vtan[...], m, l, a_ref)
            out.append((m, l))
        for half, (m, l) in enumerate(out):
            r = pl.ds(pl.multiple_of(t0 + half * tq, tq), tq)
            row = lax.broadcasted_iota(jnp.int32, (dim, tq), 0)
            stat = jnp.zeros((dim, tq), jnp.float32)
            for g in range(grp):
                cols = slice(g * tq, (g + 1) * tq)
                oastage[r, pl.ds(g * dim, dim)] = acc[half, :, pl.ds(g * tq, tq)].T
                stat = jnp.where(row == g, m[:, cols], stat)
                stat = jnp.where(row == grp + g, l[:, cols], stat)
            ststage[r, :] = stat.T
        return 0

    lax.fori_loop(0, cp * ta // (2 * tq), unit_a, 0)

    slot = y * kv + ha

    def give_a(k, _):
        d = lax.rem(me + k, cp)
        r = pl.ds(pl.multiple_of(d * ta, ta), ta)
        put(OA, oastage.at[r, :], oarecv.at[slot], d)
        put(ST, ststage.at[r, :], strecv.at[slot], d)
        return 0

    lax.fori_loop(1, cp, give_a, 0)
    r_me = pl.ds(pl.multiple_of(me * ta, ta), ta)
    local(OA, oastage.at[r_me, :], oarecv.at[slot])
    local(ST, ststage.at[r_me, :], strecv.at[slot])

    ring_second(0, kc)
    ring_second(1, vc)
    wait_in(KN, kn.at[:, x])
    ring_first(2, kn)
    wait_in(VN, vn.at[:, x])
    ring_first(3, vn)
    wait_in(Q, qbuf)
    ring_last(0, kc)
    ring_last(1, vc)

    blocks = vtc.shape[0]
    per_row = blocks // ny
    per_blk = nx // per_row
    blk = per_blk * CORES * cb

    def cached(buf, j):
        return buf[j // per_row, pl.ds(lax.rem(j, per_row) * per_blk, per_blk)].reshape(blk, dim)

    def turn_c(j, _):
        vtc[j] = cached(vc, j).T
        return 0

    lax.fori_loop(0, blocks, turn_c, 0)

    def keep(u, state):
        for half in range(2):
            m_all[2 * u + half, 0:1, :] = state[2 * half]
            l_all[2 * u + half, 0:1, :] = state[2 * half + 1]

    def unit_c(u, _):
        load_q(qbuf.at[u], 0)
        acc0, acc1 = acc.at[2 * u], acc.at[2 * u + 1]
        state = fresh(acc0, acc1)
        keep(u, two_tiles(blocks, lambda j: cached(kc, j), lambda j: vtc[j], acc0, acc1, state, None))
        return 0

    lax.fori_loop(0, kv // 2, unit_c, 0)
    ring_second(2, kn)
    ring_second(3, vn)
    lax.fori_loop(kv // 2, kv, unit_c, 0)
    ring_last(2, kn)
    ring_last(3, vn)

    def turn_n(j, _):
        vtn[j] = vn[j // nx, lax.rem(j, nx)].T
        return 0

    lax.fori_loop(0, ny * nx, turn_n, 0)
    blk_n = CORES * tb

    def unit_n(i, _):
        u = lax.rem(hb + 1 + i, kv)
        yy, cc = u // CORES, lax.rem(u, CORES)
        last = yy * nx + x
        load_q(qbuf.at[u], 0)
        acc0, acc1 = acc.at[2 * u], acc.at[2 * u + 1]
        state = (m_all[2 * u, 0:1, :], l_all[2 * u, 0:1, :], m_all[2 * u + 1, 0:1, :], l_all[2 * u + 1, 0:1, :])
        pos_k = lax.broadcasted_iota(jnp.int32, (blk_n, rows), 0)
        pos_q = cc * tb + token_of_lane((blk_n, rows))
        masks = (pos_k <= pos_q, pos_k <= pos_q + tq)
        m0, l0, m1, l1 = two_tiles(
            last + 1, lambda j: kn[j // nx, lax.rem(j, nx)], lambda j: vtn[j], acc0, acc1, state, masks)
        for half, l in enumerate((l0, l1)):
            inv = 1.0 / l
            for g in range(grp):
                cols = pl.ds(g * tq, tq)
                o = acc[2 * u + half, :, cols] * inv[:, g * tq:(g + 1) * tq]
                obuf[u, pl.ds(half * tq, tq), pl.ds(g * dim, dim)] = o.T.astype(obuf.dtype)

        @pl.when(i < kv - 1)
        def _():
            put(OB, obuf.at[u], head_cols(ob, hb, width), peer_y(u))

        @pl.when(i == kv - 1)
        def _():
            local(OB, obuf.at[u], head_cols(ob, hb, width))

        return 0

    lax.fori_loop(0, kv, unit_n, 0)

    wait_in(OA, oarecv)
    wait_in(ST, strecv)

    def merge_a(h, _):
        for g in range(grp):
            ms = [strecv[i * kv + h, :, g:g + 1] for i in range(ny)]
            ls = [strecv[i * kv + h, :, grp + g:grp + g + 1] for i in range(ny)]
            top = functools.reduce(jnp.maximum, ms)
            num = jnp.zeros((ta, dim), jnp.float32)
            den = jnp.zeros((ta, 1), jnp.float32)
            for i in range(ny):
                w = jnp.exp2((ms[i] - top) * scale2)
                num = num + w * oarecv[i * kv + h, :, pl.ds(g * dim, dim)]
                den = den + w * ls[i]
            oa[:, pl.ds(pl.multiple_of(h * width + g * dim, dim), dim)] = (num / den).astype(oa.dtype)
        return 0

    lax.fori_loop(0, kv, merge_a, 0)

    wait_in(OB, ob)
    most = kv - 1
    wait_out(KC, kcb.at[:, pl.ds(0, most * dim)])
    wait_out(VC, vcb.at[:, pl.ds(0, most * dim)])
    wait_out(KN, kb.at[:, pl.ds(0, most * dim)])
    wait_out(VN, vb.at[:, pl.ds(0, most * dim)])
    wait_out(Q, qb.at[:, pl.ds(0, most * width)])
    wait_out(KAC, kca.at[:, pl.ds(0, most * dim)])
    wait_out(VAC, vca.at[:, pl.ds(0, most * dim)])
    wait_out(KAN, ka.at[:, pl.ds(0, most * dim)])
    wait_out(VAN, va.at[:, pl.ds(0, most * dim)])
    wait_out(QA, qabuf.at[pl.ds(0, (cp - 1) * ta), :])
    wait_out(OB, obuf.at[pl.ds(0, most)])
    wait_out(OA, oarecv.at[pl.ds(0, cp - 1)])
    wait_out(ST, strecv.at[pl.ds(0, cp - 1)])
    ring_drain(0, kc)
    ring_drain(1, vc)
    ring_drain(2, kn)
    ring_drain(3, vn)


def attention(cp, kv, dim, qb, kb, vb, kcb, vcb, qa, ka, va, kca, vca):
    ny, nx = kv // CORES, cp // kv
    assert nx * CORES == kv and ny * nx * CORES == cp
    grp = qb.shape[1] // (kv * dim)
    tb, ta, cb, ca = qb.shape[0], qa.shape[0], kcb.shape[0], kca.shape[0]
    tq = tb // 2
    rows, width = grp * tq, grp * dim
    blk = CORES * tb
    assert blk == ca and (ny * nx * CORES * cb) % (ny * blk) == 0 and (cp * ta) % (2 * tq) == 0
    bf, f32 = jnp.bfloat16, jnp.float32
    vm = pltpu.VMEM
    scratch = [
        vm((kv, tb, width), bf),
        vm((ny, nx, CORES * cb, dim), bf),
        vm((ny, nx, CORES * cb, dim), bf),
        vm((ny, nx, blk, dim), bf),
        vm((ny, nx, blk, dim), bf),
        vm((cp * cb // blk, dim, blk), bf),
        vm((ny * nx, dim, blk), bf),
        vm((kv, tb, width), bf),
        vm((2 * kv, dim, rows), f32),
        vm((2 * kv, 8, rows), f32),
        vm((2 * kv, 8, rows), f32),
        vm((2, rows, dim), bf),
        vm((blk, rows), f32),
        vm((blk, rows), f32),
        vm((cp * ta, width), bf),
        vm((kv, ca, dim), bf),
        vm((kv, ca, dim), bf),
        vm((kv * ta, dim), bf),
        vm((kv * ta, dim), bf),
        vm((kv, dim, ca), bf),
        vm((dim, kv * ta), bf),
        vm((cp * ta, width), f32),
        vm((cp * ta, dim), f32),
        vm((cp, ta, width), f32),
        vm((cp, ta, dim), f32),
        pltpu.SemaphoreType.DMA((29,)),
        pltpu.SemaphoreType.DMA((29,)),
    ]
    any_spec = pl.BlockSpec(memory_space=pl.ANY)
    return pl.pallas_call(
        functools.partial(kernel, (ny, nx, kv, grp, dim)),
        out_shape=(jax.ShapeDtypeStruct(qb.shape, bf), jax.ShapeDtypeStruct(qa.shape, bf)),
        in_specs=[any_spec] * 10,
        out_specs=(any_spec, pl.BlockSpec(memory_space=pltpu.VMEM)),
        scratch_shapes=scratch,
        compiler_params=pltpu.CompilerParams(
            collective_id=0, has_side_effects=True, vmem_limit_bytes=VMEM_LIMIT),
        name="attend",
    )(qb, kb, vb, kcb, vcb, qa, ka, va, kca, vca)


def solution(mesh):
    cp_size = mesh.shape["cp"]

    def local_step(x_a, kc_a, vc_a, x_b, kc_b, vc_b, w_q, w_k, w_v, w_o):
        ta, tb = x_a.shape[0], x_b.shape[0]
        kv, dim = kc_a.shape[1:]
        me = lax.axis_index("cp")
        pos_a = kc_a.shape[0] * cp_size + me * ta + jnp.arange(ta)
        pos_b = kc_b.shape[0] * cp_size + me * tb + jnp.arange(tb)
        cos_ang, sin_ang = rope_tables(jnp.concatenate([pos_b, pos_a]), dim)
        x = jnp.concatenate([x_b, x_a], axis=0)

        def proj(w):
            return jnp.dot(x, w, preferred_element_type=jnp.float32).astype(jnp.bfloat16)

        q = rotary(proj(w_q), cos_ang, sin_ang, dim)
        k = rotary(proj(w_k), cos_ang, sin_ang, dim)
        v = proj(w_v)
        flat = lambda t: t.reshape(t.shape[0], kv * dim)
        o_b, o_a = attention(
            cp_size, kv, dim, q[:tb], k[:tb], v[:tb], flat(kc_b), flat(vc_b),
            q[tb:], k[tb:], v[tb:], flat(kc_a), flat(vc_a))
        o = jnp.concatenate([o_b, o_a], axis=0)
        y = jnp.dot(o, w_o, preferred_element_type=jnp.float32).astype(jnp.bfloat16)
        heads = lambda t: t.reshape(t.shape[0], kv, dim)
        return y[tb:], heads(k[tb:]), heads(v[tb:]), y[:tb], heads(k[:tb]), heads(v[:tb])

    row_spec = P(("dp", "cp"), None)
    kv_spec = P(("dp", "cp"), None, None)
    full_spec = P()
    return jax.shard_map(
        local_step, mesh=mesh,
        in_specs=(row_spec, kv_spec, kv_spec, row_spec, kv_spec, kv_spec, full_spec, full_spec, full_spec, full_spec),
        out_specs=(row_spec, kv_spec, kv_spec, row_spec, kv_spec, kv_spec), check_vma=False)
```

```python
import functools

import jax
import jax.numpy as jnp
from jax import lax
from jax.experimental import pallas as pl
from jax.experimental.pallas import tpu as pltpu
from jax.sharding import PartitionSpec as P

ROPE_BASE = 500000
LOG2E = 1.4426950408889634
NEG = float(jnp.finfo(jnp.float32).min)
MESH = pl.DeviceIdType.MESH
CORES = 2
VMEM_LIMIT = 62 * 1024 * 1024


def rope_tables(positions, head_dim):
    half_dim = head_dim // 2
    inv_freq = jnp.power(jnp.float32(ROPE_BASE), jnp.arange(half_dim, dtype=jnp.float32) * (-2.0 / head_dim))
    angles = positions.astype(jnp.float32)[:, None] * inv_freq[None, :]
    cos_ang, sin_ang = jnp.cos(angles), jnp.sin(angles)
    return jnp.concatenate([cos_ang, cos_ang], axis=1), jnp.concatenate([-sin_ang, sin_ang], axis=1)


def qk(keys, queries):
    return lax.dot_general(keys, queries, (((1,), (1,)), ((), ())), preferred_element_type=jnp.float32)


def fold(s, op):
    return functools.reduce(op, [s[i:i + 8] for i in range(0, s.shape[0], 8)])


def soft_step(scale2, s, vt, m, l, acc_ref):
    m_new = jnp.maximum(m, jnp.max(s, axis=0, keepdims=True))
    alpha = jnp.exp2((m - m_new) * scale2)
    e = jnp.exp2((s - m_new) * scale2)
    l_new = l * alpha + jnp.sum(e, axis=0, keepdims=True)
    pv = jnp.dot(vt, e.astype(jnp.bfloat16), preferred_element_type=jnp.float32)
    acc_ref[...] = acc_ref[...] * alpha + pv
    return m_new, l_new


def kernel(dims, xb, xa, cosf, sinf, wq, wk, wv, kcb, vcb, kca, vca, ob, oa, nkb, nvb, nka, nva,
           xs, wbuf, qsend, kvsend, rkb, rvb, rka, rva, tkb, tvb, tka, tva,
           qbuf, kc, vc, kn, vn, vtc, vtn, obuf, acc, m_all, l_all, q_s, s0, s1, p0, p1,
           qabuf, kac, vac, kan, van, vtac, vtan, oastage, ststage, oarecv, strecv,
           send_sem, recv_sem, load_sem, wsem, out_sem):
    ny, nx, kv, grp, dim = dims
    cp = ny * nx * CORES
    tb, ta = xb.shape[0], xa.shape[0]
    tq = tb // 2
    rows = grp * tq
    width = grp * dim
    pair = CORES * dim
    cb = kcb.shape[0]
    scale2 = dim ** -0.5 * LOG2E
    bf = jnp.bfloat16

    me = lax.axis_index("cp")
    c = lax.rem(me, CORES)
    x = lax.rem(me // CORES, nx)
    y = me // (CORES * nx)
    hb = y * CORES + c
    ha = x * CORES + c

    def dev(yy, xx, cc):
        return (yy * nx + xx) * CORES + cc

    def peer_y(h):
        return dev(h // CORES, x, lax.rem(h, CORES))

    def peer_x(h):
        return dev(y, h // CORES, lax.rem(h, CORES))

    def put(item, src, dst, target):
        pltpu.make_async_remote_copy(
            src_ref=src, dst_ref=dst, send_sem=send_sem.at[item], recv_sem=recv_sem.at[item],
            device_id={"cp": target}, device_id_type=MESH,
        ).start()

    def copy(src, dst, sem):
        pltpu.make_async_copy(src, dst, sem).start()

    def wait(ref, sem):
        pltpu.make_async_copy(ref, ref, sem).wait()

    def give(item, src, dst, target):
        @pl.when(target == me)
        def _():
            copy(src, dst, recv_sem.at[item])

        @pl.when(target != me)
        def _():
            put(item, src, dst, target)

    def wait_in(item, ref):
        wait(ref, recv_sem.at[item])

    def wait_out(item, ref):
        wait(ref, send_sem.at[item])

    KC, VC, Q, KN, VN, KAC, VAC, KAN, VAN, QA, OB, OA, ST = range(13)
    AG = 13

    barrier = pltpu.get_barrier_semaphore()

    def greet(d, _):
        pl.semaphore_signal(barrier, inc=1, device_id={"cp": d}, device_id_type=MESH)
        return 0

    raw = ((kcb, rkb, tkb), (vcb, rvb, tvb), (kca, rka, tka), (vca, rva, tva))
    for i, (src, dst, _) in enumerate(raw):
        copy(src, dst, load_sem.at[i])
    copy(xb, xs.at[pl.ds(0, tb), :], load_sem.at[4])
    copy(xa, xs.at[pl.ds(tb, ta), :], load_sem.at[4])

    q_steps, kv_steps = kv, kv // CORES

    def q_head(i):
        return lax.rem(hb + 1 + i, kv)

    def kv_pair(i):
        return lax.rem(y + 1 + i, ny)

    def load_wq(i, slot):
        copy(wq.at[:, pl.ds(pl.multiple_of(q_head(i) * width, width), width)], wbuf.at[slot], wsem.at[slot])

    def load_wkv(i, slot):
        cols = pl.ds(pl.multiple_of(kv_pair(i) * pair, pair), pair)
        copy(wk.at[:, cols], wbuf.at[slot, :, pl.ds(0, pair)], wsem.at[slot])
        copy(wv.at[:, cols], wbuf.at[slot, :, pl.ds(pair, pair)], wsem.at[slot])

    load_wq(0, 0)
    lax.fori_loop(0, cp, greet, 0)
    for i, (_, dst, turned) in enumerate(raw):
        wait(dst, load_sem.at[i])
        turned[...] = jnp.transpose(dst[...], (1, 0, 2))
    pl.semaphore_wait(barrier, cp)

    def scatter(item, src, dst, mine, peer):
        def one(k, _):
            h = lax.rem(mine + k, kv)
            put(item, src.at[h], dst, peer(h))
            return 0

        lax.fori_loop(1, kv, one, 0)
        copy(src.at[mine], dst, recv_sem.at[item])

    c_rows = pl.ds(pl.multiple_of(c * cb, cb), cb)
    scatter(KC, tkb, kc.at[y, x, c_rows, :], hb, peer_y)
    scatter(VC, tvb, vc.at[y, x, c_rows, :], hb, peer_y)
    scatter(KAC, tka, kac.at[ha], ha, peer_x)
    scatter(VAC, tva, vac.at[ha], ha, peer_x)

    right = dev(y, lax.rem(x + 1, nx), c)
    left = dev(y, lax.rem(x + nx - 1, nx), c)
    x_left = lax.rem(x + nx - 1, nx)
    x_right = lax.rem(x + 1, nx)
    x_far = lax.rem(x + nx // 2, nx)
    lo, hi = pl.ds(0, ny // 2), pl.ds(ny // 2, ny // 2)

    def ag_sem(i, step, direction):
        return AG + i * 4 + step * 2 + direction

    def ring_first(i, buf):
        put(ag_sem(i, 0, 0), buf.at[:, x], buf.at[:, x], right)
        put(ag_sem(i, 0, 1), buf.at[:, x], buf.at[:, x], left)

    def ring_second(i, buf):
        wait_in(ag_sem(i, 0, 0), buf.at[:, x_left])
        put(ag_sem(i, 1, 0), buf.at[lo, x_left], buf.at[lo, x_left], right)
        wait_in(ag_sem(i, 0, 1), buf.at[:, x_right])
        put(ag_sem(i, 1, 1), buf.at[hi, x_right], buf.at[hi, x_right], left)

    def ring_last(i, buf):
        wait_in(ag_sem(i, 1, 0), buf.at[lo, x_far])
        wait_in(ag_sem(i, 1, 1), buf.at[hi, x_far])

    def ring_drain(i, buf):
        wait_out(ag_sem(i, 0, 0), buf.at[:, x])
        wait_out(ag_sem(i, 0, 1), buf.at[:, x])
        wait_out(ag_sem(i, 1, 0), buf.at[lo, x])
        wait_out(ag_sem(i, 1, 1), buf.at[hi, x])

    wait(xs, load_sem.at[4])
    b_rows, a_rows = pl.ds(0, tb), pl.ds(tb, ta)
    my_a = pl.ds(pl.multiple_of(me * ta, ta), ta)

    def rope(t):
        t = t.astype(bf).astype(jnp.float32)
        return (t * cosf[...] + pltpu.roll(t, dim // 2, 1) * sinf[...]).astype(bf)

    def project(slot):
        return jnp.dot(xs[...], wbuf[slot], preferred_element_type=jnp.float32)

    def q_step(i, _):
        slot = lax.rem(i, 2)

        @pl.when(i + 1 < q_steps)
        def _():
            load_wq(i + 1, 1 - slot)

        @pl.when(i + 1 == q_steps)
        def _():
            load_wkv(0, 1 - slot)

        wait(wbuf.at[slot], wsem.at[slot])
        h = q_head(i)
        lin = project(slot)
        for g in range(grp):
            cols = slice(g * dim, (g + 1) * dim)
            qsend[h, :, cols] = rope(lin[:, cols])
        give(Q, qsend.at[h, b_rows], qbuf.at[hb], peer_y(h))
        for yy in range(ny):
            give(QA, qsend.at[h, a_rows], qabuf.at[my_a, :], dev(yy, h // CORES, lax.rem(h, CORES)))
        return 0

    def kv_step(i, _):
        slot = lax.rem(q_steps + i, 2)

        @pl.when(i + 1 < kv_steps)
        def _():
            load_wkv(i + 1, 1 - slot)

        wait(wbuf.at[slot], wsem.at[slot])
        p = kv_pair(i)
        lin = project(slot)
        for g in range(CORES):
            cols = slice(g * dim, (g + 1) * dim)
            kvsend[p, :, cols] = rope(lin[:, cols])
        kvsend[p, :, pair:2 * pair] = lin[:, pair:2 * pair].astype(bf)
        out_cols = pl.ds(pl.multiple_of(p * pair, pair), pair)
        for j, (nb, na) in enumerate(((nkb, nka), (nvb, nva))):
            cols = pl.ds(j * pair, pair)
            copy(kvsend.at[p, b_rows, cols], nb.at[:, out_cols], out_sem.at[2 * j])
            copy(kvsend.at[p, a_rows, cols], na.at[:, out_cols], out_sem.at[2 * j + 1])
        n_rows = pl.ds(pl.multiple_of(c * tb, tb), tb)
        s_rows = pl.ds(pl.multiple_of(ha * ta, ta), ta)
        for g in range(CORES):
            for j, (ib, db, ia, da) in enumerate(((KN, kn, KAN, kan), (VN, vn, VAN, van))):
                cols = pl.ds(j * pair + g * dim, dim)
                give(ib, kvsend.at[p, b_rows, cols], db.at[y, x, n_rows, :], dev(p, x, g))
                give(ia, kvsend.at[p, a_rows, cols], da.at[s_rows, :], dev(y, p, g))
        return 0

    lax.fori_loop(0, q_steps // 2, q_step, 0)
    wait_in(KC, kc.at[:, x])
    ring_first(0, kc)
    wait_in(VC, vc.at[:, x])
    ring_first(1, vc)
    lax.fori_loop(q_steps // 2, q_steps, q_step, 0)
    lax.fori_loop(0, kv_steps, kv_step, 0)

    def load_q(src, t0):
        for half in range(2):
            for g in range(grp):
                q_s[half, pl.ds(g * tq, tq), :] = src[pl.ds(t0 + half * tq, tq), pl.ds(g * dim, dim)]

    s_refs, p_refs = (s0, s1), (p0, p1)
    blk = s0.shape[0]

    def scores(t, keys):
        s = qk(keys, q_s[t])
        s_refs[t][...] = s
        return fold(s, jnp.maximum)

    def expo(t, m, l8, top8):
        m_new = jnp.maximum(m, jnp.max(top8, axis=0, keepdims=True))
        alpha = jnp.exp2((m - m_new) * scale2)
        l8 = l8 * alpha
        for r in range(0, blk, 16):
            e = jnp.exp2((s_refs[t][pl.ds(r, 16), :] - m_new) * scale2)
            p_refs[t][pl.ds(r, 16), :] = e.astype(bf)
            l8 = l8 + fold(e, jnp.add)
        return m_new, l8, alpha

    def values(t, vt, alpha, accs):
        accs[t][...] = accs[t][...] * alpha + jnp.dot(vt, p_refs[t][...], preferred_element_type=jnp.float32)

    def two_tiles(n, k_at, v_at, accs, state, masks):
        m0, l0, m1, l1 = state
        p1[...] = jnp.zeros_like(p1)
        t0 = scores(0, k_at(0))
        t1 = scores(1, k_at(0))

        def body(j, carry):
            m0, l0, m1, l1, t0, t1, alpha1 = carry
            values(1, v_at(lax.max(j - 1, 0)), alpha1, accs)
            m0, l0, alpha0 = expo(0, m0, l0, t0)
            t0 = scores(0, k_at(j + 1))
            values(0, v_at(j), alpha0, accs)
            m1, l1, alpha1 = expo(1, m1, l1, t1)
            t1 = scores(1, k_at(j + 1))
            return m0, l0, m1, l1, t0, t1, alpha1

        m0, l0, m1, l1, t0, t1, alpha1 = lax.fori_loop(
            0, n - 1, body, (m0, l0, m1, l1, t0, t1, jnp.ones((1, rows), jnp.float32)))
        values(1, v_at(lax.max(n - 2, 0)), alpha1, accs)
        if masks is not None:
            tops = []
            for t in range(2):
                s = jnp.where(masks[t], s_refs[t][...], NEG)
                s_refs[t][...] = s
                tops.append(fold(s, jnp.maximum))
            t0, t1 = tops
        m0, l0, alpha0 = expo(0, m0, l0, t0)
        values(0, v_at(n - 1), alpha0, accs)
        m1, l1, alpha1 = expo(1, m1, l1, t1)
        values(1, v_at(n - 1), alpha1, accs)
        return m0, l0, m1, l1

    def fresh(accs):
        for a in accs:
            a[...] = jnp.zeros_like(a)
        neg = jnp.full((1, rows), NEG, jnp.float32)
        zero = jnp.zeros((8, rows), jnp.float32)
        return neg, zero, neg, zero

    def total(l8):
        return jnp.sum(l8, axis=0, keepdims=True)

    def token_of_lane(shape):
        return lax.rem(lax.broadcasted_iota(jnp.int32, shape, 1), tq)

    wait_in(QA, qabuf)
    wait_in(KAC, kac)
    wait_in(VAC, vac)
    wait_in(KAN, kan)
    wait_in(VAN, van)

    def turn_a(j, _):
        vtac[j] = vac[j].T
        return 0

    lax.fori_loop(0, kv, turn_a, 0)
    vtan[...] = van[...].T
    new_a = kan.shape[0]

    def unit_a(u, _):
        t0 = pl.multiple_of(u * 2 * tq, 2 * tq)
        load_q(qabuf, t0)
        accs = (acc.at[0], acc.at[1])
        m0, l0, m1, l1 = two_tiles(kv, lambda j: kac[j], lambda j: vtac[j], accs, fresh(accs), None)
        pos_k = y * new_a + lax.broadcasted_iota(jnp.int32, (new_a, rows), 0)
        pos_q = t0 + token_of_lane((new_a, rows))
        out = []
        for half, (m, l) in enumerate(((m0, total(l0)), (m1, total(l1)))):
            s = jnp.where(pos_k <= pos_q + half * tq, qk(kan[...], q_s[half]), NEG)
            out.append(soft_step(scale2, s, vtan[...], m, l, accs[half]))
        for half, (m, l) in enumerate(out):
            r = pl.ds(pl.multiple_of(t0 + half * tq, tq), tq)
            row = lax.broadcasted_iota(jnp.int32, (dim, tq), 0)
            stat = jnp.zeros((dim, tq), jnp.float32)
            for g in range(grp):
                cols = slice(g * tq, (g + 1) * tq)
                oastage[r, pl.ds(g * dim, dim)] = acc[half, :, pl.ds(g * tq, tq)].T
                stat = jnp.where(row == g, m[:, cols], stat)
                stat = jnp.where(row == grp + g, l[:, cols], stat)
            ststage[r, :] = stat.T
        return 0

    lax.fori_loop(0, cp * ta // (2 * tq), unit_a, 0)

    slot = y * kv + ha

    def give_a(k, _):
        d = lax.rem(me + k, cp)
        r = pl.ds(pl.multiple_of(d * ta, ta), ta)
        put(OA, oastage.at[r, :], oarecv.at[slot], d)
        put(ST, ststage.at[r, :], strecv.at[slot], d)
        return 0

    lax.fori_loop(1, cp, give_a, 0)
    copy(oastage.at[my_a, :], oarecv.at[slot], recv_sem.at[OA])
    copy(ststage.at[my_a, :], strecv.at[slot], recv_sem.at[ST])

    ring_second(0, kc)
    ring_second(1, vc)
    wait_in(KN, kn.at[:, x])
    ring_first(2, kn)
    wait_in(VN, vn.at[:, x])
    ring_first(3, vn)
    wait_in(Q, qbuf)
    ring_last(0, kc)
    ring_last(1, vc)

    blocks = vtc.shape[0]
    per_row = blocks // ny
    per_blk = nx // per_row

    def cached(buf, j):
        return buf[j // per_row, pl.ds(lax.rem(j, per_row) * per_blk, per_blk)].reshape(blk, dim)

    def turn_c(j, _):
        vtc[j] = cached(vc, j).T
        return 0

    lax.fori_loop(0, blocks, turn_c, 0)

    def keep(u, state):
        for half in range(2):
            m_all[2 * u + half, 0:1, :] = state[2 * half]
            l_all[2 * u + half] = state[2 * half + 1]

    def unit_c(u, _):
        load_q(qbuf.at[u], 0)
        accs = (acc.at[2 * u], acc.at[2 * u + 1])
        keep(u, two_tiles(blocks, lambda j: cached(kc, j), lambda j: vtc[j], accs, fresh(accs), None))
        return 0

    lax.fori_loop(0, kv // 2, unit_c, 0)
    ring_second(2, kn)
    ring_second(3, vn)
    lax.fori_loop(kv // 2, kv, unit_c, 0)
    ring_last(2, kn)
    ring_last(3, vn)

    def turn_n(j, _):
        vtn[j] = vn[j // nx, lax.rem(j, nx)].T
        return 0

    lax.fori_loop(0, ny * nx, turn_n, 0)

    def unit_n(i, _):
        u = lax.rem(hb + 1 + i, kv)
        yy, cc = u // CORES, lax.rem(u, CORES)
        load_q(qbuf.at[u], 0)
        accs = (acc.at[2 * u], acc.at[2 * u + 1])
        state = (m_all[2 * u, 0:1, :], l_all[2 * u], m_all[2 * u + 1, 0:1, :], l_all[2 * u + 1])
        pos_k = lax.broadcasted_iota(jnp.int32, (blk, rows), 0)
        pos_q = cc * tb + token_of_lane((blk, rows))
        masks = (pos_k <= pos_q, pos_k <= pos_q + tq)
        m0, l0, m1, l1 = two_tiles(
            yy * nx + x + 1, lambda j: kn[j // nx, lax.rem(j, nx)], lambda j: vtn[j], accs, state, masks)
        for half, l in enumerate((l0, l1)):
            inv = 1.0 / total(l)
            for g in range(grp):
                o = acc[2 * u + half, :, pl.ds(g * tq, tq)] * inv[:, g * tq:(g + 1) * tq]
                obuf[u, pl.ds(half * tq, tq), pl.ds(g * dim, dim)] = o.T.astype(bf)
        give(OB, obuf.at[u], ob.at[:, pl.ds(pl.multiple_of(hb * width, width), width)], peer_y(u))
        return 0

    lax.fori_loop(0, kv, unit_n, 0)

    wait_in(OA, oarecv)
    wait_in(ST, strecv)

    def merge_a(h, _):
        for g in range(grp):
            ms = [strecv[i * kv + h, :, g:g + 1] for i in range(ny)]
            ls = [strecv[i * kv + h, :, grp + g:grp + g + 1] for i in range(ny)]
            top = functools.reduce(jnp.maximum, ms)
            num = jnp.zeros((ta, dim), jnp.float32)
            den = jnp.zeros((ta, 1), jnp.float32)
            for i in range(ny):
                w = jnp.exp2((ms[i] - top) * scale2)
                num = num + w * oarecv[i * kv + h, :, pl.ds(g * dim, dim)]
                den = den + w * ls[i]
            oa[:, pl.ds(pl.multiple_of(h * width + g * dim, dim), dim)] = (num / den).astype(bf)
        return 0

    lax.fori_loop(0, kv, merge_a, 0)

    wait_in(OB, ob)
    for i, ref in enumerate((nkb, nka, nvb, nva)):
        wait(ref, out_sem.at[i])
    most = pl.ds(0, kv - 1)
    for item, ref in ((KC, tkb), (VC, tvb), (KAC, tka), (VAC, tva), (Q, qbuf), (OB, obuf)):
        wait_out(item, ref.at[most])
    for item, ref in ((KN, qbuf), (VN, qbuf)):
        wait_out(item, ref.at[most, :, pl.ds(0, dim)])
    for item, ref in ((KAN, kan), (VAN, van)):
        wait_out(item, ref.at[pl.ds(0, (kv - 1) * ta), :])
    wait_out(QA, qabuf.at[pl.ds(0, (cp - 1) * ta), :])
    wait_out(OA, oarecv.at[pl.ds(0, cp - 1)])
    wait_out(ST, strecv.at[pl.ds(0, cp - 1)])
    ring_drain(0, kc)
    ring_drain(1, vc)
    ring_drain(2, kn)
    ring_drain(3, vn)


def attention(cp, xb, xa, cosf, sinf, wq, wk, wv, kcb, vcb, kca, vca):
    kv, dim = kcb.shape[1:]
    ny, nx = kv // CORES, cp // kv
    assert nx * CORES == kv and ny * nx * CORES == cp and ny == nx
    grp = wq.shape[1] // (kv * dim)
    tb, ta, cb, ca, model = xb.shape[0], xa.shape[0], kcb.shape[0], kca.shape[0], xb.shape[1]
    tq = tb // 2
    rows, width = grp * tq, grp * dim
    blk = CORES * tb
    assert blk == ca and (ny * nx * CORES * cb) % (ny * blk) == 0 and (cp * ta) % (2 * tq) == 0
    assert width == 2 * CORES * dim
    bf, f32 = jnp.bfloat16, jnp.float32
    vm = pltpu.VMEM
    scratch = [
        vm((tb + ta, model), bf),
        vm((2, model, width), bf),
        vm((kv, tb + ta, width), bf),
        vm((ny, tb + ta, width), bf),
        vm(kcb.shape, bf), vm(vcb.shape, bf), vm(kca.shape, bf), vm(vca.shape, bf),
        vm((kv, cb, dim), bf), vm((kv, cb, dim), bf), vm((kv, ca, dim), bf), vm((kv, ca, dim), bf),
        vm((kv, tb, width), bf),
        vm((ny, nx, CORES * cb, dim), bf),
        vm((ny, nx, CORES * cb, dim), bf),
        vm((ny, nx, blk, dim), bf),
        vm((ny, nx, blk, dim), bf),
        vm((cp * cb // blk, dim, blk), bf),
        vm((ny * nx, dim, blk), bf),
        vm((kv, tb, width), bf),
        vm((2 * kv, dim, rows), f32),
        vm((2 * kv, 8, rows), f32),
        vm((2 * kv, 8, rows), f32),
        vm((2, rows, dim), bf),
        vm((blk, rows), f32),
        vm((blk, rows), f32),
        vm((blk, rows), bf),
        vm((blk, rows), bf),
        vm((cp * ta, width), bf),
        vm((kv, ca, dim), bf),
        vm((kv, ca, dim), bf),
        vm((kv * ta, dim), bf),
        vm((kv * ta, dim), bf),
        vm((kv, dim, ca), bf),
        vm((dim, kv * ta), bf),
        vm((cp * ta, width), f32),
        vm((cp * ta, dim), f32),
        vm((cp, ta, width), f32),
        vm((cp, ta, dim), f32),
        pltpu.SemaphoreType.DMA((29,)),
        pltpu.SemaphoreType.DMA((29,)),
        pltpu.SemaphoreType.DMA((5,)),
        pltpu.SemaphoreType.DMA((2,)),
        pltpu.SemaphoreType.DMA((4,)),
    ]
    any_spec = pl.BlockSpec(memory_space=pl.ANY)
    vmem_spec = pl.BlockSpec(memory_space=pltpu.VMEM)
    shape = jax.ShapeDtypeStruct
    return pl.pallas_call(
        functools.partial(kernel, (ny, nx, kv, grp, dim)),
        out_shape=(shape((tb, kv * width), bf), shape((ta, kv * width), bf),
                   shape((tb, kv * dim), bf), shape((tb, kv * dim), bf),
                   shape((ta, kv * dim), bf), shape((ta, kv * dim), bf)),
        in_specs=[any_spec, any_spec, vmem_spec, vmem_spec] + [any_spec] * 7,
        out_specs=(any_spec, vmem_spec) + (any_spec,) * 4,
        scratch_shapes=scratch,
        compiler_params=pltpu.CompilerParams(
            collective_id=0, has_side_effects=True, vmem_limit_bytes=VMEM_LIMIT),
        name="attend",
    )(xb, xa, cosf, sinf, wq, wk, wv, kcb, vcb, kca, vca)


def out_kernel(ob, oa, w, yb, ya, o):
    tb = ob.shape[0]

    @pl.when(pl.program_id(0) == 0)
    def _():
        o[pl.ds(0, tb), :] = ob[...]
        o[pl.ds(tb, oa.shape[0]), :] = oa[...]

    out = jnp.dot(o[...], w[...], preferred_element_type=jnp.float32).astype(yb.dtype)
    yb[...] = out[:tb]
    ya[...] = out[tb:]


def output_projection(ob, oa, w):
    (tb, inner), ta, model = ob.shape, oa.shape[0], w.shape[1]
    cols = min(512, model)
    shape = jax.ShapeDtypeStruct
    return pl.pallas_call(
        out_kernel,
        grid=(model // cols,),
        out_shape=(shape((tb, model), ob.dtype), shape((ta, model), ob.dtype)),
        in_specs=[pl.BlockSpec((tb, inner), lambda i: (0, 0)), pl.BlockSpec((ta, inner), lambda i: (0, 0)),
                  pl.BlockSpec((inner, cols), lambda i: (0, i))],
        out_specs=(pl.BlockSpec((tb, cols), lambda i: (0, i)), pl.BlockSpec((ta, cols), lambda i: (0, i))),
        scratch_shapes=[pltpu.VMEM((tb + ta, inner), ob.dtype)],
        compiler_params=pltpu.CompilerParams(vmem_limit_bytes=VMEM_LIMIT),
        name="project_out",
    )(ob, oa, w)


def solution(mesh):
    cp_size = mesh.shape["cp"]

    def local_step(x_a, kc_a, vc_a, x_b, kc_b, vc_b, w_q, w_k, w_v, w_o):
        ta, tb = x_a.shape[0], x_b.shape[0]
        kv, dim = kc_a.shape[1:]
        me = lax.axis_index("cp")
        pos_a = kc_a.shape[0] * cp_size + me * ta + jnp.arange(ta)
        pos_b = kc_b.shape[0] * cp_size + me * tb + jnp.arange(tb)
        cosf, sinf = rope_tables(jnp.concatenate([pos_b, pos_a]), dim)
        o_b, o_a, k_b, v_b, k_a, v_a = attention(cp_size, x_b, x_a, cosf, sinf, w_q, w_k, w_v, kc_b, vc_b, kc_a, vc_a)
        y_b, y_a = output_projection(o_b, o_a, w_o)
        heads = lambda t: t.reshape(t.shape[0], kv, dim)
        return y_a, heads(k_a), heads(v_a), y_b, heads(k_b), heads(v_b)

    row_spec = P(("dp", "cp"), None)
    kv_spec = P(("dp", "cp"), None, None)
    full_spec = P()
    return jax.shard_map(
        local_step, mesh=mesh,
        in_specs=(row_spec, kv_spec, kv_spec, row_spec, kv_spec, kv_spec, full_spec, full_spec, full_spec, full_spec),
        out_specs=(row_spec, kv_spec, kv_spec, row_spec, kv_spec, kv_spec), check_vma=False)
```

```python
import functools

import jax
import jax.numpy as jnp
from jax import lax
from jax.experimental import pallas as pl
from jax.experimental.pallas import tpu as pltpu
from jax.sharding import PartitionSpec as P

ROPE_BASE = 500000
LOG2E = 1.4426950408889634
NEG = float(jnp.finfo(jnp.float32).min)
MESH = pl.DeviceIdType.MESH
CORES = 2
VMEM_LIMIT = 62 * 1024 * 1024


def rope_tables(positions, head_dim):
    half_dim = head_dim // 2
    inv_freq = jnp.power(jnp.float32(ROPE_BASE), jnp.arange(half_dim, dtype=jnp.float32) * (-2.0 / head_dim))
    angles = positions.astype(jnp.float32)[:, None] * inv_freq[None, :]
    cos_ang, sin_ang = jnp.cos(angles), jnp.sin(angles)
    return jnp.concatenate([cos_ang, cos_ang], axis=1), jnp.concatenate([-sin_ang, sin_ang], axis=1)


def qk(keys, queries):
    return lax.dot_general(keys, queries, (((1,), (1,)), ((), ())), preferred_element_type=jnp.float32)


def fold(s, op):
    return functools.reduce(op, [s[i:i + 8] for i in range(0, s.shape[0], 8)])


def soft_step(scale2, s, vt, m, l, acc_ref):
    m_new = jnp.maximum(m, jnp.max(s, axis=0, keepdims=True))
    alpha = jnp.exp2((m - m_new) * scale2)
    e = jnp.exp2((s - m_new) * scale2)
    l_new = l * alpha + jnp.sum(e, axis=0, keepdims=True)
    pv = jnp.dot(vt, e.astype(jnp.bfloat16), preferred_element_type=jnp.float32)
    acc_ref[...] = acc_ref[...] * alpha + pv
    return m_new, l_new


def kernel(dims, xb, xa, cosf, sinf, wq, wk, wv, kcb, vcb, kca, vca, ob, oa, nkb, nvb, nka, nva,
           xs, wbuf, qsend, kvsend, rkb, rvb, rka, rva, tkb, tvb, tka, tva,
           qbuf, kc, vc, kn, vn, vtc, vtn, obuf, acc, m_all, l_all, q_s, q_all, s0, s1, p0, p1,
           qabuf, kac, vac, kan, van, vtac, vtan, oastage, ststage, oarecv, strecv, odone, accx,
           send_sem, recv_sem, load_sem, wsem, out_sem):
    ny, nx, kv, grp, dim = dims
    cp = ny * nx * CORES
    tb, ta = xb.shape[0], xa.shape[0]
    tq = tb // 2
    rows = grp * tq
    width = grp * dim
    pair = CORES * dim
    cb = kcb.shape[0]
    scale2 = dim ** -0.5 * LOG2E
    bf = jnp.bfloat16

    me = lax.axis_index("cp")
    c = lax.rem(me, CORES)
    x = lax.rem(me // CORES, nx)
    y = me // (CORES * nx)
    hb = y * CORES + c
    ha = x * CORES + c

    def dev(yy, xx, cc):
        return (yy * nx + xx) * CORES + cc

    def peer_y(h):
        return dev(h // CORES, x, lax.rem(h, CORES))

    def peer_x(h):
        return dev(y, h // CORES, lax.rem(h, CORES))

    def put(item, src, dst, target):
        pltpu.make_async_remote_copy(
            src_ref=src, dst_ref=dst, send_sem=send_sem.at[item], recv_sem=recv_sem.at[item],
            device_id={"cp": target}, device_id_type=MESH,
        ).start()

    def copy(src, dst, sem):
        pltpu.make_async_copy(src, dst, sem).start()

    def wait(ref, sem):
        pltpu.make_async_copy(ref, ref, sem).wait()

    def give(item, src, dst, target):
        @pl.when(target == me)
        def _():
            copy(src, dst, recv_sem.at[item])

        @pl.when(target != me)
        def _():
            put(item, src, dst, target)

    def wait_in(item, ref):
        wait(ref, recv_sem.at[item])

    def wait_out(item, ref):
        wait(ref, send_sem.at[item])

    KC, VC, Q, KN, VN, KAC, VAC, KAN, VAN, QA, QY, OB, OA, ST, OX = range(15)
    AG = 15

    barrier = pltpu.get_barrier_semaphore()

    def greet(d, _):
        pl.semaphore_signal(barrier, inc=1, device_id={"cp": d}, device_id_type=MESH)
        return 0

    raw = ((kcb, rkb, tkb), (vcb, rvb, tvb), (kca, rka, tka), (vca, rva, tva))
    for i, (src, dst, _) in enumerate(raw):
        copy(src, dst, load_sem.at[i])
    copy(xb, xs.at[pl.ds(0, tb), :], load_sem.at[4])
    copy(xa, xs.at[pl.ds(tb, ta), :], load_sem.at[4])

    q_steps, kv_steps = kv, kv // CORES

    def q_head(i):
        return lax.rem(hb + 1 + i, kv)

    def kv_pair(i):
        return lax.rem(y + 1 + i, ny)

    def load_wq(i, slot):
        copy(wq.at[:, pl.ds(pl.multiple_of(q_head(i) * width, width), width)], wbuf.at[slot], wsem.at[slot])

    def load_wkv(i, slot):
        cols = pl.ds(pl.multiple_of(kv_pair(i) * pair, pair), pair)
        copy(wk.at[:, cols], wbuf.at[slot, :, pl.ds(0, pair)], wsem.at[slot])
        copy(wv.at[:, cols], wbuf.at[slot, :, pl.ds(pair, pair)], wsem.at[slot])

    load_wq(0, 0)
    lax.fori_loop(0, cp, greet, 0)
    for i, (_, dst, turned) in enumerate(raw):
        wait(dst, load_sem.at[i])
        turned[...] = jnp.transpose(dst[...], (1, 0, 2))
    pl.semaphore_wait(barrier, cp)

    def scatter(item, src, dst, mine, peer):
        def one(k, _):
            h = lax.rem(mine + k, kv)
            put(item, src.at[h], dst, peer(h))
            return 0

        lax.fori_loop(1, kv, one, 0)
        copy(src.at[mine], dst, recv_sem.at[item])

    c_rows = pl.ds(pl.multiple_of(c * cb, cb), cb)
    scatter(KC, tkb, kc.at[y, x, c_rows, :], hb, peer_y)
    scatter(VC, tvb, vc.at[y, x, c_rows, :], hb, peer_y)
    scatter(KAC, tka, kac.at[ha], ha, peer_x)

    right = dev(y, lax.rem(x + 1, nx), c)
    left = dev(y, lax.rem(x + nx - 1, nx), c)
    x_left = lax.rem(x + nx - 1, nx)
    x_right = lax.rem(x + 1, nx)
    x_far = lax.rem(x + nx // 2, nx)
    lo, hi = pl.ds(0, ny // 2), pl.ds(ny // 2, ny // 2)

    def ag_sem(i, step, direction):
        return AG + i * 4 + step * 2 + direction

    def ring_first(i, buf):
        put(ag_sem(i, 0, 0), buf.at[:, x], buf.at[:, x], right)
        put(ag_sem(i, 0, 1), buf.at[:, x], buf.at[:, x], left)

    def ring_second(i, buf):
        wait_in(ag_sem(i, 0, 0), buf.at[:, x_left])
        put(ag_sem(i, 1, 0), buf.at[lo, x_left], buf.at[lo, x_left], right)
        wait_in(ag_sem(i, 0, 1), buf.at[:, x_right])
        put(ag_sem(i, 1, 1), buf.at[hi, x_right], buf.at[hi, x_right], left)

    def ring_last(i, buf):
        wait_in(ag_sem(i, 1, 0), buf.at[lo, x_far])
        wait_in(ag_sem(i, 1, 1), buf.at[hi, x_far])

    def ring_drain(i, buf):
        wait_out(ag_sem(i, 0, 0), buf.at[:, x])
        wait_out(ag_sem(i, 0, 1), buf.at[:, x])
        wait_out(ag_sem(i, 1, 0), buf.at[lo, x])
        wait_out(ag_sem(i, 1, 1), buf.at[hi, x])

    wait(xs, load_sem.at[4])
    b_rows, a_rows = pl.ds(0, tb), pl.ds(tb, ta)
    my_a = pl.ds(pl.multiple_of(me * ta, ta), ta)

    def rope(t):
        t = t.astype(bf).astype(jnp.float32)
        return (t * cosf[...] + pltpu.roll(t, dim // 2, 1) * sinf[...]).astype(bf)

    def project(slot):
        return jnp.dot(xs[...], wbuf[slot], preferred_element_type=jnp.float32)

    def q_step(i, _):
        slot = lax.rem(i, 2)

        @pl.when(i + 1 < q_steps)
        def _():
            load_wq(i + 1, 1 - slot)

        @pl.when(i + 1 == q_steps)
        def _():
            load_wkv(0, 1 - slot)

        wait(wbuf.at[slot], wsem.at[slot])
        h = q_head(i)
        lin = project(slot)
        for g in range(grp):
            cols = slice(g * dim, (g + 1) * dim)
            qsend[h, :, cols] = rope(lin[:, cols])
        give(Q, qsend.at[h, b_rows], qbuf.at[hb], peer_y(h))
        give(QA, qsend.at[h, a_rows], qabuf.at[my_a, :], peer_x(h))
        return 0

    def kv_step(i, _):
        slot = lax.rem(q_steps + i, 2)

        @pl.when(i + 1 < kv_steps)
        def _():
            load_wkv(i + 1, 1 - slot)

        wait(wbuf.at[slot], wsem.at[slot])
        p = kv_pair(i)
        lin = project(slot)
        for g in range(CORES):
            cols = slice(g * dim, (g + 1) * dim)
            kvsend[p, :, cols] = rope(lin[:, cols])
        kvsend[p, :, pair:2 * pair] = lin[:, pair:2 * pair].astype(bf)
        out_cols = pl.ds(pl.multiple_of(p * pair, pair), pair)
        for j, (nb, na) in enumerate(((nkb, nka), (nvb, nva))):
            cols = pl.ds(j * pair, pair)
            copy(kvsend.at[p, b_rows, cols], nb.at[:, out_cols], out_sem.at[2 * j])
            copy(kvsend.at[p, a_rows, cols], na.at[:, out_cols], out_sem.at[2 * j + 1])
        n_rows = pl.ds(pl.multiple_of(c * tb, tb), tb)
        s_rows = pl.ds(pl.multiple_of(ha * ta, ta), ta)
        for g in range(CORES):
            for j, (ib, db, ia, da) in enumerate(((KN, kn, KAN, kan), (VN, vn, VAN, van))):
                cols = pl.ds(j * pair + g * dim, dim)
                give(ib, kvsend.at[p, b_rows, cols], db.at[y, x, n_rows, :], dev(p, x, g))
                give(ia, kvsend.at[p, a_rows, cols], da.at[s_rows, :], dev(y, p, g))
        return 0

    lax.fori_loop(0, q_steps // 2, q_step, 0)
    wait_in(KC, kc.at[:, x])
    ring_first(0, kc)
    wait_in(VC, vc.at[:, x])
    ring_first(1, vc)
    lax.fori_loop(q_steps // 2, q_steps, q_step, 0)
    lax.fori_loop(0, kv_steps, kv_step, 0)
    ring_second(0, kc)
    ring_second(1, vc)
    scatter(VAC, tva, vac.at[ha], ha, peer_x)
    new_a = kan.shape[0]
    row_a = pl.ds(pl.multiple_of(y * new_a, new_a), new_a)
    wait_in(QA, qabuf.at[row_a, :])

    def pass_qa(k, _):
        put(QY, qabuf.at[row_a, :], qabuf.at[row_a, :], dev(lax.rem(y + k, ny), x, c))
        return 0

    lax.fori_loop(1, ny, pass_qa, 0)

    def load_q(src, t0):
        for half in range(2):
            for g in range(grp):
                q_s[half, pl.ds(g * tq, tq), :] = src[pl.ds(t0 + half * tq, tq), pl.ds(g * dim, dim)]

    s_refs, p_refs = (s0, s1), (p0, p1)
    blk = s0.shape[0]

    def scores(t, keys, queries):
        s = qk(keys, queries)
        s_refs[t][...] = s
        return fold(s, jnp.maximum)

    def expo(t, m, l8, top8):
        m_new = jnp.maximum(m, jnp.max(top8, axis=0, keepdims=True))
        alpha = jnp.exp2((m - m_new) * scale2)
        l8 = l8 * alpha
        for r in range(0, blk, 16):
            e = jnp.exp2((s_refs[t][pl.ds(r, 16), :] - m_new) * scale2)
            p_refs[t][pl.ds(r, 16), :] = e.astype(bf)
            l8 = l8 + fold(e, jnp.add)
        return m_new, l8, alpha

    def values(t, vt, alpha, acc_ref):
        acc_ref[...] = acc_ref[...] * alpha + jnp.dot(vt, p_refs[t][...], preferred_element_type=jnp.float32)

    one = jnp.ones((1, rows), jnp.float32)

    def inner(n, k_at, v_at, queries, accs, state, tops):
        def body(j, carry):
            m0, l0, m1, l1, t0, t1, alpha1 = carry
            values(1, v_at(lax.max(j - 1, 0)), alpha1, accs[1])
            m0, l0, alpha0 = expo(0, m0, l0, t0)
            t0 = scores(0, k_at(j + 1), queries(0))
            values(0, v_at(j), alpha0, accs[0])
            m1, l1, alpha1 = expo(1, m1, l1, t1)
            t1 = scores(1, k_at(j + 1), queries(1))
            return m0, l0, m1, l1, t0, t1, alpha1

        p1[...] = jnp.zeros_like(p1)
        out = lax.fori_loop(0, n - 1, body, state + tops + (one,))
        values(1, v_at(lax.max(n - 2, 0)), out[6], accs[1])
        return out[:4], out[4:6]

    def fresh(accs):
        for a in accs:
            a[...] = jnp.zeros_like(a)
        neg = jnp.full((1, rows), NEG, jnp.float32)
        zero = jnp.zeros((8, rows), jnp.float32)
        return neg, zero, neg, zero

    def total(l8):
        return jnp.sum(l8, axis=0, keepdims=True)

    def token_of_lane(shape):
        return lax.rem(lax.broadcasted_iota(jnp.int32, shape, 1), tq)

    wait_in(Q, qbuf)

    def tiles_q(u, _):
        for half in range(2):
            for g in range(grp):
                q_all[2 * u + half, pl.ds(g * tq, tq), :] = qbuf[u, pl.ds(half * tq, tq), pl.ds(g * dim, dim)]
        return 0

    lax.fori_loop(0, kv, tiles_q, 0)
    ring_last(0, kc)
    ring_last(1, vc)

    blocks = vtc.shape[0]
    per_row = blocks // ny
    per_blk = nx // per_row

    def cached(buf, j):
        return buf[j // per_row, pl.ds(lax.rem(j, per_row) * per_blk, per_blk)].reshape(blk, dim)

    def turn_c(j, _):
        vtc[j] = cached(vc, j).T
        return 0

    lax.fori_loop(0, blocks, turn_c, 0)
    acc[...] = jnp.zeros_like(acc)
    p1[...] = jnp.zeros_like(p1)
    steps = kv * blocks

    def step_c(t, carry):
        m0, l0, m1, l1, t0, t1, alpha1 = carry
        u, j = t // blocks, lax.rem(t, blocks)
        before, after = lax.max(t - 1, 0), lax.min(t + 1, steps - 1)
        u_after, k_after = after // blocks, cached(kc, lax.rem(after, blocks))
        values(1, vtc[lax.rem(before, blocks)], alpha1, acc.at[2 * (before // blocks) + 1])
        m0, m1 = jnp.where(j == 0, NEG, m0), jnp.where(j == 0, NEG, m1)
        l0, l1 = jnp.where(j == 0, 0.0, l0), jnp.where(j == 0, 0.0, l1)
        m0, l0, alpha0 = expo(0, m0, l0, t0)
        t0 = scores(0, k_after, q_all[2 * u_after])
        values(0, vtc[j], alpha0, acc.at[2 * u])
        m1, l1, alpha1 = expo(1, m1, l1, t1)
        t1 = scores(1, k_after, q_all[2 * u_after + 1])
        m_all[2 * u, 0:1, :] = m0
        m_all[2 * u + 1, 0:1, :] = m1
        l_all[2 * u] = l0
        l_all[2 * u + 1] = l1
        return m0, l0, m1, l1, t0, t1, alpha1

    neg, zero = jnp.full((1, rows), NEG, jnp.float32), jnp.zeros((8, rows), jnp.float32)
    carry = (neg, zero, neg, zero, scores(0, cached(kc, 0), q_all[0]), scores(1, cached(kc, 0), q_all[1]), one)
    carry = lax.fori_loop(0, steps // 4, step_c, carry)
    wait_in(KN, kn.at[:, x])
    ring_first(2, kn)
    wait_in(VN, vn.at[:, x])
    ring_first(3, vn)
    carry = lax.fori_loop(steps // 4, steps - steps // 8, step_c, carry)
    ring_second(2, kn)
    ring_second(3, vn)
    carry = lax.fori_loop(steps - steps // 8, steps, step_c, carry)
    values(1, vtc[blocks - 1], carry[6], acc.at[2 * kv - 1])

    def other_rows(ref):
        return ref.at[pl.ds(0, (ny - 1) * new_a), :]

    wait_in(QY, other_rows(qabuf))
    wait_in(KAC, kac)
    wait_in(VAC, vac)
    wait_in(KAN, kan)
    wait_in(VAN, van)

    def turn_a(j, _):
        vtac[j] = vac[j].T
        return 0

    lax.fori_loop(0, kv, turn_a, 0)
    vtan[...] = van[...].T
    acc_a = (accx.at[0], accx.at[1])

    def unit_a(u, _):
        t0 = pl.multiple_of(u * 2 * tq, 2 * tq)
        load_q(qabuf, t0)
        tops = scores(0, kac[0], q_s[0]), scores(1, kac[0], q_s[1])
        state, tops = inner(kv, lambda j: kac[j], lambda j: vtac[j], lambda t: q_s[t], acc_a, fresh(acc_a), tops)
        pos_k = y * new_a + lax.broadcasted_iota(jnp.int32, (new_a, rows), 0)
        pos_q = t0 + token_of_lane((new_a, rows))
        out = []
        for half in range(2):
            m, l, alpha = expo(half, state[2 * half], state[2 * half + 1], tops[half])
            values(half, vtac[kv - 1], alpha, acc_a[half])
            s = jnp.where(pos_k <= pos_q + half * tq, qk(kan[...], q_s[half]), NEG)
            out.append(soft_step(scale2, s, vtan[...], m, total(l), acc_a[half]))
        for half, (m, l) in enumerate(out):
            r = pl.ds(pl.multiple_of(t0 + half * tq, tq), tq)
            row = lax.broadcasted_iota(jnp.int32, (dim, tq), 0)
            stat = jnp.zeros((dim, tq), jnp.float32)
            for g in range(grp):
                cols = slice(g * tq, (g + 1) * tq)
                oastage[r, pl.ds(g * dim, dim)] = accx[half, :, pl.ds(g * tq, tq)].T
                stat = jnp.where(row == g, m[:, cols], stat)
                stat = jnp.where(row == grp + g, l[:, cols], stat)
            ststage[r, :] = stat.T
        return 0

    lax.fori_loop(0, cp * ta // (2 * tq), unit_a, 0)

    def give_a(k, _):
        yy = lax.rem(y + k, ny)
        r = pl.ds(pl.multiple_of(yy * new_a, new_a), new_a)
        put(OA, oastage.at[r, :], oarecv.at[y], dev(yy, x, c))
        put(ST, ststage.at[r, :], strecv.at[y], dev(yy, x, c))
        return 0

    lax.fori_loop(1, ny, give_a, 0)
    copy(oastage.at[row_a, :], oarecv.at[y], recv_sem.at[OA])
    copy(ststage.at[row_a, :], strecv.at[y], recv_sem.at[ST])

    ring_last(2, kn)
    ring_last(3, vn)

    def turn_n(j, _):
        vtn[j] = vn[j // nx, lax.rem(j, nx)].T
        return 0

    lax.fori_loop(0, ny * nx, turn_n, 0)

    def new_keys(j):
        return kn[j // nx, lax.rem(j, nx)]

    def unit_of(i):
        return lax.rem(hb + 1 + i, kv)

    def unit_n(i, tops):
        u, u_after = unit_of(i), unit_of(lax.min(i + 1, kv - 1))
        yy, cc = u // CORES, lax.rem(u, CORES)
        last = yy * nx + x
        accs = (acc.at[2 * u], acc.at[2 * u + 1])
        state = (m_all[2 * u, 0:1, :], l_all[2 * u], m_all[2 * u + 1, 0:1, :], l_all[2 * u + 1])
        state, _ = inner(last + 1, new_keys, lambda j: vtn[j], lambda t: q_all[2 * u + t], accs, state, tops)
        pos_k = lax.broadcasted_iota(jnp.int32, (blk, rows), 0)
        pos_q = cc * tb + token_of_lane((blk, rows))
        tops = []
        for half in range(2):
            s = jnp.where(pos_k <= pos_q + half * tq, s_refs[half][...], NEG)
            s_refs[half][...] = s
            m, l, alpha = expo(half, state[2 * half], state[2 * half + 1], fold(s, jnp.maximum))
            tops.append(scores(half, new_keys(0), q_all[2 * u_after + half]))
            values(half, vtn[last], alpha, accs[half])
            inv = 1.0 / total(l)
            for g in range(grp):
                o = acc[2 * u + half, :, pl.ds(g * tq, tq)] * inv[:, g * tq:(g + 1) * tq]
                obuf[u, pl.ds(half * tq, tq), pl.ds(g * dim, dim)] = o.T.astype(bf)
        give(OB, obuf.at[u], ob.at[:, pl.ds(pl.multiple_of(hb * width, width), width)], peer_y(u))
        return tuple(tops)

    u = unit_of(0)
    tops = scores(0, new_keys(0), q_all[2 * u]), scores(1, new_keys(0), q_all[2 * u + 1])
    tops = lax.fori_loop(0, kv - 2, unit_n, tops)

    wait_in(OA, oarecv)
    wait_in(ST, strecv)
    for g in range(grp):
        cols = pl.ds(g * dim, dim)
        ms = [strecv[i, :, g:g + 1] for i in range(ny)]
        top = functools.reduce(jnp.maximum, ms)
        num = jnp.zeros((new_a, dim), jnp.float32)
        den = jnp.zeros((new_a, 1), jnp.float32)
        for i in range(ny):
            w = jnp.exp2((ms[i] - top) * scale2)
            num = num + w * oarecv[i, :, cols]
            den = den + w * strecv[i, :, grp + g:grp + g + 1]
        odone[:, cols] = (num / den).astype(bf)

    def home_a(r, _):
        give(OX, odone.at[pl.ds(pl.multiple_of(r * ta, ta), ta), :],
             oa.at[:, pl.ds(pl.multiple_of(ha * width, width), width)], peer_x(r))
        return 0

    lax.fori_loop(0, kv, home_a, 0)
    lax.fori_loop(kv - 2, kv, unit_n, tops)

    wait_in(OB, ob)
    wait_in(OX, oa)
    for i, ref in enumerate((nkb, nka, nvb, nva)):
        wait(ref, out_sem.at[i])
    most = pl.ds(0, kv - 1)
    for item, ref in ((KC, tkb), (VC, tvb), (KAC, tka), (VAC, tva), (Q, qbuf), (OB, obuf)):
        wait_out(item, ref.at[most])
    for item, ref in ((KN, qbuf), (VN, qbuf)):
        wait_out(item, ref.at[most, :, pl.ds(0, dim)])
    for item, ref in ((KAN, kan), (VAN, van)):
        wait_out(item, ref.at[pl.ds(0, (kv - 1) * ta), :])
    wait_out(QA, qabuf.at[pl.ds(0, (kv - 1) * ta), :])
    wait_out(OX, odone.at[pl.ds(0, (kv - 1) * ta), :])
    wait_out(QY, other_rows(qabuf))
    wait_out(OA, oarecv.at[pl.ds(0, ny - 1)])
    wait_out(ST, strecv.at[pl.ds(0, ny - 1)])
    ring_drain(0, kc)
    ring_drain(1, vc)
    ring_drain(2, kn)
    ring_drain(3, vn)


def attention(cp, xb, xa, cosf, sinf, wq, wk, wv, kcb, vcb, kca, vca):
    kv, dim = kcb.shape[1:]
    ny, nx = kv // CORES, cp // kv
    assert nx * CORES == kv and ny * nx * CORES == cp and ny == nx
    grp = wq.shape[1] // (kv * dim)
    tb, ta, cb, ca, model = xb.shape[0], xa.shape[0], kcb.shape[0], kca.shape[0], xb.shape[1]
    tq = tb // 2
    rows, width = grp * tq, grp * dim
    blk = CORES * tb
    assert blk == ca and (ny * nx * CORES * cb) % (ny * blk) == 0 and (cp * ta) % (2 * tq) == 0
    assert width == 2 * CORES * dim
    bf, f32 = jnp.bfloat16, jnp.float32
    vm = pltpu.VMEM
    scratch = [
        vm((tb + ta, model), bf),
        vm((2, model, width), bf),
        vm((kv, tb + ta, width), bf),
        vm((ny, tb + ta, width), bf),
        vm(kcb.shape, bf), vm(vcb.shape, bf), vm(kca.shape, bf), vm(vca.shape, bf),
        vm((kv, cb, dim), bf), vm((kv, cb, dim), bf), vm((kv, ca, dim), bf), vm((kv, ca, dim), bf),
        vm((kv, tb, width), bf),
        vm((ny, nx, CORES * cb, dim), bf),
        vm((ny, nx, CORES * cb, dim), bf),
        vm((ny, nx, blk, dim), bf),
        vm((ny, nx, blk, dim), bf),
        vm((cp * cb // blk, dim, blk), bf),
        vm((ny * nx, dim, blk), bf),
        vm((kv, tb, width), bf),
        vm((2 * kv, dim, rows), f32),
        vm((2 * kv, 8, rows), f32),
        vm((2 * kv, 8, rows), f32),
        vm((2, rows, dim), bf),
        vm((2 * kv, rows, dim), bf),
        vm((blk, rows), f32),
        vm((blk, rows), f32),
        vm((blk, rows), bf),
        vm((blk, rows), bf),
        vm((cp * ta, width), bf),
        vm((kv, ca, dim), bf),
        vm((kv, ca, dim), bf),
        vm((kv * ta, dim), bf),
        vm((kv * ta, dim), bf),
        vm((kv, dim, ca), bf),
        vm((dim, kv * ta), bf),
        vm((cp * ta, width), f32),
        vm((cp * ta, dim), f32),
        vm((ny, kv * ta, width), f32),
        vm((ny, kv * ta, dim), f32),
        vm((kv * ta, width), bf),
        vm((2, dim, rows), f32),
        pltpu.SemaphoreType.DMA((31,)),
        pltpu.SemaphoreType.DMA((31,)),
        pltpu.SemaphoreType.DMA((5,)),
        pltpu.SemaphoreType.DMA((2,)),
        pltpu.SemaphoreType.DMA((4,)),
    ]
    any_spec = pl.BlockSpec(memory_space=pl.ANY)
    vmem_spec = pl.BlockSpec(memory_space=pltpu.VMEM)
    shape = jax.ShapeDtypeStruct
    return pl.pallas_call(
        functools.partial(kernel, (ny, nx, kv, grp, dim)),
        out_shape=(shape((tb, kv * width), bf), shape((ta, kv * width), bf),
                   shape((tb, kv * dim), bf), shape((tb, kv * dim), bf),
                   shape((ta, kv * dim), bf), shape((ta, kv * dim), bf)),
        in_specs=[any_spec, any_spec, vmem_spec, vmem_spec] + [any_spec] * 7,
        out_specs=(any_spec,) * 6,
        scratch_shapes=scratch,
        compiler_params=pltpu.CompilerParams(
            collective_id=0, has_side_effects=True, vmem_limit_bytes=VMEM_LIMIT),
        name="attend",
    )(xb, xa, cosf, sinf, wq, wk, wv, kcb, vcb, kca, vca)


def out_kernel(ob, oa, w, yb, ya, o):
    tb = ob.shape[0]

    @pl.when(pl.program_id(0) == 0)
    def _():
        o[pl.ds(0, tb), :] = ob[...]
        o[pl.ds(tb, oa.shape[0]), :] = oa[...]

    out = jnp.dot(o[...], w[...], preferred_element_type=jnp.float32).astype(yb.dtype)
    yb[...] = out[:tb]
    ya[...] = out[tb:]


def output_projection(ob, oa, w):
    (tb, inner), ta, model = ob.shape, oa.shape[0], w.shape[1]
    cols = min(512, model)
    shape = jax.ShapeDtypeStruct
    return pl.pallas_call(
        out_kernel,
        grid=(model // cols,),
        out_shape=(shape((tb, model), ob.dtype), shape((ta, model), ob.dtype)),
        in_specs=[pl.BlockSpec((tb, inner), lambda i: (0, 0)), pl.BlockSpec((ta, inner), lambda i: (0, 0)),
                  pl.BlockSpec((inner, cols), lambda i: (0, i))],
        out_specs=(pl.BlockSpec((tb, cols), lambda i: (0, i)), pl.BlockSpec((ta, cols), lambda i: (0, i))),
        scratch_shapes=[pltpu.VMEM((tb + ta, inner), ob.dtype)],
        compiler_params=pltpu.CompilerParams(vmem_limit_bytes=VMEM_LIMIT),
        name="project_out",
    )(ob, oa, w)


def solution(mesh):
    cp_size = mesh.shape["cp"]

    def local_step(x_a, kc_a, vc_a, x_b, kc_b, vc_b, w_q, w_k, w_v, w_o):
        ta, tb = x_a.shape[0], x_b.shape[0]
        kv, dim = kc_a.shape[1:]
        me = lax.axis_index("cp")
        pos_a = kc_a.shape[0] * cp_size + me * ta + jnp.arange(ta)
        pos_b = kc_b.shape[0] * cp_size + me * tb + jnp.arange(tb)
        cosf, sinf = rope_tables(jnp.concatenate([pos_b, pos_a]), dim)
        o_b, o_a, k_b, v_b, k_a, v_a = attention(cp_size, x_b, x_a, cosf, sinf, w_q, w_k, w_v, kc_b, vc_b, kc_a, vc_a)
        y_b, y_a = output_projection(o_b, o_a, w_o)
        heads = lambda t: t.reshape(t.shape[0], kv, dim)
        return y_a, heads(k_a), heads(v_a), y_b, heads(k_b), heads(v_b)

    row_spec = P(("dp", "cp"), None)
    kv_spec = P(("dp", "cp"), None, None)
    full_spec = P()
    return jax.shard_map(
        local_step, mesh=mesh,
        in_specs=(row_spec, kv_spec, kv_spec, row_spec, kv_spec, kv_spec, full_spec, full_spec, full_spec, full_spec),
        out_specs=(row_spec, kv_spec, kv_spec, row_spec, kv_spec, kv_spec), check_vma=False)
```

```python
import functools

import jax
import jax.numpy as jnp
from jax import lax
from jax.experimental import pallas as pl
from jax.experimental.pallas import tpu as pltpu
from jax.sharding import PartitionSpec as P

ROPE_BASE = 500000
LOG2E = 1.4426950408889634
NEG = float(jnp.finfo(jnp.float32).min)
MESH = pl.DeviceIdType.MESH
CORES = 2
VMEM_LIMIT = 62 * 1024 * 1024


def rope_tables(positions, head_dim):
    half_dim = head_dim // 2
    inv_freq = jnp.power(jnp.float32(ROPE_BASE), jnp.arange(half_dim, dtype=jnp.float32) * (-2.0 / head_dim))
    angles = positions.astype(jnp.float32)[:, None] * inv_freq[None, :]
    cos_ang, sin_ang = jnp.cos(angles), jnp.sin(angles)
    return jnp.concatenate([cos_ang, cos_ang], axis=1), jnp.concatenate([-sin_ang, sin_ang], axis=1)


def qk(keys, queries):
    return lax.dot_general(keys, queries, (((1,), (1,)), ((), ())), preferred_element_type=jnp.float32)


def fold(s, op):
    return functools.reduce(op, [s[i:i + 8] for i in range(0, s.shape[0], 8)])


def soft_step(scale2, s, vt, m, l, acc_ref):
    m_new = jnp.maximum(m, jnp.max(s, axis=0, keepdims=True))
    alpha = jnp.exp2((m - m_new) * scale2)
    e = jnp.exp2((s - m_new) * scale2)
    l_new = l * alpha + jnp.sum(e, axis=0, keepdims=True)
    pv = jnp.dot(vt, e.astype(jnp.bfloat16), preferred_element_type=jnp.float32)
    acc_ref[...] = acc_ref[...] * alpha + pv
    return m_new, l_new


def kernel(dims, xb, xa, cosf, sinf, wq, wk, wv, kcb, vcb, kca, vca, ob, oa, nkb, nvb, nka, nva,
           xs, wbuf, qsend, kvsend, rkb, rvb, rka, rva, tkb, tvb, tka, tva,
           qbuf, kc, vc, kn, vn, vtc, vtn, obuf, acc, m_all, l_all, q_a, q_all, s0, s1, s2, s3, p0, p1, p2, p3,
           qabuf, kac, vac, kan, van, vtac, vtan, oastage, ststage, oarecv, strecv, odone, acc_a,
           send_sem, recv_sem, load_sem, wsem, out_sem):
    ny, nx, kv, grp, dim = dims
    cp = ny * nx * CORES
    tb, ta = xb.shape[0], xa.shape[0]
    tq = tb // 2
    rows = grp * tq
    width = grp * dim
    pair = CORES * dim
    cb = kcb.shape[0]
    scale2 = dim ** -0.5 * LOG2E
    bf = jnp.bfloat16

    me = lax.axis_index("cp")
    c = lax.rem(me, CORES)
    x = lax.rem(me // CORES, nx)
    y = me // (CORES * nx)
    hb = y * CORES + c
    ha = x * CORES + c

    def dev(yy, xx, cc):
        return (yy * nx + xx) * CORES + cc

    def peer_y(h):
        return dev(h // CORES, x, lax.rem(h, CORES))

    def peer_x(h):
        return dev(y, h // CORES, lax.rem(h, CORES))

    def put(item, src, dst, target):
        pltpu.make_async_remote_copy(
            src_ref=src, dst_ref=dst, send_sem=send_sem.at[item], recv_sem=recv_sem.at[item],
            device_id={"cp": target}, device_id_type=MESH,
        ).start()

    def copy(src, dst, sem):
        pltpu.make_async_copy(src, dst, sem).start()

    def wait(ref, sem):
        pltpu.make_async_copy(ref, ref, sem).wait()

    def give(item, src, dst, target):
        @pl.when(target == me)
        def _():
            copy(src, dst, recv_sem.at[item])

        @pl.when(target != me)
        def _():
            put(item, src, dst, target)

    def wait_in(item, ref):
        wait(ref, recv_sem.at[item])

    def wait_out(item, ref):
        wait(ref, send_sem.at[item])

    KC, VC, Q, KN, VN, KAC, VAC, KAN, VAN, QA, QY, OB, OA, ST, OX = range(15)
    QS = 15
    AG = QS + ny

    barrier = pltpu.get_barrier_semaphore()

    def greet(d, _):
        pl.semaphore_signal(barrier, inc=1, device_id={"cp": d}, device_id_type=MESH)
        return 0

    raw = ((kcb, rkb, tkb), (vcb, rvb, tvb), (kca, rka, tka), (vca, rva, tva))
    for i, (src, dst, _) in enumerate(raw):
        copy(src, dst, load_sem.at[i])
    copy(xb, xs.at[pl.ds(0, tb), :], load_sem.at[4])
    copy(xa, xs.at[pl.ds(tb, ta), :], load_sem.at[4])

    q_steps, kv_steps = kv, kv // CORES

    def q_head(i):
        return lax.rem(hb + 1 + i, kv)

    def kv_pair(i):
        return lax.rem(y + 1 + i, ny)

    def load_wq(i, slot):
        copy(wq.at[:, pl.ds(pl.multiple_of(q_head(i) * width, width), width)], wbuf.at[slot], wsem.at[slot])

    def load_wkv(i, slot):
        cols = pl.ds(pl.multiple_of(kv_pair(i) * pair, pair), pair)
        copy(wk.at[:, cols], wbuf.at[slot, :, pl.ds(0, pair)], wsem.at[slot])
        copy(wv.at[:, cols], wbuf.at[slot, :, pl.ds(pair, pair)], wsem.at[slot])

    load_wq(0, 0)
    lax.fori_loop(0, cp, greet, 0)
    for i, (_, dst, turned) in enumerate(raw):
        wait(dst, load_sem.at[i])
        turned[...] = jnp.transpose(dst[...], (1, 0, 2))
    pl.semaphore_wait(barrier, cp)

    def scatter(item, src, dst, mine, peer):
        def one(k, _):
            h = lax.rem(mine + k, kv)
            put(item, src.at[h], dst, peer(h))
            return 0

        lax.fori_loop(1, kv, one, 0)
        copy(src.at[mine], dst, recv_sem.at[item])

    c_rows = pl.ds(pl.multiple_of(c * cb, cb), cb)
    scatter(KC, tkb, kc.at[y, x, c_rows, :], hb, peer_y)
    scatter(VC, tvb, vc.at[y, x, c_rows, :], hb, peer_y)

    right = dev(y, lax.rem(x + 1, nx), c)
    left = dev(y, lax.rem(x + nx - 1, nx), c)
    x_left = lax.rem(x + nx - 1, nx)
    x_right = lax.rem(x + 1, nx)
    x_far = lax.rem(x + nx // 2, nx)
    lo, hi = pl.ds(0, ny // 2), pl.ds(ny // 2, ny // 2)

    def ag_sem(i, step, direction):
        return AG + i * 4 + step * 2 + direction

    def ring_first(i, buf):
        put(ag_sem(i, 0, 0), buf.at[:, x], buf.at[:, x], right)
        put(ag_sem(i, 0, 1), buf.at[:, x], buf.at[:, x], left)

    def ring_second(i, buf):
        wait_in(ag_sem(i, 0, 0), buf.at[:, x_left])
        put(ag_sem(i, 1, 0), buf.at[lo, x_left], buf.at[lo, x_left], right)
        wait_in(ag_sem(i, 0, 1), buf.at[:, x_right])
        put(ag_sem(i, 1, 1), buf.at[hi, x_right], buf.at[hi, x_right], left)

    def ring_last(i, buf):
        wait_in(ag_sem(i, 1, 0), buf.at[lo, x_far])
        wait_in(ag_sem(i, 1, 1), buf.at[hi, x_far])

    def ring_drain(i, buf):
        wait_out(ag_sem(i, 0, 0), buf.at[:, x])
        wait_out(ag_sem(i, 0, 1), buf.at[:, x])
        wait_out(ag_sem(i, 1, 0), buf.at[lo, x])
        wait_out(ag_sem(i, 1, 1), buf.at[hi, x])

    wait(xs, load_sem.at[4])
    b_rows, a_rows = pl.ds(0, tb), pl.ds(tb, ta)
    my_a = pl.ds(pl.multiple_of(me * ta, ta), ta)

    def rope(t):
        t = t.astype(bf).astype(jnp.float32)
        return (t * cosf[...] + pltpu.roll(t, dim // 2, 1) * sinf[...]).astype(bf)

    def project(slot):
        return jnp.dot(xs[...], wbuf[slot], preferred_element_type=jnp.float32)

    def q_step(i, _):
        slot = lax.rem(i, 2)

        @pl.when(i + 1 < q_steps)
        def _():
            load_wq(i + 1, 1 - slot)

        @pl.when(i + 1 == q_steps)
        def _():
            load_wkv(0, 1 - slot)

        wait(wbuf.at[slot], wsem.at[slot])
        h = q_head(i)
        lin = project(slot)
        for g in range(grp):
            cols = slice(g * dim, (g + 1) * dim)
            qsend[h, :, cols] = rope(lin[:, cols])
        give(QS + lax.rem(y - h // CORES + ny, ny), qsend.at[h, b_rows], qbuf.at[hb], peer_y(h))
        give(QA, qsend.at[h, a_rows], qabuf.at[my_a, :], peer_x(h))
        return 0

    def kv_step(i, _):
        slot = lax.rem(q_steps + i, 2)

        @pl.when(i + 1 < kv_steps)
        def _():
            load_wkv(i + 1, 1 - slot)

        wait(wbuf.at[slot], wsem.at[slot])
        p = kv_pair(i)
        lin = project(slot)
        for g in range(CORES):
            cols = slice(g * dim, (g + 1) * dim)
            kvsend[p, :, cols] = rope(lin[:, cols])
        kvsend[p, :, pair:2 * pair] = lin[:, pair:2 * pair].astype(bf)
        for j, (nb, na) in enumerate(((nkb, nka), (nvb, nva))):
            for g in range(CORES):
                cols = pl.ds(j * pair + g * dim, dim)
                copy(kvsend.at[p, b_rows, cols], nb.at[p * CORES + g], out_sem.at[2 * j])
                copy(kvsend.at[p, a_rows, cols], na.at[p * CORES + g], out_sem.at[2 * j + 1])
        n_rows = pl.ds(pl.multiple_of(c * tb, tb), tb)
        s_rows = pl.ds(pl.multiple_of(ha * ta, ta), ta)
        for g in range(CORES):
            for j, (ib, db, ia, da) in enumerate(((KN, kn, KAN, kan), (VN, vn, VAN, van))):
                cols = pl.ds(j * pair + g * dim, dim)
                give(ib, kvsend.at[p, b_rows, cols], db.at[y, x, n_rows, :], dev(p, x, g))
                give(ia, kvsend.at[p, a_rows, cols], da.at[s_rows, :], dev(y, p, g))
        return 0

    lax.fori_loop(0, q_steps // 2, q_step, 0)
    wait_in(KC, kc.at[:, x])
    ring_first(0, kc)
    wait_in(VC, vc.at[:, x])
    ring_first(1, vc)
    lax.fori_loop(q_steps // 2, q_steps, q_step, 0)
    ring_second(0, kc)
    ring_second(1, vc)
    scatter(KAC, tka, kac.at[ha], ha, peer_x)
    lax.fori_loop(0, kv_steps, kv_step, 0)
    scatter(VAC, tva, vac.at[ha], ha, peer_x)
    new_a = kan.shape[0]
    row_a = pl.ds(pl.multiple_of(y * new_a, new_a), new_a)
    wait_in(QA, qabuf.at[row_a, :])

    def pass_qa(k, _):
        put(QY, qabuf.at[row_a, :], qabuf.at[row_a, :], dev(lax.rem(y + k, ny), x, c))
        return 0

    lax.fori_loop(1, ny, pass_qa, 0)

    s_refs, p_refs = (s0, s1, s2, s3), (p0, p1, p2, p3)
    blk = s0.shape[0]
    tiles = range(4)

    def scores(t, keys, queries):
        s = qk(keys, queries)
        s_refs[t][...] = s
        return fold(s, jnp.maximum)

    def highest(m, top8):
        m_new = jnp.maximum(m, jnp.max(top8, axis=0, keepdims=True))
        return m_new, jnp.exp2((m - m_new) * scale2)

    def expo(t, m, l8, top8):
        m_new, alpha = highest(m, top8)
        l8 = l8 * alpha
        for r in range(0, blk, 16):
            e = jnp.exp2((s_refs[t][pl.ds(r, 16), :] - m_new) * scale2)
            p_refs[t][pl.ds(r, 16), :] = e.astype(bf)
            l8 = l8 + fold(e, jnp.add)
        return m_new, l8, alpha

    def values(t, vt, alpha, acc_ref):
        acc_ref[...] = acc_ref[...] * alpha + jnp.dot(vt, p_refs[t][...], preferred_element_type=jnp.float32)

    def step(carry, before, now, k_after, q_after, acc_before, accs):
        m, l, top = list(carry[0:4]), list(carry[4:8]), list(carry[8:12])
        values(3, before, carry[12], acc_before)
        for t in tiles:
            m[t], l[t], alpha = expo(t, m[t], l[t], top[t])
            top[t] = scores(t, k_after, q_after(t))
            if t < 3:
                values(t, now, alpha, accs[t])
        return tuple(m + l + top) + (alpha,)

    neg, zero = jnp.full((1, rows), NEG, jnp.float32), jnp.zeros((8, rows), jnp.float32)
    one = jnp.ones((1, rows), jnp.float32)

    def total(l8):
        return jnp.sum(l8, axis=0, keepdims=True)

    def token_of_lane(shape):
        return lax.rem(lax.broadcasted_iota(jnp.int32, shape, 1), tq)

    def turn(n, dst, block):
        def four(i, _):
            for k in range(4):
                dst[4 * i + k] = block(4 * i + k).T
            return 0

        lax.fori_loop(0, n // 4, four, 0)

    blocks = vtc.shape[0]
    per_row = blocks // ny
    per_blk = nx // per_row
    acc[...] = jnp.zeros_like(acc)
    p3[...] = jnp.zeros_like(p3)

    def row_of(i):
        return lax.rem(y + i, ny)

    def arrive_q(i):
        yy = row_of(i)
        wait_in(QS + i, qbuf.at[pl.ds(yy * CORES, CORES)])
        for t in tiles:
            u, half = yy * CORES + t // 2, t % 2
            for g in range(grp):
                q_all[4 * yy + t, pl.ds(g * tq, tq), :] = qbuf[u, pl.ds(half * tq, tq), pl.ds(g * dim, dim)]

    def cached(buf, j):
        return buf[j // per_row, pl.ds(lax.rem(j, per_row) * per_blk, per_blk)].reshape(blk, dim)

    arrive_q(0)
    ring_last(0, kc)
    ring_last(1, vc)
    turn(blocks, vtc, lambda j: cached(vc, j))

    def step_c(i, carry):
        yy, j = row_of(i // blocks), lax.rem(i, blocks)
        before, after = lax.max(i - 1, 0), lax.min(i + 1, ny * blocks - 1)
        y_before, y_after = row_of(before // blocks), row_of(after // blocks)
        start = j == 0
        m = tuple(jnp.where(start, NEG, v) for v in carry[0:4])
        l = tuple(jnp.where(start, 0.0, v) for v in carry[4:8])
        out = step(
            m + l + carry[8:], vtc[lax.rem(before, blocks)], vtc[j], cached(kc, lax.rem(after, blocks)),
            lambda t: q_all[4 * y_after + t], acc.at[4 * y_before + 3], [acc.at[4 * yy + t] for t in tiles])
        for t in tiles:
            m_all[4 * yy + t, 0:1, :] = out[t]
            l_all[4 * yy + t] = out[4 + t]
        return out

    tops = tuple(scores(t, cached(kc, 0), q_all[4 * y + t]) for t in tiles)
    carry = (neg,) * 4 + (zero,) * 4 + tops + (one,)
    carry = lax.fori_loop(0, blocks - 1, step_c, carry)
    arrive_q(1)
    carry = lax.fori_loop(blocks - 1, 2 * blocks - 1, step_c, carry)
    wait_in(KN, kn.at[:, x])
    ring_first(2, kn)
    wait_in(VN, vn.at[:, x])
    ring_first(3, vn)
    arrive_q(2)
    carry = lax.fori_loop(2 * blocks - 1, 3 * blocks - 1, step_c, carry)
    arrive_q(3)
    carry = lax.fori_loop(3 * blocks - 1, 4 * blocks, step_c, carry)
    ring_second(2, kn)
    ring_second(3, vn)
    values(3, vtc[blocks - 1], carry[12], acc.at[4 * row_of(ny - 1) + 3])

    def other_rows(ref):
        return ref.at[pl.ds(0, (ny - 1) * new_a), :]

    wait_in(QY, other_rows(qabuf))
    wait_in(KAC, kac)
    wait_in(VAC, vac)
    wait_in(KAN, kan)
    wait_in(VAN, van)
    turn(kv, vtac, lambda j: vac[j])
    vtan[...] = van[...].T
    for t in tiles:
        for g in range(grp):
            q_a[t, pl.ds(g * tq, tq), :] = qabuf[pl.ds(t * tq, tq), pl.ds(g * dim, dim)]
    acc_a[...] = jnp.zeros_like(acc_a)
    p3[...] = jnp.zeros_like(p3)
    accs_a = [acc_a.at[t] for t in tiles]

    def step_a(j, carry):
        return step(carry, vtac[lax.max(j - 1, 0)], vtac[j], kac[j + 1], lambda t: q_a[t], accs_a[3], accs_a)

    tops = tuple(scores(t, kac[0], q_a[t]) for t in tiles)
    carry = lax.fori_loop(0, kv - 1, step_a, (neg,) * 4 + (zero,) * 4 + tops + (one,))
    values(3, vtac[kv - 2], carry[12], accs_a[3])
    pos_k = y * new_a + lax.broadcasted_iota(jnp.int32, (new_a, rows), 0)
    pos_q = token_of_lane((new_a, rows))
    row = lax.broadcasted_iota(jnp.int32, (dim, tq), 0)
    for t in tiles:
        m, l, alpha = expo(t, carry[t], carry[4 + t], carry[8 + t])
        values(t, vtac[kv - 1], alpha, accs_a[t])
        s = jnp.where(pos_k <= pos_q + t * tq, qk(kan[...], q_a[t]), NEG)
        m, l = soft_step(scale2, s, vtan[...], m, total(l), accs_a[t])
        stat = jnp.zeros((dim, tq), jnp.float32)
        for g in range(grp):
            cols = slice(g * tq, (g + 1) * tq)
            oastage[pl.ds(t * tq, tq), pl.ds(g * dim, dim)] = acc_a[t, :, cols].T
            stat = jnp.where(row == g, m[:, cols], stat)
            stat = jnp.where(row == grp + g, l[:, cols], stat)
        ststage[pl.ds(t * tq, tq), :] = stat.T

    def give_a(k, _):
        yy = lax.rem(y + k, ny)
        r = pl.ds(pl.multiple_of(yy * new_a, new_a), new_a)
        put(OA, oastage.at[r, :], oarecv.at[y], dev(yy, x, c))
        put(ST, ststage.at[r, :], strecv.at[y], dev(yy, x, c))
        return 0

    lax.fori_loop(1, ny, give_a, 0)
    copy(oastage.at[row_a, :], oarecv.at[y], recv_sem.at[OA])
    copy(ststage.at[row_a, :], strecv.at[y], recv_sem.at[ST])

    ring_last(2, kn)
    ring_last(3, vn)
    turn(ny * nx, vtn, lambda j: vn[j // nx, lax.rem(j, nx)])

    def new_keys(j):
        return kn[j // nx, lax.rem(j, nx)]

    def rows_n(i, tops):
        yy, y_after = row_of(1 + i), row_of(lax.min(2 + i, ny))
        last = yy * nx + x
        accs = [acc.at[4 * yy + t] for t in tiles]
        p3[...] = jnp.zeros_like(p3)

        def step_n(j, carry):
            return step(carry, vtn[lax.max(j - 1, 0)], vtn[j], new_keys(j + 1), lambda t: q_all[4 * yy + t],
                        accs[3], accs)

        state = tuple(m_all[4 * yy + t, 0:1, :] for t in tiles) + tuple(l_all[4 * yy + t] for t in tiles)
        carry = lax.fori_loop(0, last, step_n, state + tuple(tops) + (one,))
        values(3, vtn[lax.max(last - 1, 0)], carry[12], accs[3])
        tops = []
        for t in tiles:
            seen = (t + 1) * tq
            tri = lax.broadcasted_iota(jnp.int32, (tq, rows), 0) <= token_of_lane((tq, rows))
            s = jnp.where(tri, s_refs[t][pl.ds(t * tq, tq), :], NEG)
            s_refs[t][pl.ds(t * tq, tq), :] = s
            top8 = fold(s, jnp.maximum)
            if t:
                top8 = jnp.maximum(top8, fold(s_refs[t][pl.ds(0, t * tq), :], jnp.maximum))
            m_new, alpha = highest(carry[t], top8)
            l8 = carry[4 + t] * alpha
            for r in range(0, seen, 16):
                e = jnp.exp2((s_refs[t][pl.ds(r, 16), :] - m_new) * scale2)
                p_refs[t][pl.ds(r, 16), :] = e.astype(bf)
                l8 = l8 + fold(e, jnp.add)
            tops.append(scores(t, new_keys(0), q_all[4 * y_after + t]))
            pv = jnp.dot(vtn[last, :, pl.ds(0, seen)], p_refs[t][pl.ds(0, seen), :], preferred_element_type=jnp.float32)
            o = (accs[t][...] * alpha + pv) * (1.0 / total(l8))
            for g in range(grp):
                obuf[yy * CORES + t // 2, pl.ds(t % 2 * tq, tq), pl.ds(g * dim, dim)] = (
                    o[:, g * tq:(g + 1) * tq].T.astype(bf))
        for cc in range(CORES):
            u = yy * CORES + cc
            give(OB, obuf.at[u], ob.at[:, pl.ds(pl.multiple_of(hb * width, width), width)], peer_y(u))
        return tuple(tops)

    tops = tuple(scores(t, new_keys(0), q_all[4 * row_of(1) + t]) for t in tiles)
    tops = lax.fori_loop(0, ny - 1, rows_n, tops)

    wait_in(OA, oarecv)
    wait_in(ST, strecv)
    for g in range(grp):
        cols = pl.ds(g * dim, dim)
        ms = [strecv[i, :, g:g + 1] for i in range(ny)]
        top = functools.reduce(jnp.maximum, ms)
        num = jnp.zeros((new_a, dim), jnp.float32)
        den = jnp.zeros((new_a, 1), jnp.float32)
        for i in range(ny):
            w = jnp.exp2((ms[i] - top) * scale2)
            num = num + w * oarecv[i, :, cols]
            den = den + w * strecv[i, :, grp + g:grp + g + 1]
        odone[:, cols] = (num / den).astype(bf)

    def home_a(r, _):
        give(OX, odone.at[pl.ds(pl.multiple_of(r * ta, ta), ta), :],
             oa.at[:, pl.ds(pl.multiple_of(ha * width, width), width)], peer_x(r))
        return 0

    lax.fori_loop(0, kv, home_a, 0)
    lax.fori_loop(ny - 1, ny, rows_n, tops)

    wait_in(OB, ob)
    wait_in(OX, oa)
    for i, ref in enumerate((nkb, nka, nvb, nva)):
        wait(ref, out_sem.at[i])
    most = pl.ds(0, kv - 1)
    for item, ref in ((KC, tkb), (VC, tvb), (KAC, tka), (VAC, tva), (OB, obuf)):
        wait_out(item, ref.at[most])
    wait_out(QS, qbuf.at[pl.ds(0, CORES - 1)])
    for i in range(1, ny):
        wait_out(QS + i, qbuf.at[pl.ds(0, CORES)])
    for item, ref in ((KN, qbuf), (VN, qbuf)):
        wait_out(item, ref.at[most, :, pl.ds(0, dim)])
    for item, ref in ((KAN, kan), (VAN, van)):
        wait_out(item, ref.at[pl.ds(0, (kv - 1) * ta), :])
    wait_out(QA, qabuf.at[pl.ds(0, (kv - 1) * ta), :])
    wait_out(OX, odone.at[pl.ds(0, (kv - 1) * ta), :])
    wait_out(QY, other_rows(qabuf))
    wait_out(OA, oarecv.at[pl.ds(0, ny - 1)])
    wait_out(ST, strecv.at[pl.ds(0, ny - 1)])
    ring_drain(0, kc)
    ring_drain(1, vc)
    ring_drain(2, kn)
    ring_drain(3, vn)


def attention(cp, xb, xa, cosf, sinf, wq, wk, wv, kcb, vcb, kca, vca):
    kv, dim = kcb.shape[1:]
    ny, nx = kv // CORES, cp // kv
    assert nx * CORES == kv and ny * nx * CORES == cp and ny == nx
    grp = wq.shape[1] // (kv * dim)
    tb, ta, cb, ca, model = xb.shape[0], xa.shape[0], kcb.shape[0], kca.shape[0], xb.shape[1]
    tq = tb // 2
    rows, width = grp * tq, grp * dim
    blk = CORES * tb
    assert blk == ca and (ny * nx * CORES * cb) % (ny * blk) == 0 and (cp * ta) % (2 * tq) == 0
    assert width == 2 * CORES * dim and cp * ta == 4 * tq and CORES == 2
    bf, f32 = jnp.bfloat16, jnp.float32
    vm = pltpu.VMEM
    scratch = [
        vm((tb + ta, model), bf),
        vm((2, model, width), bf),
        vm((kv, tb + ta, width), bf),
        vm((ny, tb + ta, width), bf),
        vm(kcb.shape, bf), vm(vcb.shape, bf), vm(kca.shape, bf), vm(vca.shape, bf),
        vm((kv, cb, dim), bf), vm((kv, cb, dim), bf), vm((kv, ca, dim), bf), vm((kv, ca, dim), bf),
        vm((kv, tb, width), bf),
        vm((ny, nx, CORES * cb, dim), bf),
        vm((ny, nx, CORES * cb, dim), bf),
        vm((ny, nx, blk, dim), bf),
        vm((ny, nx, blk, dim), bf),
        vm((cp * cb // blk, dim, blk), bf),
        vm((ny * nx, dim, blk), bf),
        vm((kv, tb, width), bf),
        vm((2 * kv, dim, rows), f32),
        vm((2 * kv, 8, rows), f32),
        vm((2 * kv, 8, rows), f32),
        vm((4, rows, dim), bf),
        vm((2 * kv, rows, dim), bf),
        vm((blk, rows), f32), vm((blk, rows), f32), vm((blk, rows), f32), vm((blk, rows), f32),
        vm((blk, rows), bf), vm((blk, rows), bf), vm((blk, rows), bf), vm((blk, rows), bf),
        vm((cp * ta, width), bf),
        vm((kv, ca, dim), bf),
        vm((kv, ca, dim), bf),
        vm((kv * ta, dim), bf),
        vm((kv * ta, dim), bf),
        vm((kv, dim, ca), bf),
        vm((dim, kv * ta), bf),
        vm((cp * ta, width), f32),
        vm((cp * ta, dim), f32),
        vm((ny, kv * ta, width), f32),
        vm((ny, kv * ta, dim), f32),
        vm((kv * ta, width), bf),
        vm((4, dim, rows), f32),
        pltpu.SemaphoreType.DMA((15 + ny + 16,)),
        pltpu.SemaphoreType.DMA((15 + ny + 16,)),
        pltpu.SemaphoreType.DMA((5,)),
        pltpu.SemaphoreType.DMA((2,)),
        pltpu.SemaphoreType.DMA((4,)),
    ]
    any_spec = pl.BlockSpec(memory_space=pl.ANY)
    vmem_spec = pl.BlockSpec(memory_space=pltpu.VMEM)
    shape = jax.ShapeDtypeStruct
    return pl.pallas_call(
        functools.partial(kernel, (ny, nx, kv, grp, dim)),
        out_shape=(shape((tb, kv * width), bf), shape((ta, kv * width), bf),
                   shape((kv, tb, dim), bf), shape((kv, tb, dim), bf),
                   shape((kv, ta, dim), bf), shape((kv, ta, dim), bf)),
        in_specs=[any_spec, any_spec, vmem_spec, vmem_spec] + [any_spec] * 7,
        out_specs=(any_spec,) * 6,
        scratch_shapes=scratch,
        compiler_params=pltpu.CompilerParams(
            collective_id=0, has_side_effects=True, vmem_limit_bytes=VMEM_LIMIT),
        name="attend",
    )(xb, xa, cosf, sinf, wq, wk, wv, kcb, vcb, kca, vca)


SLOTS = 3


def out_kernel(ob, oa, w, kb, vb, ka, va, yb, ya, nkb, nvb, nka, nva, o, wbuf, ybuf, *rest):
    new, turned, (wsem, osem, nsem, ysem) = rest[:4], rest[4:8], rest[8:]
    tb, ta = ob.shape[0], oa.shape[0]
    cols = wbuf.shape[2]
    steps = w.shape[1] // cols
    b_rows, a_rows = pl.ds(0, tb), pl.ds(tb, ta)

    def copy(src, dst, sem):
        pltpu.make_async_copy(src, dst, sem).start()

    def wait(ref, sem):
        pltpu.make_async_copy(ref, ref, sem).wait()

    def span(i):
        return pl.ds(pl.multiple_of(i * cols, cols), cols)

    def load(i):
        copy(w.at[:, span(i)], wbuf.at[lax.rem(i, SLOTS)], wsem.at[lax.rem(i, SLOTS)])

    copy(ob, o.at[b_rows, :], osem)
    copy(oa, o.at[a_rows, :], osem)
    for i in range(min(SLOTS - 1, steps)):
        load(i)
    for i, (src, dst) in enumerate(zip((kb, vb, ka, va), new)):
        copy(src, dst, nsem.at[i])
    wait(o, osem)

    def step(i, _):
        @pl.when(i + SLOTS - 1 < steps)
        def _():
            load(i + SLOTS - 1)

        slot = lax.rem(i, SLOTS)
        wait(wbuf.at[slot], wsem.at[slot])
        ybuf[i] = jnp.dot(o[...], wbuf[slot], preferred_element_type=jnp.float32).astype(ybuf.dtype)
        copy(ybuf.at[i, b_rows, :], yb.at[:, span(i)], ysem.at[0])
        copy(ybuf.at[i, a_rows, :], ya.at[:, span(i)], ysem.at[1])
        return 0

    lax.fori_loop(0, steps, step, 0)
    for i, (src, dst, out) in enumerate(zip(new, turned, (nkb, nvb, nka, nva))):
        wait(src, nsem.at[i])
        dst[...] = jnp.transpose(src[...], (1, 0, 2))
        copy(dst, out, nsem.at[i])
    wait(yb, ysem.at[0])
    wait(ya, ysem.at[1])
    for i, out in enumerate((nkb, nvb, nka, nva)):
        wait(out, nsem.at[i])


def output_projection(ob, oa, w, *new):
    (tb, inner), ta, model = ob.shape, oa.shape[0], w.shape[1]
    cols = min(512, model)
    shape = jax.ShapeDtypeStruct
    bf, vm, dma = ob.dtype, pltpu.VMEM, pltpu.SemaphoreType.DMA
    turned = [(t.shape[1], t.shape[0], t.shape[2]) for t in new]
    any_spec = pl.BlockSpec(memory_space=pl.ANY)
    return pl.pallas_call(
        out_kernel,
        out_shape=[shape((tb, model), bf), shape((ta, model), bf)] + [shape(t, bf) for t in turned],
        in_specs=[any_spec] * 7,
        out_specs=[any_spec] * 6,
        scratch_shapes=[vm((tb + ta, inner), bf), vm((SLOTS, inner, cols), bf), vm((model // cols, tb + ta, cols), bf)]
        + [vm(t.shape, bf) for t in new] + [vm(t, bf) for t in turned] + [dma((SLOTS,)), dma, dma((4,)), dma((2,))],
        compiler_params=pltpu.CompilerParams(vmem_limit_bytes=VMEM_LIMIT),
        name="project_out",
    )(ob, oa, w, *new)


def solution(mesh):
    cp_size = mesh.shape["cp"]

    def local_step(x_a, kc_a, vc_a, x_b, kc_b, vc_b, w_q, w_k, w_v, w_o):
        ta, tb = x_a.shape[0], x_b.shape[0]
        kv, dim = kc_a.shape[1:]
        me = lax.axis_index("cp")
        pos_a = kc_a.shape[0] * cp_size + me * ta + jnp.arange(ta)
        pos_b = kc_b.shape[0] * cp_size + me * tb + jnp.arange(tb)
        cosf, sinf = rope_tables(jnp.concatenate([pos_b, pos_a]), dim)
        o_b, o_a, k_b, v_b, k_a, v_a = attention(cp_size, x_b, x_a, cosf, sinf, w_q, w_k, w_v, kc_b, vc_b, kc_a, vc_a)
        y_b, y_a, k_b, v_b, k_a, v_a = output_projection(o_b, o_a, w_o, k_b, v_b, k_a, v_a)
        return y_a, k_a, v_a, y_b, k_b, v_b

    row_spec = P(("dp", "cp"), None)
    kv_spec = P(("dp", "cp"), None, None)
    full_spec = P()
    return jax.shard_map(
        local_step, mesh=mesh,
        in_specs=(row_spec, kv_spec, kv_spec, row_spec, kv_spec, kv_spec, full_spec, full_spec, full_spec, full_spec),
        out_specs=(row_spec, kv_spec, kv_spec, row_spec, kv_spec, kv_spec), check_vma=False)
```

```python
import functools

import jax
import jax.numpy as jnp
from jax import lax
from jax.experimental import pallas as pl
from jax.experimental.pallas import tpu as pltpu
from jax.sharding import PartitionSpec as P

ROPE_BASE = 500000
LOG2E = 1.4426950408889634
NEG = float(jnp.finfo(jnp.float32).min)
MESH = pl.DeviceIdType.MESH
CORES = 2
VMEM_LIMIT = 62 * 1024 * 1024
SLOTS = 3


def rope_tables(positions, head_dim):
    half_dim = head_dim // 2
    inv_freq = jnp.power(jnp.float32(ROPE_BASE), jnp.arange(half_dim, dtype=jnp.float32) * (-2.0 / head_dim))
    angles = positions.astype(jnp.float32)[:, None] * inv_freq[None, :]
    cos_ang, sin_ang = jnp.cos(angles), jnp.sin(angles)
    return jnp.concatenate([cos_ang, cos_ang], axis=1), jnp.concatenate([-sin_ang, sin_ang], axis=1)


def qk(keys, queries):
    return lax.dot_general(keys, queries, (((1,), (1,)), ((), ())), preferred_element_type=jnp.float32)


def fold(s, op):
    return functools.reduce(op, [s[i:i + 8] for i in range(0, s.shape[0], 8)])


def soft_step(scale2, s, vt, m, l, acc_ref):
    m_new = jnp.maximum(m, jnp.max(s, axis=0, keepdims=True))
    alpha = jnp.exp2((m - m_new) * scale2)
    e = jnp.exp2((s - m_new) * scale2)
    l_new = l * alpha + jnp.sum(e, axis=0, keepdims=True)
    pv = jnp.dot(vt, e.astype(jnp.bfloat16), preferred_element_type=jnp.float32)
    acc_ref[...] = acc_ref[...] * alpha + pv
    return m_new, l_new


def kernel(dims, xb, xa, cosf, sinf, wq, wk, wv, kcb, vcb, kca, vca, ob, oa, nkb, nvb, nka, nva,
           xs, wbuf, qsend, kvsend, rkb, rvb, rka, rva, tkb, tvb, tka, tva,
           qbuf, kc, vc, kn, vn, vtc, vtn, obuf, acc, m_all, l_all, q_a, q_all, s0, s1, s2, s3, p0, p1, p2, p3,
           qabuf, kac, vac, kan, van, vtac, vtan, oastage, ststage, oarecv, strecv, odone, acc_a,
           send_sem, recv_sem, load_sem, wsem, out_sem):
    ny, nx, kv, grp, dim = dims
    cp = ny * nx * CORES
    tb, ta = xb.shape[0], xa.shape[0]
    tq = tb // 2
    rows = grp * tq
    width = grp * dim
    pair = CORES * dim
    cb = kcb.shape[0]
    scale2 = dim ** -0.5 * LOG2E
    bf = jnp.bfloat16

    me = lax.axis_index("cp")
    c = lax.rem(me, CORES)
    x = lax.rem(me // CORES, nx)
    y = me // (CORES * nx)
    mine = y * CORES + c

    def dev(yy, xx, cc):
        return (yy * nx + xx) * CORES + cc

    def peer(h):
        return dev(h // CORES, x, lax.rem(h, CORES))

    def put(item, src, dst, target):
        pltpu.make_async_remote_copy(
            src_ref=src, dst_ref=dst, send_sem=send_sem.at[item], recv_sem=recv_sem.at[item],
            device_id={"cp": target}, device_id_type=MESH,
        ).start()

    def copy(src, dst, sem):
        pltpu.make_async_copy(src, dst, sem).start()

    def wait(ref, sem):
        pltpu.make_async_copy(ref, ref, sem).wait()

    def give(item, src, dst, target):
        @pl.when(target == me)
        def _():
            copy(src, dst, recv_sem.at[item])

        @pl.when(target != me)
        def _():
            put(item, src, dst, target)

    def wait_in(item, ref):
        wait(ref, recv_sem.at[item])

    def wait_out(item, ref):
        wait(ref, send_sem.at[item])

    KC, VC, Q, KN, VN, KAC, VAC, KAN, VAN, QA, QX, OB, OA, ST, OY = range(15)
    QS = 15
    AG = QS + ny

    barrier = pltpu.get_barrier_semaphore()

    def greet(d, _):
        pl.semaphore_signal(barrier, inc=1, device_id={"cp": d}, device_id_type=MESH)
        return 0

    raw = ((kcb, rkb, tkb), (vcb, rvb, tvb), (kca, rka, tka), (vca, rva, tva))
    for i, (src, dst, _) in enumerate(raw):
        copy(src, dst, load_sem.at[i])
    copy(xb, xs.at[pl.ds(0, tb), :], load_sem.at[4])
    copy(xa, xs.at[pl.ds(tb, ta), :], load_sem.at[4])

    q_steps, kv_steps = kv, kv // CORES

    def q_head(i):
        return lax.rem(mine + 1 + i, kv)

    def kv_pair(i):
        return lax.rem(y + 1 + i, ny)

    def load_q_cols(i, slot):
        copy(wq.at[:, pl.ds(pl.multiple_of(q_head(i) * width, width), width)], wbuf.at[slot], wsem.at[slot])

    def load_kv_cols(i, slot):
        cols = pl.ds(pl.multiple_of(kv_pair(i) * pair, pair), pair)
        copy(wk.at[:, cols], wbuf.at[slot, :, pl.ds(0, pair)], wsem.at[slot])
        copy(wv.at[:, cols], wbuf.at[slot, :, pl.ds(pair, pair)], wsem.at[slot])

    def load_cols(i):
        slot = lax.rem(i, SLOTS)

        @pl.when(i < kv_steps)
        def _():
            load_kv_cols(i, slot)

        @pl.when(jnp.logical_and(i >= kv_steps, i < kv_steps + q_steps))
        def _():
            load_q_cols(i - kv_steps, slot)

    for i in range(SLOTS - 1):
        load_cols(jnp.int32(i))
    lax.fori_loop(0, cp, greet, 0)
    for i, (_, dst, turned) in enumerate(raw):
        wait(dst, load_sem.at[i])
        turned[...] = jnp.transpose(dst[...], (1, 0, 2))
    pl.semaphore_wait(barrier, cp)

    def scatter(item, src, dst):
        def one(k, _):
            h = lax.rem(mine + k, kv)
            put(item, src.at[h], dst, peer(h))
            return 0

        lax.fori_loop(1, kv, one, 0)
        copy(src.at[mine], dst, recv_sem.at[item])

    c_rows = pl.ds(pl.multiple_of(c * cb, cb), cb)
    scatter(KC, tkb, kc.at[y, x, c_rows, :])
    scatter(VC, tvb, vc.at[y, x, c_rows, :])

    right = dev(y, lax.rem(x + 1, nx), c)
    left = dev(y, lax.rem(x + nx - 1, nx), c)
    x_left = lax.rem(x + nx - 1, nx)
    x_right = lax.rem(x + 1, nx)
    x_far = lax.rem(x + nx // 2, nx)
    lo, hi = pl.ds(0, ny // 2), pl.ds(ny // 2, ny // 2)

    def ag_sem(i, step, direction):
        return AG + i * 4 + step * 2 + direction

    def ring_first(i, buf):
        put(ag_sem(i, 0, 0), buf.at[:, x], buf.at[:, x], right)
        put(ag_sem(i, 0, 1), buf.at[:, x], buf.at[:, x], left)

    def ring_second(i, buf):
        wait_in(ag_sem(i, 0, 0), buf.at[:, x_left])
        put(ag_sem(i, 1, 0), buf.at[lo, x_left], buf.at[lo, x_left], right)
        wait_in(ag_sem(i, 0, 1), buf.at[:, x_right])
        put(ag_sem(i, 1, 1), buf.at[hi, x_right], buf.at[hi, x_right], left)

    def ring_last(i, buf):
        wait_in(ag_sem(i, 1, 0), buf.at[lo, x_far])
        wait_in(ag_sem(i, 1, 1), buf.at[hi, x_far])

    def ring_drain(i, buf):
        wait_out(ag_sem(i, 0, 0), buf.at[:, x])
        wait_out(ag_sem(i, 0, 1), buf.at[:, x])
        wait_out(ag_sem(i, 1, 0), buf.at[lo, x])
        wait_out(ag_sem(i, 1, 1), buf.at[hi, x])

    wait(xs, load_sem.at[4])
    b_rows, a_rows = pl.ds(0, tb), pl.ds(tb, ta)
    new_a = kv * ta
    col_a = pl.ds(pl.multiple_of(x * new_a, new_a), new_a)
    my_a = pl.ds(pl.multiple_of(x * new_a + mine * ta, ta), ta)

    def rope(t):
        t = t.astype(bf).astype(jnp.float32)
        return (t * cosf[...] + pltpu.roll(t, dim // 2, 1) * sinf[...]).astype(bf)

    def project(slot):
        return jnp.dot(xs[...], wbuf[slot], preferred_element_type=jnp.float32)

    def q_step(i, _):
        load_cols(kv_steps + i + SLOTS - 1)
        slot = lax.rem(kv_steps + i, SLOTS)
        wait(wbuf.at[slot], wsem.at[slot])
        h = q_head(i)
        lin = project(slot)
        for g in range(grp):
            cols = slice(g * dim, (g + 1) * dim)
            qsend[h, :, cols] = rope(lin[:, cols])
        give(QS + lax.rem(y - h // CORES + ny, ny), qsend.at[h, b_rows], qbuf.at[mine], peer(h))
        give(QA, qsend.at[h, a_rows], qabuf.at[my_a, :], peer(h))
        return 0

    def kv_step(i, _):
        load_cols(i + SLOTS - 1)
        slot = lax.rem(i, SLOTS)
        wait(wbuf.at[slot], wsem.at[slot])
        p = kv_pair(i)
        lin = project(slot)
        for g in range(CORES):
            cols = slice(g * dim, (g + 1) * dim)
            kvsend[p, :, cols] = rope(lin[:, cols])
        kvsend[p, :, pair:2 * pair] = lin[:, pair:2 * pair].astype(bf)
        for j, (nb, na) in enumerate(((nkb, nka), (nvb, nva))):
            for g in range(CORES):
                cols = pl.ds(j * pair + g * dim, dim)
                copy(kvsend.at[p, b_rows, cols], nb.at[p * CORES + g], out_sem.at[2 * j])
                copy(kvsend.at[p, a_rows, cols], na.at[p * CORES + g], out_sem.at[2 * j + 1])
        n_rows = pl.ds(pl.multiple_of(c * tb, tb), tb)
        s_rows = pl.ds(pl.multiple_of(mine * ta, ta), ta)
        for g in range(CORES):
            for j, (ib, db, ia, da) in enumerate(((KN, kn, KAN, kan), (VN, vn, VAN, van))):
                cols = pl.ds(j * pair + g * dim, dim)
                give(ib, kvsend.at[p, b_rows, cols], db.at[y, x, n_rows, :], dev(p, x, g))
                give(ia, kvsend.at[p, a_rows, cols], da.at[s_rows, :], dev(p, x, g))
        return 0

    lax.fori_loop(0, kv_steps, kv_step, 0)
    wait_in(KC, kc.at[:, x])
    ring_first(0, kc)
    wait_in(VC, vc.at[:, x])
    ring_first(1, vc)
    lax.fori_loop(0, q_steps - 1, q_step, 0)
    ring_second(0, kc)
    ring_second(1, vc)
    lax.fori_loop(q_steps - 1, q_steps, q_step, 0)
    wait_in(KN, kn.at[:, x])
    ring_first(2, kn)
    wait_in(VN, vn.at[:, x])
    ring_first(3, vn)
    scatter(KAC, tka, kac.at[mine])
    scatter(VAC, tva, vac.at[mine])

    s_refs, p_refs = (s0, s1, s2, s3), (p0, p1, p2, p3)
    blk = s0.shape[0]
    tiles = range(4)

    def scores(t, keys, queries):
        s = qk(keys, queries)
        s_refs[t][...] = s
        return fold(s, jnp.maximum)

    def highest(m, top8):
        m_new = jnp.maximum(m, jnp.max(top8, axis=0, keepdims=True))
        return m_new, jnp.exp2((m - m_new) * scale2)

    def expo(t, m, l8, top8):
        m_new, alpha = highest(m, top8)
        l8 = l8 * alpha
        for r in range(0, blk, 16):
            e = jnp.exp2((s_refs[t][pl.ds(r, 16), :] - m_new) * scale2)
            p_refs[t][pl.ds(r, 16), :] = e.astype(bf)
            l8 = l8 + fold(e, jnp.add)
        return m_new, l8, alpha

    def values(t, vt, alpha, acc_ref):
        acc_ref[...] = acc_ref[...] * alpha + jnp.dot(vt, p_refs[t][...], preferred_element_type=jnp.float32)

    def step(carry, before, now, k_after, q_after, acc_before, accs):
        m, l, top = list(carry[0:4]), list(carry[4:8]), list(carry[8:12])
        values(3, before, carry[12], acc_before)
        for t in tiles:
            m[t], l[t], alpha = expo(t, m[t], l[t], top[t])
            top[t] = scores(t, k_after, q_after(t))
            if t < 3:
                values(t, now, alpha, accs[t])
        return tuple(m + l + top) + (alpha,)

    neg, zero = jnp.full((1, rows), NEG, jnp.float32), jnp.zeros((8, rows), jnp.float32)
    one = jnp.ones((1, rows), jnp.float32)

    def total(l8):
        return jnp.sum(l8, axis=0, keepdims=True)

    def others(ref):
        return ref.at[pl.ds(0, (nx - 1) * new_a), :]

    def token_of_lane(shape):
        return lax.rem(lax.broadcasted_iota(jnp.int32, shape, 1), tq)

    def turn(n, dst, block):
        def four(i, _):
            for k in range(4):
                dst[4 * i + k] = block(4 * i + k).T
            return 0

        lax.fori_loop(0, n // 4, four, 0)

    blocks = vtc.shape[0]
    per_row = blocks // ny
    per_blk = nx // per_row
    acc[...] = jnp.zeros_like(acc)
    p3[...] = jnp.zeros_like(p3)

    def row_of(i):
        return lax.rem(y + i, ny)

    def arrive_q(i):
        yy = row_of(i)
        wait_in(QS + i, qbuf.at[pl.ds(yy * CORES, CORES)])
        for t in tiles:
            u, half = yy * CORES + t // 2, t % 2
            for g in range(grp):
                q_all[4 * yy + t, pl.ds(g * tq, tq), :] = qbuf[u, pl.ds(half * tq, tq), pl.ds(g * dim, dim)]

    def cached(buf, j):
        return buf[j // per_row, pl.ds(lax.rem(j, per_row) * per_blk, per_blk)].reshape(blk, dim)

    arrive_q(0)
    ring_last(0, kc)
    ring_last(1, vc)
    turn(blocks, vtc, lambda j: cached(vc, j))

    def step_c(i, carry):
        yy, j = row_of(i // blocks), lax.rem(i, blocks)
        before, after = lax.max(i - 1, 0), lax.min(i + 1, ny * blocks - 1)
        y_before, y_after = row_of(before // blocks), row_of(after // blocks)
        start = j == 0
        m = tuple(jnp.where(start, NEG, v) for v in carry[0:4])
        l = tuple(jnp.where(start, 0.0, v) for v in carry[4:8])
        out = step(
            m + l + carry[8:], vtc[lax.rem(before, blocks)], vtc[j], cached(kc, lax.rem(after, blocks)),
            lambda t: q_all[4 * y_after + t], acc.at[4 * y_before + 3], [acc.at[4 * yy + t] for t in tiles])
        for t in tiles:
            m_all[4 * yy + t, 0:1, :] = out[t]
            l_all[4 * yy + t] = out[4 + t]
        return out

    tops = tuple(scores(t, cached(kc, 0), q_all[4 * y + t]) for t in tiles)
    carry = (neg,) * 4 + (zero,) * 4 + tops + (one,)
    carry = lax.fori_loop(0, blocks - 1, step_c, carry)
    arrive_q(1)
    carry = lax.fori_loop(blocks - 1, 2 * blocks - 1, step_c, carry)
    wait_in(QA, qabuf.at[col_a, :])

    def pass_qa(k, _):
        put(QX, qabuf.at[col_a, :], qabuf.at[col_a, :], dev(y, lax.rem(x + k, nx), c))
        return 0

    lax.fori_loop(1, nx, pass_qa, 0)
    arrive_q(2)
    carry = lax.fori_loop(2 * blocks - 1, 3 * blocks - 1, step_c, carry)
    arrive_q(3)
    ring_second(2, kn)
    ring_second(3, vn)
    carry = lax.fori_loop(3 * blocks - 1, 4 * blocks, step_c, carry)
    values(3, vtc[blocks - 1], carry[12], acc.at[4 * row_of(ny - 1) + 3])

    ring_last(2, kn)
    ring_last(3, vn)
    turn(ny * nx, vtn, lambda j: vn[j // nx, lax.rem(j, nx)])

    def new_keys(j):
        return kn[j // nx, lax.rem(j, nx)]

    def rows_n(i, tops):
        yy, y_after = row_of(1 + i), row_of(lax.min(2 + i, ny))
        last = yy * nx + x
        accs = [acc.at[4 * yy + t] for t in tiles]
        p3[...] = jnp.zeros_like(p3)

        def step_n(j, carry):
            return step(carry, vtn[lax.max(j - 1, 0)], vtn[j], new_keys(j + 1), lambda t: q_all[4 * yy + t],
                        accs[3], accs)

        state = tuple(m_all[4 * yy + t, 0:1, :] for t in tiles) + tuple(l_all[4 * yy + t] for t in tiles)
        carry = lax.fori_loop(0, last, step_n, state + tuple(tops) + (one,))
        values(3, vtn[lax.max(last - 1, 0)], carry[12], accs[3])
        tops = []
        for t in tiles:
            seen = (t + 1) * tq
            tri = lax.broadcasted_iota(jnp.int32, (tq, rows), 0) <= token_of_lane((tq, rows))
            s = jnp.where(tri, s_refs[t][pl.ds(t * tq, tq), :], NEG)
            s_refs[t][pl.ds(t * tq, tq), :] = s
            top8 = fold(s, jnp.maximum)
            if t:
                top8 = jnp.maximum(top8, fold(s_refs[t][pl.ds(0, t * tq), :], jnp.maximum))
            m_new, alpha = highest(carry[t], top8)
            l8 = carry[4 + t] * alpha
            for r in range(0, seen, 16):
                e = jnp.exp2((s_refs[t][pl.ds(r, 16), :] - m_new) * scale2)
                p_refs[t][pl.ds(r, 16), :] = e.astype(bf)
                l8 = l8 + fold(e, jnp.add)
            tops.append(scores(t, new_keys(0), q_all[4 * y_after + t]))
            pv = jnp.dot(vtn[last, :, pl.ds(0, seen)], p_refs[t][pl.ds(0, seen), :], preferred_element_type=jnp.float32)
            o = (accs[t][...] * alpha + pv) * (1.0 / total(l8))
            for g in range(grp):
                obuf[yy * CORES + t // 2, pl.ds(t % 2 * tq, tq), pl.ds(g * dim, dim)] = (
                    o[:, g * tq:(g + 1) * tq].T.astype(bf))
        for cc in range(CORES):
            u = yy * CORES + cc
            give(OB, obuf.at[u], ob.at[:, pl.ds(pl.multiple_of(mine * width, width), width)], peer(u))
        return tuple(tops)

    tops = tuple(scores(t, new_keys(0), q_all[4 * row_of(1) + t]) for t in tiles)
    tops = lax.fori_loop(0, 1, rows_n, tops)

    wait_in(QX, others(qabuf))
    wait_in(KAC, kac)
    wait_in(VAC, vac)
    wait_in(KAN, kan)
    wait_in(VAN, van)
    turn(kv, vtac, lambda j: vac[j])
    vtan[...] = van[...].T
    for t in tiles:
        for g in range(grp):
            q_a[t, pl.ds(g * tq, tq), :] = qabuf[pl.ds(t * tq, tq), pl.ds(g * dim, dim)]
    acc_a[...] = jnp.zeros_like(acc_a)
    p3[...] = jnp.zeros_like(p3)
    accs_a = [acc_a.at[t] for t in tiles]

    def step_a(j, carry):
        return step(carry, vtac[lax.max(j - 1, 0)], vtac[j], kac[j + 1], lambda t: q_a[t], accs_a[3], accs_a)

    tops = tuple(scores(t, kac[0], q_a[t]) for t in tiles)
    carry = lax.fori_loop(0, kv - 1, step_a, (neg,) * 4 + (zero,) * 4 + tops + (one,))
    values(3, vtac[kv - 2], carry[12], accs_a[3])

    def token_a(r, xx):
        holder = dev(r // (CORES * ta), xx, lax.rem(r // ta, CORES))
        return holder * ta + lax.rem(r, ta)

    pos_k = token_a(lax.broadcasted_iota(jnp.int32, (new_a, rows), 0), x)
    place_q = token_of_lane((new_a, rows))
    row = lax.broadcasted_iota(jnp.int32, (dim, tq), 0)
    for t in tiles:
        m, l, alpha = expo(t, carry[t], carry[4 + t], carry[8 + t])
        values(t, vtac[kv - 1], alpha, accs_a[t])
        s = jnp.where(pos_k <= token_a(place_q, t), qk(kan[...], q_a[t]), NEG)
        m, l = soft_step(scale2, s, vtan[...], m, total(l), accs_a[t])
        stat = jnp.zeros((dim, tq), jnp.float32)
        for g in range(grp):
            cols = slice(g * tq, (g + 1) * tq)
            oastage[pl.ds(t * tq, tq), pl.ds(g * dim, dim)] = acc_a[t, :, cols].T
            stat = jnp.where(row == g, m[:, cols], stat)
            stat = jnp.where(row == grp + g, l[:, cols], stat)
        ststage[pl.ds(t * tq, tq), :] = stat.T

    def give_a(k, _):
        xx = lax.rem(x + k, nx)
        r = pl.ds(pl.multiple_of(xx * new_a, new_a), new_a)
        put(OA, oastage.at[r, :], oarecv.at[x], dev(y, xx, c))
        put(ST, ststage.at[r, :], strecv.at[x], dev(y, xx, c))
        return 0

    lax.fori_loop(1, nx, give_a, 0)
    copy(oastage.at[col_a, :], oarecv.at[x], recv_sem.at[OA])
    copy(ststage.at[col_a, :], strecv.at[x], recv_sem.at[ST])

    tops = tuple(scores(t, new_keys(0), q_all[4 * row_of(2) + t]) for t in tiles)
    tops = lax.fori_loop(1, ny - 1, rows_n, tops)

    wait_in(OA, oarecv)
    wait_in(ST, strecv)
    for g in range(grp):
        cols = pl.ds(g * dim, dim)
        ms = [strecv[i, :, g:g + 1] for i in range(nx)]
        top = functools.reduce(jnp.maximum, ms)
        num = jnp.zeros((new_a, dim), jnp.float32)
        den = jnp.zeros((new_a, 1), jnp.float32)
        for i in range(nx):
            w = jnp.exp2((ms[i] - top) * scale2)
            num = num + w * oarecv[i, :, cols]
            den = den + w * strecv[i, :, grp + g:grp + g + 1]
        odone[:, cols] = (num / den).astype(bf)

    def home_a(r, _):
        give(OY, odone.at[pl.ds(pl.multiple_of(r * ta, ta), ta), :],
             oa.at[:, pl.ds(pl.multiple_of(mine * width, width), width)], peer(r))
        return 0

    lax.fori_loop(0, kv, home_a, 0)
    lax.fori_loop(ny - 1, ny, rows_n, tops)

    wait_in(OB, ob)
    wait_in(OY, oa)
    for i, ref in enumerate((nkb, nka, nvb, nva)):
        wait(ref, out_sem.at[i])
    most = pl.ds(0, kv - 1)
    for item, ref in ((KC, tkb), (VC, tvb), (KAC, tka), (VAC, tva), (OB, obuf)):
        wait_out(item, ref.at[most])
    wait_out(QS, qbuf.at[pl.ds(0, CORES - 1)])
    for i in range(1, ny):
        wait_out(QS + i, qbuf.at[pl.ds(0, CORES)])
    for item, ref in ((KN, qbuf), (VN, qbuf)):
        wait_out(item, ref.at[most, :, pl.ds(0, dim)])
    for item, ref in ((KAN, kan), (VAN, van)):
        wait_out(item, ref.at[pl.ds(0, (kv - 1) * ta), :])
    wait_out(QA, qabuf.at[pl.ds(0, (kv - 1) * ta), :])
    wait_out(OY, odone.at[pl.ds(0, (kv - 1) * ta), :])
    wait_out(QX, others(qabuf))
    wait_out(OA, oarecv.at[pl.ds(0, nx - 1)])
    wait_out(ST, strecv.at[pl.ds(0, nx - 1)])
    ring_drain(0, kc)
    ring_drain(1, vc)
    ring_drain(2, kn)
    ring_drain(3, vn)


def attention(cp, xb, xa, cosf, sinf, wq, wk, wv, kcb, vcb, kca, vca):
    kv, dim = kcb.shape[1:]
    ny, nx = kv // CORES, cp // kv
    assert nx * CORES == kv and ny * nx * CORES == cp and ny == nx
    grp = wq.shape[1] // (kv * dim)
    tb, ta, cb, ca, model = xb.shape[0], xa.shape[0], kcb.shape[0], kca.shape[0], xb.shape[1]
    tq = tb // 2
    rows, width = grp * tq, grp * dim
    blk = CORES * tb
    assert blk == ca and (ny * nx * CORES * cb) % (ny * blk) == 0 and (cp * ta) % (2 * tq) == 0
    assert width == 2 * CORES * dim and kv * ta == tq and nx == 4 and CORES == 2
    bf, f32 = jnp.bfloat16, jnp.float32
    vm = pltpu.VMEM
    scratch = [
        vm((tb + ta, model), bf),
        vm((SLOTS, model, width), bf),
        vm((kv, tb + ta, width), bf),
        vm((ny, tb + ta, width), bf),
        vm(kcb.shape, bf), vm(vcb.shape, bf), vm(kca.shape, bf), vm(vca.shape, bf),
        vm((kv, cb, dim), bf), vm((kv, cb, dim), bf), vm((kv, ca, dim), bf), vm((kv, ca, dim), bf),
        vm((kv, tb, width), bf),
        vm((ny, nx, CORES * cb, dim), bf),
        vm((ny, nx, CORES * cb, dim), bf),
        vm((ny, nx, blk, dim), bf),
        vm((ny, nx, blk, dim), bf),
        vm((cp * cb // blk, dim, blk), bf),
        vm((ny * nx, dim, blk), bf),
        vm((kv, tb, width), bf),
        vm((2 * kv, dim, rows), f32),
        vm((2 * kv, 8, rows), f32),
        vm((2 * kv, 8, rows), f32),
        vm((4, rows, dim), bf),
        vm((2 * kv, rows, dim), bf),
        vm((blk, rows), f32), vm((blk, rows), f32), vm((blk, rows), f32), vm((blk, rows), f32),
        vm((blk, rows), bf), vm((blk, rows), bf), vm((blk, rows), bf), vm((blk, rows), bf),
        vm((cp * ta, width), bf),
        vm((kv, ca, dim), bf),
        vm((kv, ca, dim), bf),
        vm((kv * ta, dim), bf),
        vm((kv * ta, dim), bf),
        vm((kv, dim, ca), bf),
        vm((dim, kv * ta), bf),
        vm((cp * ta, width), f32),
        vm((cp * ta, dim), f32),
        vm((nx, kv * ta, width), f32),
        vm((nx, kv * ta, dim), f32),
        vm((kv * ta, width), bf),
        vm((4, dim, rows), f32),
        pltpu.SemaphoreType.DMA((15 + ny + 16,)),
        pltpu.SemaphoreType.DMA((15 + ny + 16,)),
        pltpu.SemaphoreType.DMA((5,)),
        pltpu.SemaphoreType.DMA((SLOTS,)),
        pltpu.SemaphoreType.DMA((4,)),
    ]
    any_spec = pl.BlockSpec(memory_space=pl.ANY)
    vmem_spec = pl.BlockSpec(memory_space=pltpu.VMEM)
    shape = jax.ShapeDtypeStruct
    return pl.pallas_call(
        functools.partial(kernel, (ny, nx, kv, grp, dim)),
        out_shape=(shape((tb, kv * width), bf), shape((ta, kv * width), bf),
                   shape((kv, tb, dim), bf), shape((kv, tb, dim), bf),
                   shape((kv, ta, dim), bf), shape((kv, ta, dim), bf)),
        in_specs=[any_spec, any_spec, vmem_spec, vmem_spec] + [any_spec] * 7,
        out_specs=(any_spec,) * 6,
        scratch_shapes=scratch,
        compiler_params=pltpu.CompilerParams(
            collective_id=0, has_side_effects=True, vmem_limit_bytes=VMEM_LIMIT),
        name="attend",
    )(xb, xa, cosf, sinf, wq, wk, wv, kcb, vcb, kca, vca)


def out_kernel(ob, oa, w, kb, vb, ka, va, yb, ya, nkb, nvb, nka, nva, o, wbuf, ybuf, *rest):
    new, turned, (wsem, osem, nsem, ysem) = rest[:4], rest[4:8], rest[8:]
    tb, ta = ob.shape[0], oa.shape[0]
    cols = wbuf.shape[2]
    steps = w.shape[1] // cols
    b_rows, a_rows = pl.ds(0, tb), pl.ds(tb, ta)

    def copy(src, dst, sem):
        pltpu.make_async_copy(src, dst, sem).start()

    def wait(ref, sem):
        pltpu.make_async_copy(ref, ref, sem).wait()

    def span(i):
        return pl.ds(pl.multiple_of(i * cols, cols), cols)

    def load(i):
        copy(w.at[:, span(i)], wbuf.at[lax.rem(i, SLOTS)], wsem.at[lax.rem(i, SLOTS)])

    copy(ob, o.at[b_rows, :], osem)
    copy(oa, o.at[a_rows, :], osem)
    for i in range(min(SLOTS - 1, steps)):
        load(i)
    for i, (src, dst) in enumerate(zip((kb, vb, ka, va), new)):
        copy(src, dst, nsem.at[i])
    wait(o, osem)

    def step(i, _):
        @pl.when(i + SLOTS - 1 < steps)
        def _():
            load(i + SLOTS - 1)

        slot = lax.rem(i, SLOTS)
        wait(wbuf.at[slot], wsem.at[slot])
        ybuf[i] = jnp.dot(o[...], wbuf[slot], preferred_element_type=jnp.float32).astype(ybuf.dtype)
        copy(ybuf.at[i, b_rows, :], yb.at[:, span(i)], ysem.at[0])
        copy(ybuf.at[i, a_rows, :], ya.at[:, span(i)], ysem.at[1])
        return 0

    lax.fori_loop(0, steps, step, 0)
    for i, (src, dst, out) in enumerate(zip(new, turned, (nkb, nvb, nka, nva))):
        wait(src, nsem.at[i])
        dst[...] = jnp.transpose(src[...], (1, 0, 2))
        copy(dst, out, nsem.at[i])
    wait(yb, ysem.at[0])
    wait(ya, ysem.at[1])
    for i, out in enumerate((nkb, nvb, nka, nva)):
        wait(out, nsem.at[i])


def output_projection(ob, oa, w, *new):
    (tb, inner), ta, model = ob.shape, oa.shape[0], w.shape[1]
    cols = min(512, model)
    shape = jax.ShapeDtypeStruct
    bf, vm, dma = ob.dtype, pltpu.VMEM, pltpu.SemaphoreType.DMA
    turned = [(t.shape[1], t.shape[0], t.shape[2]) for t in new]
    any_spec = pl.BlockSpec(memory_space=pl.ANY)
    return pl.pallas_call(
        out_kernel,
        out_shape=[shape((tb, model), bf), shape((ta, model), bf)] + [shape(t, bf) for t in turned],
        in_specs=[any_spec] * 7,
        out_specs=[any_spec] * 6,
        scratch_shapes=[vm((tb + ta, inner), bf), vm((SLOTS, inner, cols), bf), vm((model // cols, tb + ta, cols), bf)]
        + [vm(t.shape, bf) for t in new] + [vm(t, bf) for t in turned] + [dma((SLOTS,)), dma, dma((4,)), dma((2,))],
        compiler_params=pltpu.CompilerParams(vmem_limit_bytes=VMEM_LIMIT),
        name="project_out",
    )(ob, oa, w, *new)


def solution(mesh):
    cp_size = mesh.shape["cp"]

    def local_step(x_a, kc_a, vc_a, x_b, kc_b, vc_b, w_q, w_k, w_v, w_o):
        ta, tb = x_a.shape[0], x_b.shape[0]
        kv, dim = kc_a.shape[1:]
        me = lax.axis_index("cp")
        pos_a = kc_a.shape[0] * cp_size + me * ta + jnp.arange(ta)
        pos_b = kc_b.shape[0] * cp_size + me * tb + jnp.arange(tb)
        cosf, sinf = rope_tables(jnp.concatenate([pos_b, pos_a]), dim)
        o_b, o_a, k_b, v_b, k_a, v_a = attention(cp_size, x_b, x_a, cosf, sinf, w_q, w_k, w_v, kc_b, vc_b, kc_a, vc_a)
        y_b, y_a, k_b, v_b, k_a, v_a = output_projection(o_b, o_a, w_o, k_b, v_b, k_a, v_a)
        return y_a, k_a, v_a, y_b, k_b, v_b

    row_spec = P(("dp", "cp"), None)
    kv_spec = P(("dp", "cp"), None, None)
    full_spec = P()
    return jax.shard_map(
        local_step, mesh=mesh,
        in_specs=(row_spec, kv_spec, kv_spec, row_spec, kv_spec, kv_spec, full_spec, full_spec, full_spec, full_spec),
        out_specs=(row_spec, kv_spec, kv_spec, row_spec, kv_spec, kv_spec), check_vma=False)
```

```python
import functools

import jax
import jax.numpy as jnp
from jax import lax
from jax.experimental import pallas as pl
from jax.experimental.pallas import tpu as pltpu
from jax.sharding import PartitionSpec as P

ROPE_BASE = 500000
LOG2E = 1.4426950408889634
NEG = float(jnp.finfo(jnp.float32).min)
MESH = pl.DeviceIdType.MESH
CORES = 2
VMEM_LIMIT = 62 * 1024 * 1024
SLOTS = 3


def rope_tables(positions, head_dim):
    half_dim = head_dim // 2
    inv_freq = jnp.power(jnp.float32(ROPE_BASE), jnp.arange(half_dim, dtype=jnp.float32) * (-2.0 / head_dim))
    angles = positions.astype(jnp.float32)[:, None] * inv_freq[None, :]
    cos_ang, sin_ang = jnp.cos(angles), jnp.sin(angles)
    return jnp.concatenate([cos_ang, cos_ang], axis=1), jnp.concatenate([-sin_ang, sin_ang], axis=1)


def qk(keys, queries):
    return lax.dot_general(keys, queries, (((1,), (1,)), ((), ())), preferred_element_type=jnp.float32)


def fold(s, op):
    return functools.reduce(op, [s[i:i + 8] for i in range(0, s.shape[0], 8)])


def soft_step(scale2, s, vt, m, l, acc_ref):
    m_new = jnp.maximum(m, jnp.max(s, axis=0, keepdims=True))
    alpha = jnp.exp2((m - m_new) * scale2)
    e = jnp.exp2((s - m_new) * scale2)
    l_new = l * alpha + jnp.sum(e, axis=0, keepdims=True)
    pv = jnp.dot(vt, e.astype(jnp.bfloat16), preferred_element_type=jnp.float32)
    acc_ref[...] = acc_ref[...] * alpha + pv
    return m_new, l_new


def kernel(dims, xb, xa, cosf, sinf, wq, wk, wv, kcb, vcb, kca, vca, ob, oa, nkb, nvb, nka, nva,
           xs, wbuf, qsend, kvsend, rkb, rvb, rka, rva, tkb, tvb, tka, tva,
           qbuf, kc, vc, kn, vn, vtc, vtn, obuf, acc, m_all, l_all, q_a, q_all, s0, s1, s2, s3, p0, p1, p2, p3,
           qabuf, kac, vac, kan, van, vtac, vtan, oastage, ststage, oarecv, strecv, odone, acc_a,
           send_sem, recv_sem, load_sem, wsem, out_sem):
    ny, nx, kv, grp, dim = dims
    cp = ny * nx * CORES
    tb, ta = xb.shape[0], xa.shape[0]
    tq = tb // 2
    rows = grp * tq
    width = grp * dim
    pair = CORES * dim
    cb = kcb.shape[0]
    scale2 = dim ** -0.5 * LOG2E
    bf = jnp.bfloat16

    me = lax.axis_index("cp")
    c = lax.rem(me, CORES)
    x = lax.rem(me // CORES, nx)
    y = me // (CORES * nx)
    mine = y * CORES + c

    def dev(yy, xx, cc):
        return (yy * nx + xx) * CORES + cc

    def peer(h):
        return dev(h // CORES, x, lax.rem(h, CORES))

    def put(item, src, dst, target):
        pltpu.make_async_remote_copy(
            src_ref=src, dst_ref=dst, send_sem=send_sem.at[item], recv_sem=recv_sem.at[item],
            device_id={"cp": target}, device_id_type=MESH,
        ).start()

    def copy(src, dst, sem):
        pltpu.make_async_copy(src, dst, sem).start()

    def wait(ref, sem):
        pltpu.make_async_copy(ref, ref, sem).wait()

    def give(item, src, dst, target):
        @pl.when(target == me)
        def _():
            copy(src, dst, recv_sem.at[item])

        @pl.when(target != me)
        def _():
            put(item, src, dst, target)

    def wait_in(item, ref):
        wait(ref, recv_sem.at[item])

    def wait_out(item, ref):
        wait(ref, send_sem.at[item])

    KC, VC, Q, KN, VN, KAC, VAC, KAN, VAN, QA, QX, OB, OA, ST, OY = range(15)
    QS = 15
    AG = QS + ny

    barrier = pltpu.get_barrier_semaphore()

    def greet(d, _):
        pl.semaphore_signal(barrier, inc=1, device_id={"cp": d}, device_id_type=MESH)
        return 0

    raw = ((kcb, rkb, tkb), (vcb, rvb, tvb), (kca, rka, tka), (vca, rva, tva))
    for i, (src, dst, _) in enumerate(raw):
        copy(src, dst, load_sem.at[i])
    copy(xb, xs.at[pl.ds(0, tb), :], load_sem.at[4])
    copy(xa, xs.at[pl.ds(tb, ta), :], load_sem.at[4])

    q_steps, kv_steps = kv, kv // CORES

    def q_head(i):
        return lax.rem(mine + 1 + i, kv)

    def kv_pair(i):
        return lax.rem(y + 1 + i, ny)

    def load_q_cols(i, slot):
        copy(wq.at[:, pl.ds(pl.multiple_of(q_head(i) * width, width), width)], wbuf.at[slot], wsem.at[slot])

    def load_kv_cols(i, slot):
        cols = pl.ds(pl.multiple_of(kv_pair(i) * pair, pair), pair)
        copy(wk.at[:, cols], wbuf.at[slot, :, pl.ds(0, pair)], wsem.at[slot])
        copy(wv.at[:, cols], wbuf.at[slot, :, pl.ds(pair, pair)], wsem.at[slot])

    def load_cols(i):
        slot = lax.rem(i, SLOTS)

        @pl.when(i < kv_steps)
        def _():
            load_kv_cols(i, slot)

        @pl.when(jnp.logical_and(i >= kv_steps, i < kv_steps + q_steps))
        def _():
            load_q_cols(i - kv_steps, slot)

    for i in range(SLOTS - 1):
        load_cols(jnp.int32(i))
    lax.fori_loop(0, cp, greet, 0)
    for i, (_, dst, turned) in enumerate(raw):
        wait(dst, load_sem.at[i])
        turned[...] = jnp.transpose(dst[...], (1, 0, 2))
    pl.semaphore_wait(barrier, cp)

    def scatter(item, src, dst):
        def one(k, _):
            h = lax.rem(mine + k, kv)
            put(item, src.at[h], dst, peer(h))
            return 0

        lax.fori_loop(1, kv, one, 0)
        copy(src.at[mine], dst, recv_sem.at[item])

    c_rows = pl.ds(pl.multiple_of(c * cb, cb), cb)
    scatter(KC, tkb, kc.at[y, x, c_rows, :])
    scatter(VC, tvb, vc.at[y, x, c_rows, :])

    right = dev(y, lax.rem(x + 1, nx), c)
    left = dev(y, lax.rem(x + nx - 1, nx), c)
    x_left = lax.rem(x + nx - 1, nx)
    x_right = lax.rem(x + 1, nx)
    x_far = lax.rem(x + nx // 2, nx)
    lo, hi = pl.ds(0, ny // 2), pl.ds(ny // 2, ny // 2)

    def ag_sem(i, step, direction):
        return AG + i * 4 + step * 2 + direction

    def ring_first(i, buf):
        put(ag_sem(i, 0, 0), buf.at[:, x], buf.at[:, x], right)
        put(ag_sem(i, 0, 1), buf.at[:, x], buf.at[:, x], left)

    def ring_second(i, buf):
        wait_in(ag_sem(i, 0, 0), buf.at[:, x_left])
        put(ag_sem(i, 1, 0), buf.at[lo, x_left], buf.at[lo, x_left], right)
        wait_in(ag_sem(i, 0, 1), buf.at[:, x_right])
        put(ag_sem(i, 1, 1), buf.at[hi, x_right], buf.at[hi, x_right], left)

    def ring_last(i, buf):
        wait_in(ag_sem(i, 1, 0), buf.at[lo, x_far])
        wait_in(ag_sem(i, 1, 1), buf.at[hi, x_far])

    def ring_drain(i, buf):
        wait_out(ag_sem(i, 0, 0), buf.at[:, x])
        wait_out(ag_sem(i, 0, 1), buf.at[:, x])
        wait_out(ag_sem(i, 1, 0), buf.at[lo, x])
        wait_out(ag_sem(i, 1, 1), buf.at[hi, x])

    wait(xs, load_sem.at[4])
    b_rows, a_rows = pl.ds(0, tb), pl.ds(tb, ta)
    new_a = kv * ta
    col_a = pl.ds(pl.multiple_of(x * new_a, new_a), new_a)
    my_a = pl.ds(pl.multiple_of(x * new_a + mine * ta, ta), ta)

    def rope(t):
        t = t.astype(bf).astype(jnp.float32)
        return (t * cosf[...] + pltpu.roll(t, dim // 2, 1) * sinf[...]).astype(bf)

    def project(slot):
        return jnp.dot(xs[...], wbuf[slot], preferred_element_type=jnp.float32)

    def q_step(i, _):
        load_cols(kv_steps + i + SLOTS - 1)
        slot = lax.rem(kv_steps + i, SLOTS)
        wait(wbuf.at[slot], wsem.at[slot])
        h = q_head(i)
        lin = project(slot)
        for g in range(grp):
            cols = slice(g * dim, (g + 1) * dim)
            qsend[h, :, cols] = rope(lin[:, cols])
        give(QS + lax.rem(y - h // CORES + ny, ny), qsend.at[h, b_rows], qbuf.at[mine], peer(h))
        give(QA, qsend.at[h, a_rows], qabuf.at[my_a, :], peer(h))
        return 0

    def kv_step(i, _):
        load_cols(i + SLOTS - 1)
        slot = lax.rem(i, SLOTS)
        wait(wbuf.at[slot], wsem.at[slot])
        p = kv_pair(i)
        lin = project(slot)
        for g in range(CORES):
            cols = slice(g * dim, (g + 1) * dim)
            kvsend[p, :, cols] = rope(lin[:, cols])
        kvsend[p, :, pair:2 * pair] = lin[:, pair:2 * pair].astype(bf)
        for j, (nb, na) in enumerate(((nkb, nka), (nvb, nva))):
            for g in range(CORES):
                cols = pl.ds(j * pair + g * dim, dim)
                copy(kvsend.at[p, b_rows, cols], nb.at[p * CORES + g], out_sem.at[2 * j])
                copy(kvsend.at[p, a_rows, cols], na.at[p * CORES + g], out_sem.at[2 * j + 1])
        n_rows = pl.ds(pl.multiple_of(c * tb, tb), tb)
        s_rows = pl.ds(pl.multiple_of(mine * ta, ta), ta)
        for g in range(CORES):
            for j, (ib, db, ia, da) in enumerate(((KN, kn, KAN, kan), (VN, vn, VAN, van))):
                cols = pl.ds(j * pair + g * dim, dim)
                give(ib, kvsend.at[p, b_rows, cols], db.at[y, x, n_rows, :], dev(p, x, g))
                give(ia, kvsend.at[p, a_rows, cols], da.at[s_rows, :], dev(p, x, g))
        return 0

    lax.fori_loop(0, kv_steps, kv_step, 0)
    wait_in(KC, kc.at[:, x])
    ring_first(0, kc)
    wait_in(VC, vc.at[:, x])
    ring_first(1, vc)
    lax.fori_loop(0, q_steps - 1, q_step, 0)
    ring_second(0, kc)
    ring_second(1, vc)
    lax.fori_loop(q_steps - 1, q_steps, q_step, 0)
    wait_in(KN, kn.at[:, x])
    ring_first(2, kn)
    wait_in(VN, vn.at[:, x])
    ring_first(3, vn)
    scatter(KAC, tka, kac.at[mine])
    scatter(VAC, tva, vac.at[mine])

    s_refs, p_refs = (s0, s1, s2, s3), (p0, p1, p2, p3)
    blk = s0.shape[0]
    tiles = range(4)

    def scores(t, keys, queries):
        s = qk(keys, queries)
        s_refs[t][...] = s
        return fold(s, jnp.maximum)

    def highest(m, top8):
        m_new = jnp.maximum(m, jnp.max(top8, axis=0, keepdims=True))
        return m_new, jnp.exp2((m - m_new) * scale2)

    def expo(t, m, l8, top8):
        m_new, alpha = highest(m, top8)
        l8 = l8 * alpha
        for r in range(0, blk, 16):
            e = jnp.exp2((s_refs[t][pl.ds(r, 16), :] - m_new) * scale2)
            p_refs[t][pl.ds(r, 16), :] = e.astype(bf)
            l8 = l8 + fold(e, jnp.add)
        return m_new, l8, alpha

    def values(t, vt, alpha, acc_ref):
        acc_ref[...] = acc_ref[...] * alpha + jnp.dot(vt, p_refs[t][...], preferred_element_type=jnp.float32)

    def step(carry, before, now, k_after, q_after, acc_before, accs):
        m, l, top = list(carry[0:4]), list(carry[4:8]), list(carry[8:12])
        values(3, before, carry[12], acc_before)
        for t in tiles:
            m[t], l[t], alpha = expo(t, m[t], l[t], top[t])
            top[t] = scores(t, k_after, q_after(t))
            if t < 3:
                values(t, now, alpha, accs[t])
        return tuple(m + l + top) + (alpha,)

    neg, zero = jnp.full((1, rows), NEG, jnp.float32), jnp.zeros((8, rows), jnp.float32)
    one = jnp.ones((1, rows), jnp.float32)

    def total(l8):
        return jnp.sum(l8, axis=0, keepdims=True)

    def others(ref):
        return ref.at[pl.ds(0, (nx - 1) * new_a), :]

    def token_of_lane(shape):
        return lax.rem(lax.broadcasted_iota(jnp.int32, shape, 1), tq)

    def turn(n, dst, block):
        def four(i, _):
            for k in range(4):
                dst[4 * i + k] = block(4 * i + k).T
            return 0

        lax.fori_loop(0, n // 4, four, 0)

    blocks = vtc.shape[0]
    per_row = blocks // ny
    per_blk = nx // per_row
    acc[...] = jnp.zeros_like(acc)
    p3[...] = jnp.zeros_like(p3)

    def row_of(i):
        return lax.rem(y + ny - i, ny)

    def arrive_q(i):
        yy = row_of(i)
        wait_in(QS + (ny - i) % ny, qbuf.at[pl.ds(yy * CORES, CORES)])
        for t in tiles:
            u, half = yy * CORES + t // 2, t % 2
            for g in range(grp):
                q_all[4 * yy + t, pl.ds(g * tq, tq), :] = qbuf[u, pl.ds(half * tq, tq), pl.ds(g * dim, dim)]

    def cached(buf, j):
        return buf[j // per_row, pl.ds(lax.rem(j, per_row) * per_blk, per_blk)].reshape(blk, dim)

    arrive_q(0)
    ring_last(0, kc)
    ring_last(1, vc)
    turn(blocks, vtc, lambda j: cached(vc, j))

    def step_c(i, carry):
        yy, j = row_of(i // blocks), lax.rem(i, blocks)
        before, after = lax.max(i - 1, 0), lax.min(i + 1, ny * blocks - 1)
        y_before, y_after = row_of(before // blocks), row_of(after // blocks)
        start = j == 0
        m = tuple(jnp.where(start, NEG, v) for v in carry[0:4])
        l = tuple(jnp.where(start, 0.0, v) for v in carry[4:8])
        out = step(
            m + l + carry[8:], vtc[lax.rem(before, blocks)], vtc[j], cached(kc, lax.rem(after, blocks)),
            lambda t: q_all[4 * y_after + t], acc.at[4 * y_before + 3], [acc.at[4 * yy + t] for t in tiles])
        for t in tiles:
            m_all[4 * yy + t, 0:1, :] = out[t]
            l_all[4 * yy + t] = out[4 + t]
        return out

    tops = tuple(scores(t, cached(kc, 0), q_all[4 * y + t]) for t in tiles)
    carry = (neg,) * 4 + (zero,) * 4 + tops + (one,)
    carry = lax.fori_loop(0, blocks - 1, step_c, carry)
    arrive_q(1)
    carry = lax.fori_loop(blocks - 1, 2 * blocks - 1, step_c, carry)
    wait_in(QA, qabuf.at[col_a, :])

    def pass_qa(k, _):
        put(QX, qabuf.at[col_a, :], qabuf.at[col_a, :], dev(y, lax.rem(x + k, nx), c))
        return 0

    lax.fori_loop(1, nx, pass_qa, 0)
    arrive_q(2)
    carry = lax.fori_loop(2 * blocks - 1, 3 * blocks - 1, step_c, carry)
    arrive_q(3)
    ring_second(2, kn)
    ring_second(3, vn)
    carry = lax.fori_loop(3 * blocks - 1, 4 * blocks, step_c, carry)
    values(3, vtc[blocks - 1], carry[12], acc.at[4 * row_of(ny - 1) + 3])

    ring_last(2, kn)
    ring_last(3, vn)
    turn(ny * nx, vtn, lambda j: vn[j // nx, lax.rem(j, nx)])

    def new_keys(j):
        return kn[j // nx, lax.rem(j, nx)]

    def row_n(i):
        return lax.rem(y + ny + jnp.where(c == 0, 1 + i, ny - 1 - i), ny)

    def rows_n(i, tops):
        yy, y_after = row_n(i), row_n(lax.min(i + 1, ny - 1))
        last = yy * nx + x
        accs = [acc.at[4 * yy + t] for t in tiles]
        p3[...] = jnp.zeros_like(p3)

        def step_n(j, carry):
            return step(carry, vtn[lax.max(j - 1, 0)], vtn[j], new_keys(j + 1), lambda t: q_all[4 * yy + t],
                        accs[3], accs)

        state = tuple(m_all[4 * yy + t, 0:1, :] for t in tiles) + tuple(l_all[4 * yy + t] for t in tiles)
        carry = lax.fori_loop(0, last, step_n, state + tuple(tops) + (one,))
        values(3, vtn[lax.max(last - 1, 0)], carry[12], accs[3])
        tops = []
        for t in tiles:
            seen = (t + 1) * tq
            tri = lax.broadcasted_iota(jnp.int32, (tq, rows), 0) <= token_of_lane((tq, rows))
            s = jnp.where(tri, s_refs[t][pl.ds(t * tq, tq), :], NEG)
            s_refs[t][pl.ds(t * tq, tq), :] = s
            top8 = fold(s, jnp.maximum)
            if t:
                top8 = jnp.maximum(top8, fold(s_refs[t][pl.ds(0, t * tq), :], jnp.maximum))
            m_new, alpha = highest(carry[t], top8)
            l8 = carry[4 + t] * alpha
            for r in range(0, seen, 16):
                e = jnp.exp2((s_refs[t][pl.ds(r, 16), :] - m_new) * scale2)
                p_refs[t][pl.ds(r, 16), :] = e.astype(bf)
                l8 = l8 + fold(e, jnp.add)
            tops.append(scores(t, new_keys(0), q_all[4 * y_after + t]))
            pv = jnp.dot(vtn[last, :, pl.ds(0, seen)], p_refs[t][pl.ds(0, seen), :], preferred_element_type=jnp.float32)
            o = (accs[t][...] * alpha + pv) * (1.0 / total(l8))
            for g in range(grp):
                obuf[yy * CORES + t // 2, pl.ds(t % 2 * tq, tq), pl.ds(g * dim, dim)] = (
                    o[:, g * tq:(g + 1) * tq].T.astype(bf))
        for cc in range(CORES):
            u = yy * CORES + cc
            give(OB, obuf.at[u], ob.at[:, pl.ds(pl.multiple_of(mine * width, width), width)], peer(u))
        return tuple(tops)

    tops = tuple(scores(t, new_keys(0), q_all[4 * row_n(0) + t]) for t in tiles)
    tops = lax.fori_loop(0, 1, rows_n, tops)

    wait_in(QX, others(qabuf))
    wait_in(KAC, kac)
    wait_in(VAC, vac)
    wait_in(KAN, kan)
    wait_in(VAN, van)
    turn(kv, vtac, lambda j: vac[j])
    vtan[...] = van[...].T
    for t in tiles:
        for g in range(grp):
            q_a[t, pl.ds(g * tq, tq), :] = qabuf[pl.ds(t * tq, tq), pl.ds(g * dim, dim)]
    acc_a[...] = jnp.zeros_like(acc_a)
    p3[...] = jnp.zeros_like(p3)
    accs_a = [acc_a.at[t] for t in tiles]

    def step_a(j, carry):
        return step(carry, vtac[lax.max(j - 1, 0)], vtac[j], kac[j + 1], lambda t: q_a[t], accs_a[3], accs_a)

    tops = tuple(scores(t, kac[0], q_a[t]) for t in tiles)
    carry = lax.fori_loop(0, kv - 1, step_a, (neg,) * 4 + (zero,) * 4 + tops + (one,))
    values(3, vtac[kv - 2], carry[12], accs_a[3])

    def token_a(r, xx):
        holder = dev(r // (CORES * ta), xx, lax.rem(r // ta, CORES))
        return holder * ta + lax.rem(r, ta)

    pos_k = token_a(lax.broadcasted_iota(jnp.int32, (new_a, rows), 0), x)
    place_q = token_of_lane((new_a, rows))
    row = lax.broadcasted_iota(jnp.int32, (dim, tq), 0)
    for t in tiles:
        m, l, alpha = expo(t, carry[t], carry[4 + t], carry[8 + t])
        values(t, vtac[kv - 1], alpha, accs_a[t])
        s = jnp.where(pos_k <= token_a(place_q, t), qk(kan[...], q_a[t]), NEG)
        m, l = soft_step(scale2, s, vtan[...], m, total(l), accs_a[t])
        stat = jnp.zeros((dim, tq), jnp.float32)
        for g in range(grp):
            cols = slice(g * tq, (g + 1) * tq)
            oastage[pl.ds(t * tq, tq), pl.ds(g * dim, dim)] = acc_a[t, :, cols].T
            stat = jnp.where(row == g, m[:, cols], stat)
            stat = jnp.where(row == grp + g, l[:, cols], stat)
        ststage[pl.ds(t * tq, tq), :] = stat.T

    def give_a(k, _):
        xx = lax.rem(x + k, nx)
        r = pl.ds(pl.multiple_of(xx * new_a, new_a), new_a)
        put(OA, oastage.at[r, :], oarecv.at[x], dev(y, xx, c))
        put(ST, ststage.at[r, :], strecv.at[x], dev(y, xx, c))
        return 0

    lax.fori_loop(1, nx, give_a, 0)
    copy(oastage.at[col_a, :], oarecv.at[x], recv_sem.at[OA])
    copy(ststage.at[col_a, :], strecv.at[x], recv_sem.at[ST])

    tops = tuple(scores(t, new_keys(0), q_all[4 * row_n(1) + t]) for t in tiles)
    tops = lax.fori_loop(1, ny - 1, rows_n, tops)

    wait_in(OA, oarecv)
    wait_in(ST, strecv)
    for g in range(grp):
        cols = pl.ds(g * dim, dim)
        ms = [strecv[i, :, g:g + 1] for i in range(nx)]
        top = functools.reduce(jnp.maximum, ms)
        num = jnp.zeros((new_a, dim), jnp.float32)
        den = jnp.zeros((new_a, 1), jnp.float32)
        for i in range(nx):
            w = jnp.exp2((ms[i] - top) * scale2)
            num = num + w * oarecv[i, :, cols]
            den = den + w * strecv[i, :, grp + g:grp + g + 1]
        odone[:, cols] = (num / den).astype(bf)

    def home_a(r, _):
        give(OY, odone.at[pl.ds(pl.multiple_of(r * ta, ta), ta), :],
             oa.at[:, pl.ds(pl.multiple_of(mine * width, width), width)], peer(r))
        return 0

    lax.fori_loop(0, kv, home_a, 0)
    lax.fori_loop(ny - 1, ny, rows_n, tops)

    wait_in(OB, ob)
    wait_in(OY, oa)
    for i, ref in enumerate((nkb, nka, nvb, nva)):
        wait(ref, out_sem.at[i])
    most = pl.ds(0, kv - 1)
    for item, ref in ((KC, tkb), (VC, tvb), (KAC, tka), (VAC, tva), (OB, obuf)):
        wait_out(item, ref.at[most])
    wait_out(QS, qbuf.at[pl.ds(0, CORES - 1)])
    for i in range(1, ny):
        wait_out(QS + i, qbuf.at[pl.ds(0, CORES)])
    for item, ref in ((KN, qbuf), (VN, qbuf)):
        wait_out(item, ref.at[most, :, pl.ds(0, dim)])
    for item, ref in ((KAN, kan), (VAN, van)):
        wait_out(item, ref.at[pl.ds(0, (kv - 1) * ta), :])
    wait_out(QA, qabuf.at[pl.ds(0, (kv - 1) * ta), :])
    wait_out(OY, odone.at[pl.ds(0, (kv - 1) * ta), :])
    wait_out(QX, others(qabuf))
    wait_out(OA, oarecv.at[pl.ds(0, nx - 1)])
    wait_out(ST, strecv.at[pl.ds(0, nx - 1)])
    ring_drain(0, kc)
    ring_drain(1, vc)
    ring_drain(2, kn)
    ring_drain(3, vn)


def attention(cp, xb, xa, cosf, sinf, wq, wk, wv, kcb, vcb, kca, vca):
    kv, dim = kcb.shape[1:]
    ny, nx = kv // CORES, cp // kv
    assert nx * CORES == kv and ny * nx * CORES == cp and ny == nx
    grp = wq.shape[1] // (kv * dim)
    tb, ta, cb, ca, model = xb.shape[0], xa.shape[0], kcb.shape[0], kca.shape[0], xb.shape[1]
    tq = tb // 2
    rows, width = grp * tq, grp * dim
    blk = CORES * tb
    assert blk == ca and (ny * nx * CORES * cb) % (ny * blk) == 0 and (cp * ta) % (2 * tq) == 0
    assert width == 2 * CORES * dim and kv * ta == tq and nx == 4 and CORES == 2
    bf, f32 = jnp.bfloat16, jnp.float32
    vm = pltpu.VMEM
    scratch = [
        vm((tb + ta, model), bf),
        vm((SLOTS, model, width), bf),
        vm((kv, tb + ta, width), bf),
        vm((ny, tb + ta, width), bf),
        vm(kcb.shape, bf), vm(vcb.shape, bf), vm(kca.shape, bf), vm(vca.shape, bf),
        vm((kv, cb, dim), bf), vm((kv, cb, dim), bf), vm((kv, ca, dim), bf), vm((kv, ca, dim), bf),
        vm((kv, tb, width), bf),
        vm((ny, nx, CORES * cb, dim), bf),
        vm((ny, nx, CORES * cb, dim), bf),
        vm((ny, nx, blk, dim), bf),
        vm((ny, nx, blk, dim), bf),
        vm((cp * cb // blk, dim, blk), bf),
        vm((ny * nx, dim, blk), bf),
        vm((kv, tb, width), bf),
        vm((2 * kv, dim, rows), f32),
        vm((2 * kv, 8, rows), f32),
        vm((2 * kv, 8, rows), f32),
        vm((4, rows, dim), bf),
        vm((2 * kv, rows, dim), bf),
        vm((blk, rows), f32), vm((blk, rows), f32), vm((blk, rows), f32), vm((blk, rows), f32),
        vm((blk, rows), bf), vm((blk, rows), bf), vm((blk, rows), bf), vm((blk, rows), bf),
        vm((cp * ta, width), bf),
        vm((kv, ca, dim), bf),
        vm((kv, ca, dim), bf),
        vm((kv * ta, dim), bf),
        vm((kv * ta, dim), bf),
        vm((kv, dim, ca), bf),
        vm((dim, kv * ta), bf),
        vm((cp * ta, width), f32),
        vm((cp * ta, dim), f32),
        vm((nx, kv * ta, width), f32),
        vm((nx, kv * ta, dim), f32),
        vm((kv * ta, width), bf),
        vm((4, dim, rows), f32),
        pltpu.SemaphoreType.DMA((15 + ny + 16,)),
        pltpu.SemaphoreType.DMA((15 + ny + 16,)),
        pltpu.SemaphoreType.DMA((5,)),
        pltpu.SemaphoreType.DMA((SLOTS,)),
        pltpu.SemaphoreType.DMA((4,)),
    ]
    any_spec = pl.BlockSpec(memory_space=pl.ANY)
    vmem_spec = pl.BlockSpec(memory_space=pltpu.VMEM)
    shape = jax.ShapeDtypeStruct
    return pl.pallas_call(
        functools.partial(kernel, (ny, nx, kv, grp, dim)),
        out_shape=(shape((tb, kv * width), bf), shape((ta, kv * width), bf),
                   shape((kv, tb, dim), bf), shape((kv, tb, dim), bf),
                   shape((kv, ta, dim), bf), shape((kv, ta, dim), bf)),
        in_specs=[any_spec, any_spec, vmem_spec, vmem_spec] + [any_spec] * 7,
        out_specs=(any_spec,) * 6,
        scratch_shapes=scratch,
        compiler_params=pltpu.CompilerParams(
            collective_id=0, has_side_effects=True, vmem_limit_bytes=VMEM_LIMIT),
        name="attend",
    )(xb, xa, cosf, sinf, wq, wk, wv, kcb, vcb, kca, vca)


def out_kernel(ob, oa, w, kb, vb, ka, va, yb, ya, nkb, nvb, nka, nva, o, wbuf, ybuf, *rest):
    new, turned, (wsem, osem, nsem, ysem) = rest[:4], rest[4:8], rest[8:]
    tb, ta = ob.shape[0], oa.shape[0]
    cols = wbuf.shape[2]
    steps = w.shape[1] // cols
    b_rows, a_rows = pl.ds(0, tb), pl.ds(tb, ta)

    def copy(src, dst, sem):
        pltpu.make_async_copy(src, dst, sem).start()

    def wait(ref, sem):
        pltpu.make_async_copy(ref, ref, sem).wait()

    def span(i):
        return pl.ds(pl.multiple_of(i * cols, cols), cols)

    def load(i):
        copy(w.at[:, span(i)], wbuf.at[lax.rem(i, SLOTS)], wsem.at[lax.rem(i, SLOTS)])

    copy(ob, o.at[b_rows, :], osem)
    copy(oa, o.at[a_rows, :], osem)
    for i in range(min(SLOTS - 1, steps)):
        load(i)
    for i, (src, dst) in enumerate(zip((kb, vb, ka, va), new)):
        copy(src, dst, nsem.at[i])
    wait(o, osem)

    def step(i, _):
        @pl.when(i + SLOTS - 1 < steps)
        def _():
            load(i + SLOTS - 1)

        slot = lax.rem(i, SLOTS)
        wait(wbuf.at[slot], wsem.at[slot])
        ybuf[i] = jnp.dot(o[...], wbuf[slot], preferred_element_type=jnp.float32).astype(ybuf.dtype)
        copy(ybuf.at[i, b_rows, :], yb.at[:, span(i)], ysem.at[0])
        copy(ybuf.at[i, a_rows, :], ya.at[:, span(i)], ysem.at[1])
        return 0

    lax.fori_loop(0, steps, step, 0)
    for i, (src, dst, out) in enumerate(zip(new, turned, (nkb, nvb, nka, nva))):
        wait(src, nsem.at[i])
        dst[...] = jnp.transpose(src[...], (1, 0, 2))
        copy(dst, out, nsem.at[i])
    wait(yb, ysem.at[0])
    wait(ya, ysem.at[1])
    for i, out in enumerate((nkb, nvb, nka, nva)):
        wait(out, nsem.at[i])


def output_projection(ob, oa, w, *new):
    (tb, inner), ta, model = ob.shape, oa.shape[0], w.shape[1]
    cols = min(512, model)
    shape = jax.ShapeDtypeStruct
    bf, vm, dma = ob.dtype, pltpu.VMEM, pltpu.SemaphoreType.DMA
    turned = [(t.shape[1], t.shape[0], t.shape[2]) for t in new]
    any_spec = pl.BlockSpec(memory_space=pl.ANY)
    return pl.pallas_call(
        out_kernel,
        out_shape=[shape((tb, model), bf), shape((ta, model), bf)] + [shape(t, bf) for t in turned],
        in_specs=[any_spec] * 7,
        out_specs=[any_spec] * 6,
        scratch_shapes=[vm((tb + ta, inner), bf), vm((SLOTS, inner, cols), bf), vm((model // cols, tb + ta, cols), bf)]
        + [vm(t.shape, bf) for t in new] + [vm(t, bf) for t in turned] + [dma((SLOTS,)), dma, dma((4,)), dma((2,))],
        compiler_params=pltpu.CompilerParams(vmem_limit_bytes=VMEM_LIMIT),
        name="project_out",
    )(ob, oa, w, *new)


def solution(mesh):
    cp_size = mesh.shape["cp"]

    def local_step(x_a, kc_a, vc_a, x_b, kc_b, vc_b, w_q, w_k, w_v, w_o):
        ta, tb = x_a.shape[0], x_b.shape[0]
        kv, dim = kc_a.shape[1:]
        me = lax.axis_index("cp")
        pos_a = kc_a.shape[0] * cp_size + me * ta + jnp.arange(ta)
        pos_b = kc_b.shape[0] * cp_size + me * tb + jnp.arange(tb)
        cosf, sinf = rope_tables(jnp.concatenate([pos_b, pos_a]), dim)
        o_b, o_a, k_b, v_b, k_a, v_a = attention(cp_size, x_b, x_a, cosf, sinf, w_q, w_k, w_v, kc_b, vc_b, kc_a, vc_a)
        y_b, y_a, k_b, v_b, k_a, v_a = output_projection(o_b, o_a, w_o, k_b, v_b, k_a, v_a)
        return y_a, k_a, v_a, y_b, k_b, v_b

    row_spec = P(("dp", "cp"), None)
    kv_spec = P(("dp", "cp"), None, None)
    full_spec = P()
    return jax.shard_map(
        local_step, mesh=mesh,
        in_specs=(row_spec, kv_spec, kv_spec, row_spec, kv_spec, kv_spec, full_spec, full_spec, full_spec, full_spec),
        out_specs=(row_spec, kv_spec, kv_spec, row_spec, kv_spec, kv_spec), check_vma=False)
```

```python
import functools

import jax
import jax.numpy as jnp
from jax import lax
from jax.experimental import pallas as pl
from jax.experimental.pallas import tpu as pltpu
from jax.sharding import PartitionSpec as P

ROPE_BASE = 500000
LOG2E = 1.4426950408889634
NEG = float(jnp.finfo(jnp.float32).min)
MESH = pl.DeviceIdType.MESH
CORES = 2
VMEM_LIMIT = 62 * 1024 * 1024
SLOTS = 3


def rope_tables(positions, head_dim):
    half_dim = head_dim // 2
    inv_freq = jnp.power(jnp.float32(ROPE_BASE), jnp.arange(half_dim, dtype=jnp.float32) * (-2.0 / head_dim))
    angles = positions.astype(jnp.float32)[:, None] * inv_freq[None, :]
    cos_ang, sin_ang = jnp.cos(angles), jnp.sin(angles)
    return jnp.concatenate([cos_ang, cos_ang], axis=1), jnp.concatenate([-sin_ang, sin_ang], axis=1)


def qk(keys, queries):
    return lax.dot_general(keys, queries, (((1,), (1,)), ((), ())), preferred_element_type=jnp.float32)


def fold(s, op):
    return functools.reduce(op, [s[i:i + 8] for i in range(0, s.shape[0], 8)])


def soft_step(scale2, s, vt, m, l, acc_ref):
    m_new = jnp.maximum(m, jnp.max(s, axis=0, keepdims=True))
    alpha = jnp.exp2((m - m_new) * scale2)
    e = jnp.exp2((s - m_new) * scale2)
    l_new = l * alpha + jnp.sum(e, axis=0, keepdims=True)
    pv = jnp.dot(vt, e.astype(jnp.bfloat16), preferred_element_type=jnp.float32)
    acc_ref[...] = acc_ref[...] * alpha + pv
    return m_new, l_new


def kernel(dims, xb, xa, cosf, sinf, wq, wk, wv, kcb, vcb, kca, vca, ob, oa, nkb, nvb, nka, nva,
           xs, wbuf, qsend, kvsend, rkb, rvb, rka, rva, tkb, tvb, tka, tva,
           qbuf, kc, vc, kn, vn, vtc, vtn, obuf, acc, m_all, l_all, q_a, q_all, s0, s1, s2, s3, p0, p1, p2, p3,
           qabuf, kac, vac, kan, van, vtac, vtan, oastage, ststage, oarecv, strecv, odone, acc_a,
           send_sem, recv_sem, load_sem, wsem, out_sem):
    ny, nx, kv, grp, dim = dims
    cp = ny * nx * CORES
    tb, ta = xb.shape[0], xa.shape[0]
    tq = tb // 2
    rows = grp * tq
    width = grp * dim
    pair = CORES * dim
    cb = kcb.shape[0]
    scale2 = dim ** -0.5 * LOG2E
    bf = jnp.bfloat16

    me = lax.axis_index("cp")
    c = lax.rem(me, CORES)
    x = lax.rem(me // CORES, nx)
    y = me // (CORES * nx)
    mine = y * CORES + c

    def dev(yy, xx, cc):
        return (yy * nx + xx) * CORES + cc

    def peer(h):
        return dev(h // CORES, x, lax.rem(h, CORES))

    def put(item, src, dst, target):
        pltpu.make_async_remote_copy(
            src_ref=src, dst_ref=dst, send_sem=send_sem.at[item], recv_sem=recv_sem.at[item],
            device_id={"cp": target}, device_id_type=MESH,
        ).start()

    def copy(src, dst, sem):
        pltpu.make_async_copy(src, dst, sem).start()

    def wait(ref, sem):
        pltpu.make_async_copy(ref, ref, sem).wait()

    def give(item, src, dst, target):
        @pl.when(target == me)
        def _():
            copy(src, dst, recv_sem.at[item])

        @pl.when(target != me)
        def _():
            put(item, src, dst, target)

    def wait_in(item, ref):
        wait(ref, recv_sem.at[item])

    def wait_out(item, ref):
        wait(ref, send_sem.at[item])

    KC, VC, Q, KN, VN, KAC, VAC, KAN, VAN, QA, QX, OB, OA, ST, OY = range(15)
    QS = 15
    AG = QS + ny

    barrier = pltpu.get_barrier_semaphore()

    def greet(d, _):
        pl.semaphore_signal(barrier, inc=1, device_id={"cp": d}, device_id_type=MESH)
        return 0

    raw = ((kcb, rkb, tkb), (vcb, rvb, tvb), (kca, rka, tka), (vca, rva, tva))
    for i, (src, dst, _) in enumerate(raw):
        copy(src, dst, load_sem.at[i])
    copy(xb, xs.at[pl.ds(0, tb), :], load_sem.at[4])
    copy(xa, xs.at[pl.ds(tb, ta), :], load_sem.at[4])

    q_steps, kv_steps = kv, kv // CORES

    def q_head(i):
        return lax.rem(mine + 1 + i, kv)

    def kv_pair(i):
        return lax.rem(y + 1 + i, ny)

    def load_q_cols(i, slot):
        copy(wq.at[:, pl.ds(pl.multiple_of(q_head(i) * width, width), width)], wbuf.at[slot], wsem.at[slot])

    def load_kv_cols(i, slot):
        cols = pl.ds(pl.multiple_of(kv_pair(i) * pair, pair), pair)
        copy(wk.at[:, cols], wbuf.at[slot, :, pl.ds(0, pair)], wsem.at[slot])
        copy(wv.at[:, cols], wbuf.at[slot, :, pl.ds(pair, pair)], wsem.at[slot])

    def load_cols(i):
        slot = lax.rem(i, SLOTS)

        @pl.when(i < kv_steps)
        def _():
            load_kv_cols(i, slot)

        @pl.when(jnp.logical_and(i >= kv_steps, i < kv_steps + q_steps))
        def _():
            load_q_cols(i - kv_steps, slot)

    for i in range(SLOTS - 1):
        load_cols(jnp.int32(i))
    lax.fori_loop(0, cp, greet, 0)

    def turn_raw(i):
        _, dst, turned = raw[i]
        wait(dst, load_sem.at[i])
        turned[...] = jnp.transpose(dst[...], (1, 0, 2))

    turn_raw(0)
    turn_raw(1)

    def scatter(item, src, dst):
        def one(k, _):
            h = lax.rem(mine + k, kv)
            put(item, src.at[h], dst, peer(h))
            return 0

        lax.fori_loop(1, kv, one, 0)
        copy(src.at[mine], dst, recv_sem.at[item])

    right = dev(y, lax.rem(x + 1, nx), c)
    left = dev(y, lax.rem(x + nx - 1, nx), c)
    x_left = lax.rem(x + nx - 1, nx)
    x_right = lax.rem(x + 1, nx)
    x_far = lax.rem(x + nx // 2, nx)
    lo, hi = pl.ds(0, ny // 2), pl.ds(ny // 2, ny // 2)

    def ag_sem(i, step, direction):
        return AG + i * 4 + step * 2 + direction

    def ring_first(i, buf):
        put(ag_sem(i, 0, 0), buf.at[:, x], buf.at[:, x], right)
        put(ag_sem(i, 0, 1), buf.at[:, x], buf.at[:, x], left)

    def ring_second(i, buf):
        wait_in(ag_sem(i, 0, 0), buf.at[:, x_left])
        put(ag_sem(i, 1, 0), buf.at[lo, x_left], buf.at[lo, x_left], right)
        wait_in(ag_sem(i, 0, 1), buf.at[:, x_right])
        put(ag_sem(i, 1, 1), buf.at[hi, x_right], buf.at[hi, x_right], left)

    def ring_last(i, buf):
        wait_in(ag_sem(i, 1, 0), buf.at[lo, x_far])
        wait_in(ag_sem(i, 1, 1), buf.at[hi, x_far])

    def ring_drain(i, buf):
        wait_out(ag_sem(i, 0, 0), buf.at[:, x])
        wait_out(ag_sem(i, 0, 1), buf.at[:, x])
        wait_out(ag_sem(i, 1, 0), buf.at[lo, x])
        wait_out(ag_sem(i, 1, 1), buf.at[hi, x])

    wait(xs, load_sem.at[4])
    b_rows, a_rows = pl.ds(0, tb), pl.ds(tb, ta)
    new_a = kv * ta
    col_a = pl.ds(pl.multiple_of(x * new_a, new_a), new_a)
    my_a = pl.ds(pl.multiple_of(x * new_a + mine * ta, ta), ta)

    def rope(t):
        t = t.astype(bf).astype(jnp.float32)
        return (t * cosf[...] + pltpu.roll(t, dim // 2, 1) * sinf[...]).astype(bf)

    def project(slot):
        return jnp.dot(xs[...], wbuf[slot], preferred_element_type=jnp.float32)

    def q_step(i, _):
        load_cols(kv_steps + i + SLOTS - 1)
        slot = lax.rem(kv_steps + i, SLOTS)
        wait(wbuf.at[slot], wsem.at[slot])
        h = q_head(i)
        lin = project(slot)
        for g in range(grp):
            cols = slice(g * dim, (g + 1) * dim)
            qsend[h, :, cols] = rope(lin[:, cols])
        give(QS + lax.rem(y - h // CORES + ny, ny), qsend.at[h, b_rows], qbuf.at[mine], peer(h))
        give(QA, qsend.at[h, a_rows], qabuf.at[my_a, :], peer(h))
        return 0

    def kv_project(i):
        load_cols(i + SLOTS - 1)
        slot = lax.rem(i, SLOTS)
        wait(wbuf.at[slot], wsem.at[slot])
        p = kv_pair(i)
        lin = project(slot)
        for g in range(CORES):
            cols = slice(g * dim, (g + 1) * dim)
            kvsend[p, :, cols] = rope(lin[:, cols])
        kvsend[p, :, pair:2 * pair] = lin[:, pair:2 * pair].astype(bf)

    def kv_give(i):
        p = kv_pair(i)
        for j, (nb, na) in enumerate(((nkb, nka), (nvb, nva))):
            for g in range(CORES):
                cols = pl.ds(j * pair + g * dim, dim)
                copy(kvsend.at[p, b_rows, cols], nb.at[p * CORES + g], out_sem.at[2 * j])
                copy(kvsend.at[p, a_rows, cols], na.at[p * CORES + g], out_sem.at[2 * j + 1])
        n_rows = pl.ds(pl.multiple_of(c * tb, tb), tb)
        s_rows = pl.ds(pl.multiple_of(mine * ta, ta), ta)
        for g in range(CORES):
            for j, (ib, db, ia, da) in enumerate(((KN, kn, KAN, kan), (VN, vn, VAN, van))):
                cols = pl.ds(j * pair + g * dim, dim)
                give(ib, kvsend.at[p, b_rows, cols], db.at[y, x, n_rows, :], dev(p, x, g))
                give(ia, kvsend.at[p, a_rows, cols], da.at[s_rows, :], dev(p, x, g))

    def kv_step(i, _):
        kv_project(i)
        kv_give(i)
        return 0

    kv_project(jnp.int32(0))
    pl.semaphore_wait(barrier, cp)
    c_rows = pl.ds(pl.multiple_of(c * cb, cb), cb)
    scatter(KC, tkb, kc.at[y, x, c_rows, :])
    scatter(VC, tvb, vc.at[y, x, c_rows, :])
    kv_give(jnp.int32(0))
    lax.fori_loop(1, kv_steps, kv_step, 0)
    wait_in(KC, kc.at[:, x])
    ring_first(0, kc)
    wait_in(VC, vc.at[:, x])
    ring_first(1, vc)
    lax.fori_loop(0, q_steps - 1, q_step, 0)
    ring_second(0, kc)
    ring_second(1, vc)
    lax.fori_loop(q_steps - 1, q_steps, q_step, 0)
    wait_in(KN, kn.at[:, x])
    ring_first(2, kn)
    wait_in(VN, vn.at[:, x])
    ring_first(3, vn)
    turn_raw(2)
    scatter(KAC, tka, kac.at[mine])
    turn_raw(3)
    scatter(VAC, tva, vac.at[mine])

    s_refs, p_refs = (s0, s1, s2, s3), (p0, p1, p2, p3)
    blk = s0.shape[0]
    tiles = range(4)

    def scores(t, keys, queries):
        s = qk(keys, queries)
        s_refs[t][...] = s
        return fold(s, jnp.maximum)

    def highest(m, top8):
        m_new = jnp.maximum(m, jnp.max(top8, axis=0, keepdims=True))
        return m_new, jnp.exp2((m - m_new) * scale2)

    def expo(t, m, l8, top8):
        m_new, alpha = highest(m, top8)
        l8 = l8 * alpha
        for r in range(0, blk, 16):
            e = jnp.exp2((s_refs[t][pl.ds(r, 16), :] - m_new) * scale2)
            p_refs[t][pl.ds(r, 16), :] = e.astype(bf)
            l8 = l8 + fold(e, jnp.add)
        return m_new, l8, alpha

    def values(t, vt, alpha, acc_ref):
        acc_ref[...] = acc_ref[...] * alpha + jnp.dot(vt, p_refs[t][...], preferred_element_type=jnp.float32)

    def step(carry, before, now, k_after, q_after, acc_before, accs):
        m, l, top = list(carry[0:4]), list(carry[4:8]), list(carry[8:12])
        values(3, before, carry[12], acc_before)
        for t in tiles:
            m[t], l[t], alpha = expo(t, m[t], l[t], top[t])
            top[t] = scores(t, k_after, q_after(t))
            if t < 3:
                values(t, now, alpha, accs[t])
        return tuple(m + l + top) + (alpha,)

    neg, zero = jnp.full((1, rows), NEG, jnp.float32), jnp.zeros((8, rows), jnp.float32)
    one = jnp.ones((1, rows), jnp.float32)

    def total(l8):
        return jnp.sum(l8, axis=0, keepdims=True)

    def others(ref):
        return ref.at[pl.ds(0, (nx - 1) * new_a), :]

    def token_of_lane(shape):
        return lax.rem(lax.broadcasted_iota(jnp.int32, shape, 1), tq)

    def turn(first, end, dst, block):
        n = 2 if first % 4 or end % 4 else 4

        def some(i, _):
            for k in range(n):
                dst[n * i + k] = block(n * i + k).T
            return 0

        lax.fori_loop(first // n, end // n, some, 0)

    blocks = vtc.shape[0]
    per_col = blocks // nx
    part = ny // per_col
    acc[...] = jnp.zeros_like(acc)
    p3[...] = jnp.zeros_like(p3)

    def row_of(i):
        return lax.rem(y + ny - i, ny)

    def arrive_q(i):
        yy = row_of(i)
        wait_in(QS + (ny - i) % ny, qbuf.at[pl.ds(yy * CORES, CORES)])
        for t in tiles:
            u, half = yy * CORES + t // 2, t % 2
            for g in range(grp):
                q_all[4 * yy + t, pl.ds(g * tq, tq), :] = qbuf[u, pl.ds(half * tq, tq), pl.ds(g * dim, dim)]

    def cached(buf, j):
        i = j // per_col
        xx = jnp.where(i == 0, x, jnp.where(i == 1, x_left, jnp.where(i == 2, x_right, x_far)))
        return buf[pl.ds(lax.rem(j, per_col) * part, part), xx].reshape(blk, dim)

    def turn_c(first, end):
        turn(first, end, vtc, lambda j: cached(vc, j))

    near = blocks - per_col
    arrive_q(0)
    turn_c(0, near)

    def step_c(i, carry):
        yy, j = row_of(i // blocks), lax.rem(i, blocks)
        before, after = lax.max(i - 1, 0), lax.min(i + 1, ny * blocks - 1)
        y_before, y_after = row_of(before // blocks), row_of(after // blocks)
        start = j == 0
        m = tuple(jnp.where(start, NEG, v) for v in carry[0:4])
        l = tuple(jnp.where(start, 0.0, v) for v in carry[4:8])
        out = step(
            m + l + carry[8:], vtc[lax.rem(before, blocks)], vtc[j], cached(kc, lax.rem(after, blocks)),
            lambda t: q_all[4 * y_after + t], acc.at[4 * y_before + 3], [acc.at[4 * yy + t] for t in tiles])
        for t in tiles:
            m_all[4 * yy + t, 0:1, :] = out[t]
            l_all[4 * yy + t] = out[4 + t]
        return out

    tops = tuple(scores(t, cached(kc, jnp.int32(0)), q_all[4 * y + t]) for t in tiles)
    carry = (neg,) * 4 + (zero,) * 4 + tops + (one,)
    carry = lax.fori_loop(0, near - 1, step_c, carry)
    ring_last(0, kc)
    ring_last(1, vc)
    turn_c(near, blocks)
    carry = lax.fori_loop(near - 1, blocks - 1, step_c, carry)
    arrive_q(1)
    carry = lax.fori_loop(blocks - 1, 2 * blocks - 1, step_c, carry)
    wait_in(QA, qabuf.at[col_a, :])

    def pass_qa(k, _):
        put(QX, qabuf.at[col_a, :], qabuf.at[col_a, :], dev(y, lax.rem(x + k, nx), c))
        return 0

    lax.fori_loop(1, nx, pass_qa, 0)
    arrive_q(2)
    carry = lax.fori_loop(2 * blocks - 1, 3 * blocks - 1, step_c, carry)
    arrive_q(3)
    ring_second(2, kn)
    ring_second(3, vn)
    carry = lax.fori_loop(3 * blocks - 1, 4 * blocks, step_c, carry)
    values(3, vtc[blocks - 1], carry[12], acc.at[4 * row_of(ny - 1) + 3])

    ring_last(2, kn)
    ring_last(3, vn)
    turn(0, ny * nx, vtn, lambda j: vn[j // nx, lax.rem(j, nx)])

    def new_keys(j):
        return kn[j // nx, lax.rem(j, nx)]

    def row_n(i):
        return lax.rem(y + ny + jnp.where(c == 0, 1 + i, ny - 1 - i), ny)

    def rows_n(i, tops):
        yy, y_after = row_n(i), row_n(lax.min(i + 1, ny - 1))
        last = yy * nx + x
        accs = [acc.at[4 * yy + t] for t in tiles]
        p3[...] = jnp.zeros_like(p3)

        def step_n(j, carry):
            return step(carry, vtn[lax.max(j - 1, 0)], vtn[j], new_keys(j + 1), lambda t: q_all[4 * yy + t],
                        accs[3], accs)

        state = tuple(m_all[4 * yy + t, 0:1, :] for t in tiles) + tuple(l_all[4 * yy + t] for t in tiles)
        carry = lax.fori_loop(0, last, step_n, state + tuple(tops) + (one,))
        values(3, vtn[lax.max(last - 1, 0)], carry[12], accs[3])
        tops = []
        for t in tiles:
            seen = (t + 1) * tq
            tri = lax.broadcasted_iota(jnp.int32, (tq, rows), 0) <= token_of_lane((tq, rows))
            s = jnp.where(tri, s_refs[t][pl.ds(t * tq, tq), :], NEG)
            s_refs[t][pl.ds(t * tq, tq), :] = s
            top8 = fold(s, jnp.maximum)
            if t:
                top8 = jnp.maximum(top8, fold(s_refs[t][pl.ds(0, t * tq), :], jnp.maximum))
            m_new, alpha = highest(carry[t], top8)
            l8 = carry[4 + t] * alpha
            for r in range(0, seen, 16):
                e = jnp.exp2((s_refs[t][pl.ds(r, 16), :] - m_new) * scale2)
                p_refs[t][pl.ds(r, 16), :] = e.astype(bf)
                l8 = l8 + fold(e, jnp.add)
            tops.append(scores(t, new_keys(0), q_all[4 * y_after + t]))
            pv = jnp.dot(vtn[last, :, pl.ds(0, seen)], p_refs[t][pl.ds(0, seen), :], preferred_element_type=jnp.float32)
            o = (accs[t][...] * alpha + pv) * (1.0 / total(l8))
            for g in range(grp):
                obuf[yy * CORES + t // 2, pl.ds(t % 2 * tq, tq), pl.ds(g * dim, dim)] = (
                    o[:, g * tq:(g + 1) * tq].T.astype(bf))
        for cc in range(CORES):
            u = yy * CORES + cc
            give(OB, obuf.at[u], ob.at[:, pl.ds(pl.multiple_of(mine * width, width), width)], peer(u))
        return tuple(tops)

    tops = tuple(scores(t, new_keys(0), q_all[4 * row_n(0) + t]) for t in tiles)
    tops = lax.fori_loop(0, 1, rows_n, tops)

    wait_in(QX, others(qabuf))
    wait_in(KAC, kac)
    wait_in(VAC, vac)
    wait_in(KAN, kan)
    wait_in(VAN, van)
    turn(0, kv, vtac, lambda j: vac[j])
    vtan[...] = van[...].T
    for t in tiles:
        for g in range(grp):
            q_a[t, pl.ds(g * tq, tq), :] = qabuf[pl.ds(t * tq, tq), pl.ds(g * dim, dim)]
    acc_a[...] = jnp.zeros_like(acc_a)
    p3[...] = jnp.zeros_like(p3)
    accs_a = [acc_a.at[t] for t in tiles]

    def step_a(j, carry):
        return step(carry, vtac[lax.max(j - 1, 0)], vtac[j], kac[j + 1], lambda t: q_a[t], accs_a[3], accs_a)

    tops = tuple(scores(t, kac[0], q_a[t]) for t in tiles)
    carry = lax.fori_loop(0, kv - 1, step_a, (neg,) * 4 + (zero,) * 4 + tops + (one,))
    values(3, vtac[kv - 2], carry[12], accs_a[3])

    def token_a(r, xx):
        holder = dev(r // (CORES * ta), xx, lax.rem(r // ta, CORES))
        return holder * ta + lax.rem(r, ta)

    pos_k = token_a(lax.broadcasted_iota(jnp.int32, (new_a, rows), 0), x)
    place_q = token_of_lane((new_a, rows))
    row = lax.broadcasted_iota(jnp.int32, (dim, tq), 0)
    for t in tiles:
        m, l, alpha = expo(t, carry[t], carry[4 + t], carry[8 + t])
        values(t, vtac[kv - 1], alpha, accs_a[t])
        s = jnp.where(pos_k <= token_a(place_q, t), qk(kan[...], q_a[t]), NEG)
        m, l = soft_step(scale2, s, vtan[...], m, total(l), accs_a[t])
        stat = jnp.zeros((dim, tq), jnp.float32)
        for g in range(grp):
            cols = slice(g * tq, (g + 1) * tq)
            oastage[pl.ds(t * tq, tq), pl.ds(g * dim, dim)] = acc_a[t, :, cols].T
            stat = jnp.where(row == g, m[:, cols], stat)
            stat = jnp.where(row == grp + g, l[:, cols], stat)
        ststage[pl.ds(t * tq, tq), :] = stat.T

    def give_a(k, _):
        xx = lax.rem(x + k, nx)
        r = pl.ds(pl.multiple_of(xx * new_a, new_a), new_a)
        put(OA, oastage.at[r, :], oarecv.at[x], dev(y, xx, c))
        put(ST, ststage.at[r, :], strecv.at[x], dev(y, xx, c))
        return 0

    lax.fori_loop(1, nx, give_a, 0)
    copy(oastage.at[col_a, :], oarecv.at[x], recv_sem.at[OA])
    copy(ststage.at[col_a, :], strecv.at[x], recv_sem.at[ST])

    tops = tuple(scores(t, new_keys(0), q_all[4 * row_n(1) + t]) for t in tiles)
    tops = lax.fori_loop(1, ny - 1, rows_n, tops)

    wait_in(OA, oarecv)
    wait_in(ST, strecv)
    for g in range(grp):
        cols = pl.ds(g * dim, dim)
        ms = [strecv[i, :, g:g + 1] for i in range(nx)]
        top = functools.reduce(jnp.maximum, ms)
        num = jnp.zeros((new_a, dim), jnp.float32)
        den = jnp.zeros((new_a, 1), jnp.float32)
        for i in range(nx):
            w = jnp.exp2((ms[i] - top) * scale2)
            num = num + w * oarecv[i, :, cols]
            den = den + w * strecv[i, :, grp + g:grp + g + 1]
        odone[:, cols] = (num / den).astype(bf)

    def home_a(r, _):
        give(OY, odone.at[pl.ds(pl.multiple_of(r * ta, ta), ta), :],
             oa.at[:, pl.ds(pl.multiple_of(mine * width, width), width)], peer(r))
        return 0

    lax.fori_loop(0, kv, home_a, 0)
    lax.fori_loop(ny - 1, ny, rows_n, tops)

    wait_in(OB, ob)
    wait_in(OY, oa)
    for i, ref in enumerate((nkb, nka, nvb, nva)):
        wait(ref, out_sem.at[i])
    most = pl.ds(0, kv - 1)
    for item, ref in ((KC, tkb), (VC, tvb), (KAC, tka), (VAC, tva), (OB, obuf)):
        wait_out(item, ref.at[most])
    wait_out(QS, qbuf.at[pl.ds(0, CORES - 1)])
    for i in range(1, ny):
        wait_out(QS + i, qbuf.at[pl.ds(0, CORES)])
    for item, ref in ((KN, qbuf), (VN, qbuf)):
        wait_out(item, ref.at[most, :, pl.ds(0, dim)])
    for item, ref in ((KAN, kan), (VAN, van)):
        wait_out(item, ref.at[pl.ds(0, (kv - 1) * ta), :])
    wait_out(QA, qabuf.at[pl.ds(0, (kv - 1) * ta), :])
    wait_out(OY, odone.at[pl.ds(0, (kv - 1) * ta), :])
    wait_out(QX, others(qabuf))
    wait_out(OA, oarecv.at[pl.ds(0, nx - 1)])
    wait_out(ST, strecv.at[pl.ds(0, nx - 1)])
    ring_drain(0, kc)
    ring_drain(1, vc)
    ring_drain(2, kn)
    ring_drain(3, vn)


def attention(cp, xb, xa, cosf, sinf, wq, wk, wv, kcb, vcb, kca, vca):
    kv, dim = kcb.shape[1:]
    ny, nx = kv // CORES, cp // kv
    assert nx * CORES == kv and ny * nx * CORES == cp and ny == nx
    grp = wq.shape[1] // (kv * dim)
    tb, ta, cb, ca, model = xb.shape[0], xa.shape[0], kcb.shape[0], kca.shape[0], xb.shape[1]
    tq = tb // 2
    rows, width = grp * tq, grp * dim
    blk = CORES * tb
    assert blk == ca and (ny * CORES * cb) % (2 * blk) == 0 and (cp * ta) % (2 * tq) == 0
    assert width == 2 * CORES * dim and kv * ta == tq and nx == 4 and CORES == 2
    bf, f32 = jnp.bfloat16, jnp.float32
    vm = pltpu.VMEM
    scratch = [
        vm((tb + ta, model), bf),
        vm((SLOTS, model, width), bf),
        vm((kv, tb + ta, width), bf),
        vm((ny, tb + ta, width), bf),
        vm(kcb.shape, bf), vm(vcb.shape, bf), vm(kca.shape, bf), vm(vca.shape, bf),
        vm((kv, cb, dim), bf), vm((kv, cb, dim), bf), vm((kv, ca, dim), bf), vm((kv, ca, dim), bf),
        vm((kv, tb, width), bf),
        vm((ny, nx, CORES * cb, dim), bf),
        vm((ny, nx, CORES * cb, dim), bf),
        vm((ny, nx, blk, dim), bf),
        vm((ny, nx, blk, dim), bf),
        vm((cp * cb // blk, dim, blk), bf),
        vm((ny * nx, dim, blk), bf),
        vm((kv, tb, width), bf),
        vm((2 * kv, dim, rows), f32),
        vm((2 * kv, 8, rows), f32),
        vm((2 * kv, 8, rows), f32),
        vm((4, rows, dim), bf),
        vm((2 * kv, rows, dim), bf),
        vm((blk, rows), f32), vm((blk, rows), f32), vm((blk, rows), f32), vm((blk, rows), f32),
        vm((blk, rows), bf), vm((blk, rows), bf), vm((blk, rows), bf), vm((blk, rows), bf),
        vm((cp * ta, width), bf),
        vm((kv, ca, dim), bf),
        vm((kv, ca, dim), bf),
        vm((kv * ta, dim), bf),
        vm((kv * ta, dim), bf),
        vm((kv, dim, ca), bf),
        vm((dim, kv * ta), bf),
        vm((cp * ta, width), f32),
        vm((cp * ta, dim), f32),
        vm((nx, kv * ta, width), f32),
        vm((nx, kv * ta, dim), f32),
        vm((kv * ta, width), bf),
        vm((4, dim, rows), f32),
        pltpu.SemaphoreType.DMA((15 + ny + 16,)),
        pltpu.SemaphoreType.DMA((15 + ny + 16,)),
        pltpu.SemaphoreType.DMA((5,)),
        pltpu.SemaphoreType.DMA((SLOTS,)),
        pltpu.SemaphoreType.DMA((4,)),
    ]
    any_spec = pl.BlockSpec(memory_space=pl.ANY)
    vmem_spec = pl.BlockSpec(memory_space=pltpu.VMEM)
    shape = jax.ShapeDtypeStruct
    return pl.pallas_call(
        functools.partial(kernel, (ny, nx, kv, grp, dim)),
        out_shape=(shape((tb, kv * width), bf), shape((ta, kv * width), bf),
                   shape((kv, tb, dim), bf), shape((kv, tb, dim), bf),
                   shape((kv, ta, dim), bf), shape((kv, ta, dim), bf)),
        in_specs=[any_spec, any_spec, vmem_spec, vmem_spec] + [any_spec] * 7,
        out_specs=(any_spec,) * 6,
        scratch_shapes=scratch,
        compiler_params=pltpu.CompilerParams(
            collective_id=0, has_side_effects=True, vmem_limit_bytes=VMEM_LIMIT),
        name="attend",
    )(xb, xa, cosf, sinf, wq, wk, wv, kcb, vcb, kca, vca)


def out_kernel(ob, oa, w, kb, vb, ka, va, yb, ya, nkb, nvb, nka, nva, o, wbuf, ybuf, *rest):
    new, turned, (wsem, osem, nsem, ysem) = rest[:4], rest[4:8], rest[8:]
    tb, ta = ob.shape[0], oa.shape[0]
    cols = wbuf.shape[2]
    steps = w.shape[1] // cols
    b_rows, a_rows = pl.ds(0, tb), pl.ds(tb, ta)

    def copy(src, dst, sem):
        pltpu.make_async_copy(src, dst, sem).start()

    def wait(ref, sem):
        pltpu.make_async_copy(ref, ref, sem).wait()

    def span(i):
        return pl.ds(pl.multiple_of(i * cols, cols), cols)

    def load(i):
        copy(w.at[:, span(i)], wbuf.at[lax.rem(i, SLOTS)], wsem.at[lax.rem(i, SLOTS)])

    copy(ob, o.at[b_rows, :], osem)
    copy(oa, o.at[a_rows, :], osem)
    for i in range(min(SLOTS - 1, steps)):
        load(i)
    for i, (src, dst) in enumerate(zip((kb, vb, ka, va), new)):
        copy(src, dst, nsem.at[i])
    wait(o, osem)

    def step(i, _):
        @pl.when(i + SLOTS - 1 < steps)
        def _():
            load(i + SLOTS - 1)

        slot = lax.rem(i, SLOTS)
        wait(wbuf.at[slot], wsem.at[slot])
        ybuf[i] = jnp.dot(o[...], wbuf[slot], preferred_element_type=jnp.float32).astype(ybuf.dtype)
        copy(ybuf.at[i, b_rows, :], yb.at[:, span(i)], ysem.at[0])
        copy(ybuf.at[i, a_rows, :], ya.at[:, span(i)], ysem.at[1])
        return 0

    lax.fori_loop(0, steps, step, 0)
    for i, (src, dst, out) in enumerate(zip(new, turned, (nkb, nvb, nka, nva))):
        wait(src, nsem.at[i])
        dst[...] = jnp.transpose(src[...], (1, 0, 2))
        copy(dst, out, nsem.at[i])
    wait(yb, ysem.at[0])
    wait(ya, ysem.at[1])
    for i, out in enumerate((nkb, nvb, nka, nva)):
        wait(out, nsem.at[i])


def output_projection(ob, oa, w, *new):
    (tb, inner), ta, model = ob.shape, oa.shape[0], w.shape[1]
    cols = min(512, model)
    shape = jax.ShapeDtypeStruct
    bf, vm, dma = ob.dtype, pltpu.VMEM, pltpu.SemaphoreType.DMA
    turned = [(t.shape[1], t.shape[0], t.shape[2]) for t in new]
    any_spec = pl.BlockSpec(memory_space=pl.ANY)
    return pl.pallas_call(
        out_kernel,
        out_shape=[shape((tb, model), bf), shape((ta, model), bf)] + [shape(t, bf) for t in turned],
        in_specs=[any_spec] * 7,
        out_specs=[any_spec] * 6,
        scratch_shapes=[vm((tb + ta, inner), bf), vm((SLOTS, inner, cols), bf), vm((model // cols, tb + ta, cols), bf)]
        + [vm(t.shape, bf) for t in new] + [vm(t, bf) for t in turned] + [dma((SLOTS,)), dma, dma((4,)), dma((2,))],
        compiler_params=pltpu.CompilerParams(vmem_limit_bytes=VMEM_LIMIT),
        name="project_out",
    )(ob, oa, w, *new)


def solution(mesh):
    cp_size = mesh.shape["cp"]

    def local_step(x_a, kc_a, vc_a, x_b, kc_b, vc_b, w_q, w_k, w_v, w_o):
        ta, tb = x_a.shape[0], x_b.shape[0]
        kv, dim = kc_a.shape[1:]
        me = lax.axis_index("cp")
        pos_a = kc_a.shape[0] * cp_size + me * ta + jnp.arange(ta)
        pos_b = kc_b.shape[0] * cp_size + me * tb + jnp.arange(tb)
        cosf, sinf = rope_tables(jnp.concatenate([pos_b, pos_a]), dim)
        o_b, o_a, k_b, v_b, k_a, v_a = attention(cp_size, x_b, x_a, cosf, sinf, w_q, w_k, w_v, kc_b, vc_b, kc_a, vc_a)
        y_b, y_a, k_b, v_b, k_a, v_a = output_projection(o_b, o_a, w_o, k_b, v_b, k_a, v_a)
        return y_a, k_a, v_a, y_b, k_b, v_b

    row_spec = P(("dp", "cp"), None)
    kv_spec = P(("dp", "cp"), None, None)
    full_spec = P()
    return jax.shard_map(
        local_step, mesh=mesh,
        in_specs=(row_spec, kv_spec, kv_spec, row_spec, kv_spec, kv_spec, full_spec, full_spec, full_spec, full_spec),
        out_specs=(row_spec, kv_spec, kv_spec, row_spec, kv_spec, kv_spec), check_vma=False)
```

```python
import functools

import jax
import jax.numpy as jnp
from jax import lax
from jax.experimental import pallas as pl
from jax.experimental.pallas import tpu as pltpu
from jax.sharding import PartitionSpec as P

ROPE_BASE = 500000
LOG2E = 1.4426950408889634
NEG = float(jnp.finfo(jnp.float32).min)
MESH = pl.DeviceIdType.MESH
CORES = 2
VMEM_LIMIT = 62 * 1024 * 1024
SLOTS = 3


def rope_tables(positions, head_dim):
    half_dim = head_dim // 2
    inv_freq = jnp.power(jnp.float32(ROPE_BASE), jnp.arange(half_dim, dtype=jnp.float32) * (-2.0 / head_dim))
    angles = positions.astype(jnp.float32)[:, None] * inv_freq[None, :]
    cos_ang, sin_ang = jnp.cos(angles), jnp.sin(angles)
    return jnp.concatenate([cos_ang, cos_ang], axis=1), jnp.concatenate([-sin_ang, sin_ang], axis=1)


def qk(keys, queries):
    return lax.dot_general(keys, queries, (((1,), (1,)), ((), ())), preferred_element_type=jnp.float32)


def fold(s, op):
    return functools.reduce(op, [s[i:i + 8] for i in range(0, s.shape[0], 8)])


def soft_step(scale2, s, vt, m, l, acc_ref):
    m_new = jnp.maximum(m, jnp.max(s, axis=0, keepdims=True))
    alpha = jnp.exp2((m - m_new) * scale2)
    e = jnp.exp2((s - m_new) * scale2)
    l_new = l * alpha + jnp.sum(e, axis=0, keepdims=True)
    pv = jnp.dot(vt, e.astype(jnp.bfloat16), preferred_element_type=jnp.float32)
    acc_ref[...] = acc_ref[...] * alpha + pv
    return m_new, l_new


def kernel(dims, xb, xa, cosf, sinf, wq, wk, wv, kcb, vcb, kca, vca, ob, oa, nkb, nvb, nka, nva,
           xs, wbuf, qsend, kvsend, rkb, rvb, rka, rva, tkb, tvb, tka, tva,
           qbuf, kc, vc, kn, vn, vtc, vtn, obuf, acc, m_all, l_all, q_a, q_all, s0, s1, s2, s3, p0, p1, p2, p3,
           qabuf, kac, vac, kan, van, vtac, vtan, oastage, ststage, oarecv, strecv, odone, acc_a,
           send_sem, recv_sem, load_sem, wsem, out_sem):
    ny, nx, kv, grp, dim = dims
    cp = ny * nx * CORES
    tb, ta = xb.shape[0], xa.shape[0]
    tq = tb // 2
    rows = grp * tq
    width = grp * dim
    pair = CORES * dim
    cb = kcb.shape[0]
    scale2 = dim ** -0.5 * LOG2E
    bf = jnp.bfloat16

    me = lax.axis_index("cp")
    c = lax.rem(me, CORES)
    x = lax.rem(me // CORES, nx)
    y = me // (CORES * nx)
    mine = y * CORES + c

    def dev(yy, xx, cc):
        return (yy * nx + xx) * CORES + cc

    def peer(h):
        return dev(h // CORES, x, lax.rem(h, CORES))

    def put(item, src, dst, target):
        pltpu.make_async_remote_copy(
            src_ref=src, dst_ref=dst, send_sem=send_sem.at[item], recv_sem=recv_sem.at[item],
            device_id={"cp": target}, device_id_type=MESH,
        ).start()

    def copy(src, dst, sem):
        pltpu.make_async_copy(src, dst, sem).start()

    def wait(ref, sem):
        pltpu.make_async_copy(ref, ref, sem).wait()

    def give(item, src, dst, target):
        @pl.when(target == me)
        def _():
            copy(src, dst, recv_sem.at[item])

        @pl.when(target != me)
        def _():
            put(item, src, dst, target)

    def wait_in(item, ref):
        wait(ref, recv_sem.at[item])

    def wait_out(item, ref):
        wait(ref, send_sem.at[item])

    KC, VC, Q, KN, VN, KAC, VAC, KAN, VAN, QA, QX, OB, OA, ST, OY = range(15)
    QS = 15
    AG = QS + ny

    barrier = pltpu.get_barrier_semaphore()

    def greet(d, _):
        pl.semaphore_signal(barrier, inc=1, device_id={"cp": d}, device_id_type=MESH)
        return 0

    raw = ((kcb, rkb, tkb), (vcb, rvb, tvb), (kca, rka, tka), (vca, rva, tva))
    for i, (src, dst, _) in enumerate(raw):
        copy(src, dst, load_sem.at[i])
    copy(xb, xs.at[pl.ds(0, tb), :], load_sem.at[4])
    copy(xa, xs.at[pl.ds(tb, ta), :], load_sem.at[4])

    q_steps, kv_steps = kv, kv // CORES

    def q_head(i):
        return lax.rem(mine + 1 + i, kv)

    def kv_pair(i):
        return lax.rem(y + 1 + i, ny)

    def load_q_cols(i, slot):
        copy(wq.at[:, pl.ds(pl.multiple_of(q_head(i) * width, width), width)], wbuf.at[slot], wsem.at[slot])

    def load_kv_cols(i, slot):
        cols = pl.ds(pl.multiple_of(kv_pair(i) * pair, pair), pair)
        copy(wk.at[:, cols], wbuf.at[slot, :, pl.ds(0, pair)], wsem.at[slot])
        copy(wv.at[:, cols], wbuf.at[slot, :, pl.ds(pair, pair)], wsem.at[slot])

    def load_cols(i):
        slot = lax.rem(i, SLOTS)

        @pl.when(i < kv_steps)
        def _():
            load_kv_cols(i, slot)

        @pl.when(jnp.logical_and(i >= kv_steps, i < kv_steps + q_steps))
        def _():
            load_q_cols(i - kv_steps, slot)

    for i in range(SLOTS - 1):
        load_cols(jnp.int32(i))
    lax.fori_loop(0, cp, greet, 0)
    for i, (_, dst, turned) in enumerate(raw):
        wait(dst, load_sem.at[i])
        turned[...] = jnp.transpose(dst[...], (1, 0, 2))
    pl.semaphore_wait(barrier, cp)

    def scatter(item, src, dst):
        def one(k, _):
            h = lax.rem(mine + k, kv)
            put(item, src.at[h], dst, peer(h))
            return 0

        lax.fori_loop(1, kv, one, 0)
        copy(src.at[mine], dst, recv_sem.at[item])

    c_rows = pl.ds(pl.multiple_of(c * cb, cb), cb)
    scatter(KC, tkb, kc.at[y, x, c_rows, :])
    scatter(VC, tvb, vc.at[y, x, c_rows, :])

    right = dev(y, lax.rem(x + 1, nx), c)
    left = dev(y, lax.rem(x + nx - 1, nx), c)
    x_left = lax.rem(x + nx - 1, nx)
    x_right = lax.rem(x + 1, nx)
    x_far = lax.rem(x + nx // 2, nx)
    lo, hi = pl.ds(0, ny // 2), pl.ds(ny // 2, ny // 2)

    def ag_sem(i, step, direction):
        return AG + i * 4 + step * 2 + direction

    def ring_first(i, buf):
        put(ag_sem(i, 0, 0), buf.at[:, x], buf.at[:, x], right)
        put(ag_sem(i, 0, 1), buf.at[:, x], buf.at[:, x], left)

    def ring_second(i, buf):
        wait_in(ag_sem(i, 0, 0), buf.at[:, x_left])
        put(ag_sem(i, 1, 0), buf.at[lo, x_left], buf.at[lo, x_left], right)
        wait_in(ag_sem(i, 0, 1), buf.at[:, x_right])
        put(ag_sem(i, 1, 1), buf.at[hi, x_right], buf.at[hi, x_right], left)

    def ring_last(i, buf):
        wait_in(ag_sem(i, 1, 0), buf.at[lo, x_far])
        wait_in(ag_sem(i, 1, 1), buf.at[hi, x_far])

    def ring_drain(i, buf):
        wait_out(ag_sem(i, 0, 0), buf.at[:, x])
        wait_out(ag_sem(i, 0, 1), buf.at[:, x])
        wait_out(ag_sem(i, 1, 0), buf.at[lo, x])
        wait_out(ag_sem(i, 1, 1), buf.at[hi, x])

    wait(xs, load_sem.at[4])
    b_rows, a_rows = pl.ds(0, tb), pl.ds(tb, ta)
    new_a = kv * ta
    col_a = pl.ds(pl.multiple_of(x * new_a, new_a), new_a)
    my_a = pl.ds(pl.multiple_of(x * new_a + mine * ta, ta), ta)

    def rope(t):
        t = t.astype(bf).astype(jnp.float32)
        return (t * cosf[...] + pltpu.roll(t, dim // 2, 1) * sinf[...]).astype(bf)

    def project(slot):
        return jnp.dot(xs[...], wbuf[slot], preferred_element_type=jnp.float32)

    def q_step(i, _):
        load_cols(kv_steps + i + SLOTS - 1)
        slot = lax.rem(kv_steps + i, SLOTS)
        wait(wbuf.at[slot], wsem.at[slot])
        h = q_head(i)
        lin = project(slot)
        for g in range(grp):
            cols = slice(g * dim, (g + 1) * dim)
            qsend[h, :, cols] = rope(lin[:, cols])
        give(QS + lax.rem(y - h // CORES + ny, ny), qsend.at[h, b_rows], qbuf.at[mine], peer(h))
        give(QA, qsend.at[h, a_rows], qabuf.at[my_a, :], peer(h))
        return 0

    def kv_step(i, _):
        load_cols(i + SLOTS - 1)
        slot = lax.rem(i, SLOTS)
        wait(wbuf.at[slot], wsem.at[slot])
        p = kv_pair(i)
        lin = project(slot)
        for g in range(CORES):
            cols = slice(g * dim, (g + 1) * dim)
            kvsend[p, :, cols] = rope(lin[:, cols])
        kvsend[p, :, pair:2 * pair] = lin[:, pair:2 * pair].astype(bf)
        for j, (nb, na) in enumerate(((nkb, nka), (nvb, nva))):
            for g in range(CORES):
                cols = pl.ds(j * pair + g * dim, dim)
                copy(kvsend.at[p, b_rows, cols], nb.at[p * CORES + g], out_sem.at[2 * j])
                copy(kvsend.at[p, a_rows, cols], na.at[p * CORES + g], out_sem.at[2 * j + 1])
        n_rows = pl.ds(pl.multiple_of(c * tb, tb), tb)
        s_rows = pl.ds(pl.multiple_of(mine * ta, ta), ta)
        for g in range(CORES):
            for j, (ib, db, ia, da) in enumerate(((KN, kn, KAN, kan), (VN, vn, VAN, van))):
                cols = pl.ds(j * pair + g * dim, dim)
                give(ib, kvsend.at[p, b_rows, cols], db.at[y, x, n_rows, :], dev(p, x, g))
                give(ia, kvsend.at[p, a_rows, cols], da.at[s_rows, :], dev(p, x, g))
        return 0

    lax.fori_loop(0, kv_steps, kv_step, 0)
    wait_in(KC, kc.at[:, x])
    ring_first(0, kc)
    wait_in(VC, vc.at[:, x])
    ring_first(1, vc)
    lax.fori_loop(0, q_steps - 1, q_step, 0)
    ring_second(0, kc)
    ring_second(1, vc)
    lax.fori_loop(q_steps - 1, q_steps, q_step, 0)
    wait_in(KN, kn.at[:, x])
    ring_first(2, kn)
    wait_in(VN, vn.at[:, x])
    ring_first(3, vn)
    scatter(KAC, tka, kac.at[mine])
    scatter(VAC, tva, vac.at[mine])

    s_refs, p_refs = (s0, s1, s2, s3), (p0, p1, p2, p3)
    blk = s0.shape[0]
    tiles = range(4)

    def scores(t, keys, queries):
        s = qk(keys, queries)
        s_refs[t][...] = s
        return fold(s, jnp.maximum)

    def highest(m, top8):
        m_new = jnp.maximum(m, jnp.max(top8, axis=0, keepdims=True))
        return m_new, jnp.exp2((m - m_new) * scale2)

    def expo(t, m, l8, top8):
        m_new, alpha = highest(m, top8)
        l8 = l8 * alpha
        for r in range(0, blk, 16):
            e = jnp.exp2((s_refs[t][pl.ds(r, 16), :] - m_new) * scale2)
            p_refs[t][pl.ds(r, 16), :] = e.astype(bf)
            l8 = l8 + fold(e, jnp.add)
        return m_new, l8, alpha

    def values(t, vt, alpha, acc_ref):
        acc_ref[...] = acc_ref[...] * alpha + jnp.dot(vt, p_refs[t][...], preferred_element_type=jnp.float32)

    def step(carry, before, now, k_after, q_after, acc_before, accs):
        m, l, top = list(carry[0:4]), list(carry[4:8]), list(carry[8:12])
        values(3, before, carry[12], acc_before)
        for t in tiles:
            m[t], l[t], alpha = expo(t, m[t], l[t], top[t])
            top[t] = scores(t, k_after, q_after(t))
            if t < 3:
                values(t, now, alpha, accs[t])
        return tuple(m + l + top) + (alpha,)

    neg, zero = jnp.full((1, rows), NEG, jnp.float32), jnp.zeros((8, rows), jnp.float32)
    one = jnp.ones((1, rows), jnp.float32)

    def total(l8):
        return jnp.sum(l8, axis=0, keepdims=True)

    def others(ref):
        return ref.at[pl.ds(0, (nx - 1) * new_a), :]

    def token_of_lane(shape):
        return lax.rem(lax.broadcasted_iota(jnp.int32, shape, 1), tq)

    def turn(first, end, dst, block):
        n = 2 if first % 4 or end % 4 else 4

        def some(i, _):
            for k in range(n):
                dst[n * i + k] = block(n * i + k).T
            return 0

        lax.fori_loop(first // n, end // n, some, 0)

    blocks = vtc.shape[0]
    per_col = blocks // nx
    part = ny // per_col
    acc[...] = jnp.zeros_like(acc)
    p3[...] = jnp.zeros_like(p3)

    def row_of(i):
        return lax.rem(y + ny - i, ny)

    def arrive_q(i):
        yy = row_of(i)
        wait_in(QS + (ny - i) % ny, qbuf.at[pl.ds(yy * CORES, CORES)])
        for t in tiles:
            u, half = yy * CORES + t // 2, t % 2
            for g in range(grp):
                q_all[4 * yy + t, pl.ds(g * tq, tq), :] = qbuf[u, pl.ds(half * tq, tq), pl.ds(g * dim, dim)]

    def cached(buf, j):
        i = j // per_col
        xx = jnp.where(i == 0, x, jnp.where(i == 1, x_left, jnp.where(i == 2, x_right, x_far)))
        return buf[pl.ds(lax.rem(j, per_col) * part, part), xx].reshape(blk, dim)

    def turn_c(first, end):
        turn(first, end, vtc, lambda j: cached(vc, j))

    near = blocks - per_col
    arrive_q(0)
    turn_c(0, near)

    def step_c(i, carry):
        yy, j = row_of(i // blocks), lax.rem(i, blocks)
        before, after = lax.max(i - 1, 0), lax.min(i + 1, ny * blocks - 1)
        y_before, y_after = row_of(before // blocks), row_of(after // blocks)
        start = j == 0
        m = tuple(jnp.where(start, NEG, v) for v in carry[0:4])
        l = tuple(jnp.where(start, 0.0, v) for v in carry[4:8])
        out = step(
            m + l + carry[8:], vtc[lax.rem(before, blocks)], vtc[j], cached(kc, lax.rem(after, blocks)),
            lambda t: q_all[4 * y_after + t], acc.at[4 * y_before + 3], [acc.at[4 * yy + t] for t in tiles])
        for t in tiles:
            m_all[4 * yy + t, 0:1, :] = out[t]
            l_all[4 * yy + t] = out[4 + t]
        return out

    tops = tuple(scores(t, cached(kc, jnp.int32(0)), q_all[4 * y + t]) for t in tiles)
    carry = (neg,) * 4 + (zero,) * 4 + tops + (one,)
    carry = lax.fori_loop(0, near - 1, step_c, carry)
    ring_last(0, kc)
    ring_last(1, vc)
    turn_c(near, blocks)
    carry = lax.fori_loop(near - 1, blocks - 1, step_c, carry)
    arrive_q(1)
    carry = lax.fori_loop(blocks - 1, 2 * blocks - 1, step_c, carry)
    wait_in(QA, qabuf.at[col_a, :])

    def pass_qa(k, _):
        put(QX, qabuf.at[col_a, :], qabuf.at[col_a, :], dev(y, lax.rem(x + k, nx), c))
        return 0

    lax.fori_loop(1, nx, pass_qa, 0)
    arrive_q(2)
    carry = lax.fori_loop(2 * blocks - 1, 3 * blocks - 1, step_c, carry)
    arrive_q(3)
    ring_second(2, kn)
    ring_second(3, vn)
    carry = lax.fori_loop(3 * blocks - 1, 4 * blocks, step_c, carry)
    values(3, vtc[blocks - 1], carry[12], acc.at[4 * row_of(ny - 1) + 3])

    ring_last(2, kn)
    ring_last(3, vn)
    turn(0, ny * nx, vtn, lambda j: vn[j // nx, lax.rem(j, nx)])

    def new_keys(j):
        return kn[j // nx, lax.rem(j, nx)]

    def row_n(i):
        return lax.rem(y + ny + jnp.where(c == 0, 1 + i, ny - 1 - i), ny)

    def rows_n(i, tops):
        yy, y_after = row_n(i), row_n(lax.min(i + 1, ny - 1))
        last = yy * nx + x
        accs = [acc.at[4 * yy + t] for t in tiles]
        p3[...] = jnp.zeros_like(p3)

        def step_n(j, carry):
            return step(carry, vtn[lax.max(j - 1, 0)], vtn[j], new_keys(j + 1), lambda t: q_all[4 * yy + t],
                        accs[3], accs)

        state = tuple(m_all[4 * yy + t, 0:1, :] for t in tiles) + tuple(l_all[4 * yy + t] for t in tiles)
        carry = lax.fori_loop(0, last, step_n, state + tuple(tops) + (one,))
        values(3, vtn[lax.max(last - 1, 0)], carry[12], accs[3])
        tops = []
        for t in tiles:
            seen = (t + 1) * tq
            tri = lax.broadcasted_iota(jnp.int32, (tq, rows), 0) <= token_of_lane((tq, rows))
            s = jnp.where(tri, s_refs[t][pl.ds(t * tq, tq), :], NEG)
            s_refs[t][pl.ds(t * tq, tq), :] = s
            top8 = fold(s, jnp.maximum)
            if t:
                top8 = jnp.maximum(top8, fold(s_refs[t][pl.ds(0, t * tq), :], jnp.maximum))
            m_new, alpha = highest(carry[t], top8)
            l8 = carry[4 + t] * alpha
            for r in range(0, seen, 16):
                e = jnp.exp2((s_refs[t][pl.ds(r, 16), :] - m_new) * scale2)
                p_refs[t][pl.ds(r, 16), :] = e.astype(bf)
                l8 = l8 + fold(e, jnp.add)
            tops.append(scores(t, new_keys(0), q_all[4 * y_after + t]))
            pv = jnp.dot(vtn[last, :, pl.ds(0, seen)], p_refs[t][pl.ds(0, seen), :], preferred_element_type=jnp.float32)
            o = (accs[t][...] * alpha + pv) * (1.0 / total(l8))
            for g in range(grp):
                obuf[yy * CORES + t // 2, pl.ds(t % 2 * tq, tq), pl.ds(g * dim, dim)] = (
                    o[:, g * tq:(g + 1) * tq].T.astype(bf))
        for cc in range(CORES):
            u = yy * CORES + cc
            give(OB, obuf.at[u], ob.at[:, pl.ds(pl.multiple_of(mine * width, width), width)], peer(u))
        return tuple(tops)

    tops = tuple(scores(t, new_keys(0), q_all[4 * row_n(0) + t]) for t in tiles)
    tops = lax.fori_loop(0, 1, rows_n, tops)

    wait_in(QX, others(qabuf))
    wait_in(KAC, kac)
    wait_in(VAC, vac)
    wait_in(KAN, kan)
    wait_in(VAN, van)
    turn(0, kv, vtac, lambda j: vac[j])
    vtan[...] = van[...].T
    for t in tiles:
        for g in range(grp):
            q_a[t, pl.ds(g * tq, tq), :] = qabuf[pl.ds(t * tq, tq), pl.ds(g * dim, dim)]
    acc_a[...] = jnp.zeros_like(acc_a)
    p3[...] = jnp.zeros_like(p3)
    accs_a = [acc_a.at[t] for t in tiles]

    def step_a(j, carry):
        return step(carry, vtac[lax.max(j - 1, 0)], vtac[j], kac[j + 1], lambda t: q_a[t], accs_a[3], accs_a)

    tops = tuple(scores(t, kac[0], q_a[t]) for t in tiles)
    carry = lax.fori_loop(0, kv - 1, step_a, (neg,) * 4 + (zero,) * 4 + tops + (one,))
    values(3, vtac[kv - 2], carry[12], accs_a[3])

    def token_a(r, xx):
        holder = dev(r // (CORES * ta), xx, lax.rem(r // ta, CORES))
        return holder * ta + lax.rem(r, ta)

    pos_k = token_a(lax.broadcasted_iota(jnp.int32, (new_a, rows), 0), x)
    place_q = token_of_lane((new_a, rows))
    row = lax.broadcasted_iota(jnp.int32, (dim, tq), 0)
    for t in tiles:
        m, l, alpha = expo(t, carry[t], carry[4 + t], carry[8 + t])
        values(t, vtac[kv - 1], alpha, accs_a[t])
        s = jnp.where(pos_k <= token_a(place_q, t), qk(kan[...], q_a[t]), NEG)
        m, l = soft_step(scale2, s, vtan[...], m, total(l), accs_a[t])
        stat = jnp.zeros((dim, tq), jnp.float32)
        for g in range(grp):
            cols = slice(g * tq, (g + 1) * tq)
            oastage[pl.ds(t * tq, tq), pl.ds(g * dim, dim)] = acc_a[t, :, cols].T
            stat = jnp.where(row == g, m[:, cols], stat)
            stat = jnp.where(row == grp + g, l[:, cols], stat)
        ststage[pl.ds(t * tq, tq), :] = stat.T

    def give_a(k, _):
        xx = lax.rem(x + k, nx)
        r = pl.ds(pl.multiple_of(xx * new_a, new_a), new_a)
        put(OA, oastage.at[r, :], oarecv.at[x], dev(y, xx, c))
        put(ST, ststage.at[r, :], strecv.at[x], dev(y, xx, c))
        return 0

    lax.fori_loop(1, nx, give_a, 0)
    copy(oastage.at[col_a, :], oarecv.at[x], recv_sem.at[OA])
    copy(ststage.at[col_a, :], strecv.at[x], recv_sem.at[ST])

    tops = tuple(scores(t, new_keys(0), q_all[4 * row_n(1) + t]) for t in tiles)
    tops = lax.fori_loop(1, ny - 1, rows_n, tops)

    wait_in(OA, oarecv)
    wait_in(ST, strecv)
    for g in range(grp):
        cols = pl.ds(g * dim, dim)
        ms = [strecv[i, :, g:g + 1] for i in range(nx)]
        top = functools.reduce(jnp.maximum, ms)
        num = jnp.zeros((new_a, dim), jnp.float32)
        den = jnp.zeros((new_a, 1), jnp.float32)
        for i in range(nx):
            w = jnp.exp2((ms[i] - top) * scale2)
            num = num + w * oarecv[i, :, cols]
            den = den + w * strecv[i, :, grp + g:grp + g + 1]
        odone[:, cols] = (num / den).astype(bf)

    def home_a(r, _):
        give(OY, odone.at[pl.ds(pl.multiple_of(r * ta, ta), ta), :],
             oa.at[:, pl.ds(pl.multiple_of(mine * width, width), width)], peer(r))
        return 0

    lax.fori_loop(0, kv, home_a, 0)
    lax.fori_loop(ny - 1, ny, rows_n, tops)

    wait_in(OB, ob)
    wait_in(OY, oa)
    for i, ref in enumerate((nkb, nka, nvb, nva)):
        wait(ref, out_sem.at[i])
    most = pl.ds(0, kv - 1)
    for item, ref in ((KC, tkb), (VC, tvb), (KAC, tka), (VAC, tva), (OB, obuf)):
        wait_out(item, ref.at[most])
    wait_out(QS, qbuf.at[pl.ds(0, CORES - 1)])
    for i in range(1, ny):
        wait_out(QS + i, qbuf.at[pl.ds(0, CORES)])
    for item, ref in ((KN, qbuf), (VN, qbuf)):
        wait_out(item, ref.at[most, :, pl.ds(0, dim)])
    for item, ref in ((KAN, kan), (VAN, van)):
        wait_out(item, ref.at[pl.ds(0, (kv - 1) * ta), :])
    wait_out(QA, qabuf.at[pl.ds(0, (kv - 1) * ta), :])
    wait_out(OY, odone.at[pl.ds(0, (kv - 1) * ta), :])
    wait_out(QX, others(qabuf))
    wait_out(OA, oarecv.at[pl.ds(0, nx - 1)])
    wait_out(ST, strecv.at[pl.ds(0, nx - 1)])
    ring_drain(0, kc)
    ring_drain(1, vc)
    ring_drain(2, kn)
    ring_drain(3, vn)


def attention(cp, xb, xa, cosf, sinf, wq, wk, wv, kcb, vcb, kca, vca):
    kv, dim = kcb.shape[1:]
    ny, nx = kv // CORES, cp // kv
    assert nx * CORES == kv and ny * nx * CORES == cp and ny == nx
    grp = wq.shape[1] // (kv * dim)
    tb, ta, cb, ca, model = xb.shape[0], xa.shape[0], kcb.shape[0], kca.shape[0], xb.shape[1]
    tq = tb // 2
    rows, width = grp * tq, grp * dim
    blk = CORES * tb
    assert blk == ca and (ny * CORES * cb) % (2 * blk) == 0 and (cp * ta) % (2 * tq) == 0
    assert width == 2 * CORES * dim and kv * ta == tq and nx == 4 and CORES == 2
    bf, f32 = jnp.bfloat16, jnp.float32
    vm = pltpu.VMEM
    scratch = [
        vm((tb + ta, model), bf),
        vm((SLOTS, model, width), bf),
        vm((kv, tb + ta, width), bf),
        vm((ny, tb + ta, width), bf),
        vm(kcb.shape, bf), vm(vcb.shape, bf), vm(kca.shape, bf), vm(vca.shape, bf),
        vm((kv, cb, dim), bf), vm((kv, cb, dim), bf), vm((kv, ca, dim), bf), vm((kv, ca, dim), bf),
        vm((kv, tb, width), bf),
        vm((ny, nx, CORES * cb, dim), bf),
        vm((ny, nx, CORES * cb, dim), bf),
        vm((ny, nx, blk, dim), bf),
        vm((ny, nx, blk, dim), bf),
        vm((cp * cb // blk, dim, blk), bf),
        vm((ny * nx, dim, blk), bf),
        vm((kv, tb, width), bf),
        vm((2 * kv, dim, rows), f32),
        vm((2 * kv, 8, rows), f32),
        vm((2 * kv, 8, rows), f32),
        vm((4, rows, dim), bf),
        vm((2 * kv, rows, dim), bf),
        vm((blk, rows), f32), vm((blk, rows), f32), vm((blk, rows), f32), vm((blk, rows), f32),
        vm((blk, rows), bf), vm((blk, rows), bf), vm((blk, rows), bf), vm((blk, rows), bf),
        vm((cp * ta, width), bf),
        vm((kv, ca, dim), bf),
        vm((kv, ca, dim), bf),
        vm((kv * ta, dim), bf),
        vm((kv * ta, dim), bf),
        vm((kv, dim, ca), bf),
        vm((dim, kv * ta), bf),
        vm((cp * ta, width), f32),
        vm((cp * ta, dim), f32),
        vm((nx, kv * ta, width), f32),
        vm((nx, kv * ta, dim), f32),
        vm((kv * ta, width), bf),
        vm((4, dim, rows), f32),
        pltpu.SemaphoreType.DMA((15 + ny + 16,)),
        pltpu.SemaphoreType.DMA((15 + ny + 16,)),
        pltpu.SemaphoreType.DMA((5,)),
        pltpu.SemaphoreType.DMA((SLOTS,)),
        pltpu.SemaphoreType.DMA((4,)),
    ]
    any_spec = pl.BlockSpec(memory_space=pl.ANY)
    vmem_spec = pl.BlockSpec(memory_space=pltpu.VMEM)
    shape = jax.ShapeDtypeStruct
    return pl.pallas_call(
        functools.partial(kernel, (ny, nx, kv, grp, dim)),
        out_shape=(shape((tb, kv * width), bf), shape((ta, kv * width), bf),
                   shape((kv, tb, dim), bf), shape((kv, tb, dim), bf),
                   shape((kv, ta, dim), bf), shape((kv, ta, dim), bf)),
        in_specs=[any_spec, any_spec, vmem_spec, vmem_spec] + [any_spec] * 7,
        out_specs=(any_spec,) * 6,
        scratch_shapes=scratch,
        compiler_params=pltpu.CompilerParams(
            collective_id=0, has_side_effects=True, vmem_limit_bytes=VMEM_LIMIT),
        name="attend",
    )(xb, xa, cosf, sinf, wq, wk, wv, kcb, vcb, kca, vca)


def out_kernel(ob, oa, w, kb, vb, ka, va, yb, ya, nkb, nvb, nka, nva, o, wbuf, ybuf, *rest):
    new, turned, (wsem, osem, nsem, ysem) = rest[:4], rest[4:8], rest[8:]
    tb, ta = ob.shape[0], oa.shape[0]
    cols = wbuf.shape[2]
    steps = w.shape[1] // cols
    b_rows, a_rows = pl.ds(0, tb), pl.ds(tb, ta)

    def copy(src, dst, sem):
        pltpu.make_async_copy(src, dst, sem).start()

    def wait(ref, sem):
        pltpu.make_async_copy(ref, ref, sem).wait()

    def span(i):
        return pl.ds(pl.multiple_of(i * cols, cols), cols)

    def load(i):
        copy(w.at[:, span(i)], wbuf.at[lax.rem(i, SLOTS)], wsem.at[lax.rem(i, SLOTS)])

    copy(ob, o.at[b_rows, :], osem)
    copy(oa, o.at[a_rows, :], osem)
    for i in range(min(SLOTS - 1, steps)):
        load(i)
    for i, (src, dst) in enumerate(zip((kb, vb, ka, va), new)):
        copy(src, dst, nsem.at[i])
    wait(o, osem)

    def step(i, _):
        @pl.when(i + SLOTS - 1 < steps)
        def _():
            load(i + SLOTS - 1)

        slot = lax.rem(i, SLOTS)
        wait(wbuf.at[slot], wsem.at[slot])
        ybuf[i] = jnp.dot(o[...], wbuf[slot], preferred_element_type=jnp.float32).astype(ybuf.dtype)
        copy(ybuf.at[i, b_rows, :], yb.at[:, span(i)], ysem.at[0])
        copy(ybuf.at[i, a_rows, :], ya.at[:, span(i)], ysem.at[1])
        return 0

    lax.fori_loop(0, steps, step, 0)
    for i, (src, dst, out) in enumerate(zip(new, turned, (nkb, nvb, nka, nva))):
        wait(src, nsem.at[i])
        dst[...] = jnp.transpose(src[...], (1, 0, 2))
        copy(dst, out, nsem.at[i])
    wait(yb, ysem.at[0])
    wait(ya, ysem.at[1])
    for i, out in enumerate((nkb, nvb, nka, nva)):
        wait(out, nsem.at[i])


def output_projection(ob, oa, w, *new):
    (tb, inner), ta, model = ob.shape, oa.shape[0], w.shape[1]
    cols = min(512, model)
    shape = jax.ShapeDtypeStruct
    bf, vm, dma = ob.dtype, pltpu.VMEM, pltpu.SemaphoreType.DMA
    turned = [(t.shape[1], t.shape[0], t.shape[2]) for t in new]
    any_spec = pl.BlockSpec(memory_space=pl.ANY)
    return pl.pallas_call(
        out_kernel,
        out_shape=[shape((tb, model), bf), shape((ta, model), bf)] + [shape(t, bf) for t in turned],
        in_specs=[any_spec] * 7,
        out_specs=[any_spec] * 6,
        scratch_shapes=[vm((tb + ta, inner), bf), vm((SLOTS, inner, cols), bf), vm((model // cols, tb + ta, cols), bf)]
        + [vm(t.shape, bf) for t in new] + [vm(t, bf) for t in turned] + [dma((SLOTS,)), dma, dma((4,)), dma((2,))],
        compiler_params=pltpu.CompilerParams(vmem_limit_bytes=VMEM_LIMIT),
        name="project_out",
    )(ob, oa, w, *new)


def solution(mesh):
    cp_size = mesh.shape["cp"]

    def local_step(x_a, kc_a, vc_a, x_b, kc_b, vc_b, w_q, w_k, w_v, w_o):
        ta, tb = x_a.shape[0], x_b.shape[0]
        kv, dim = kc_a.shape[1:]
        me = lax.axis_index("cp")
        pos_a = kc_a.shape[0] * cp_size + me * ta + jnp.arange(ta)
        pos_b = kc_b.shape[0] * cp_size + me * tb + jnp.arange(tb)
        cosf, sinf = rope_tables(jnp.concatenate([pos_b, pos_a]), dim)
        o_b, o_a, k_b, v_b, k_a, v_a = attention(cp_size, x_b, x_a, cosf, sinf, w_q, w_k, w_v, kc_b, vc_b, kc_a, vc_a)
        y_b, y_a, k_b, v_b, k_a, v_a = output_projection(o_b, o_a, w_o, k_b, v_b, k_a, v_a)
        return y_a, k_a, v_a, y_b, k_b, v_b

    row_spec = P(("dp", "cp"), None)
    kv_spec = P(("dp", "cp"), None, None)
    full_spec = P()
    return jax.shard_map(
        local_step, mesh=mesh,
        in_specs=(row_spec, kv_spec, kv_spec, row_spec, kv_spec, kv_spec, full_spec, full_spec, full_spec, full_spec),
        out_specs=(row_spec, kv_spec, kv_spec, row_spec, kv_spec, kv_spec), check_vma=False)
```

```python
import functools

import jax
import jax.numpy as jnp
from jax import lax
from jax.experimental import pallas as pl
from jax.experimental.pallas import tpu as pltpu
from jax.sharding import PartitionSpec as P

ROPE_BASE = 500000
LOG2E = 1.4426950408889634
NEG = float(jnp.finfo(jnp.float32).min)
MESH = pl.DeviceIdType.MESH
CORES = 2
VMEM_LIMIT = 62 * 1024 * 1024
SLOTS = 3


def rope_tables(positions, head_dim):
    half_dim = head_dim // 2
    inv_freq = jnp.power(jnp.float32(ROPE_BASE), jnp.arange(half_dim, dtype=jnp.float32) * (-2.0 / head_dim))
    angles = positions.astype(jnp.float32)[:, None] * inv_freq[None, :]
    cos_ang, sin_ang = jnp.cos(angles), jnp.sin(angles)
    return jnp.concatenate([cos_ang, cos_ang], axis=1), jnp.concatenate([-sin_ang, sin_ang], axis=1)


def qk(keys, queries):
    return lax.dot_general(keys, queries, (((1,), (1,)), ((), ())), preferred_element_type=jnp.float32)


def fold(s, op):
    return functools.reduce(op, [s[i:i + 8] for i in range(0, s.shape[0], 8)])


def soft_step(scale2, s, vt, m, l, acc_ref):
    m_new = jnp.maximum(m, jnp.max(s, axis=0, keepdims=True))
    alpha = jnp.exp2((m - m_new) * scale2)
    e = jnp.exp2((s - m_new) * scale2)
    l_new = l * alpha + jnp.sum(e, axis=0, keepdims=True)
    pv = jnp.dot(vt, e.astype(jnp.bfloat16), preferred_element_type=jnp.float32)
    acc_ref[...] = acc_ref[...] * alpha + pv
    return m_new, l_new


def kernel(dims, xb, xa, cosf, sinf, wq, wk, wv, kcb, vcb, kca, vca, ob, oa, nkb, nvb, nka, nva,
           xs, wbuf, qsend, kvsend, rkb, rvb, rka, rva, tkb, tvb, tka, tva,
           qbuf, kc, vc, kn, vn, vtc, vtn, obuf, acc, m_all, l_all, q_a, q_all, s0, s1, s2, s3, p0, p1, p2, p3,
           qabuf, kac, vac, kan, van, vtac, vtan, oastage, ststage, oarecv, strecv, odone, acc_a,
           send_sem, recv_sem, load_sem, wsem, out_sem):
    ny, nx, kv, grp, dim = dims
    cp = ny * nx * CORES
    tb, ta = xb.shape[0], xa.shape[0]
    tq = tb // 2
    rows = grp * tq
    width = grp * dim
    pair = CORES * dim
    cb = kcb.shape[0]
    scale2 = dim ** -0.5 * LOG2E
    bf = jnp.bfloat16

    me = lax.axis_index("cp")
    c = lax.rem(me, CORES)
    x = lax.rem(me // CORES, nx)
    y = me // (CORES * nx)
    mine = y * CORES + c

    def dev(yy, xx, cc):
        return (yy * nx + xx) * CORES + cc

    def peer(h):
        return dev(h // CORES, x, lax.rem(h, CORES))

    def put(item, src, dst, target):
        pltpu.make_async_remote_copy(
            src_ref=src, dst_ref=dst, send_sem=send_sem.at[item], recv_sem=recv_sem.at[item],
            device_id={"cp": target}, device_id_type=MESH,
        ).start()

    def copy(src, dst, sem):
        pltpu.make_async_copy(src, dst, sem).start()

    def wait(ref, sem):
        pltpu.make_async_copy(ref, ref, sem).wait()

    def give(item, src, dst, target):
        @pl.when(target == me)
        def _():
            copy(src, dst, recv_sem.at[item])

        @pl.when(target != me)
        def _():
            put(item, src, dst, target)

    def wait_in(item, ref):
        wait(ref, recv_sem.at[item])

    def wait_out(item, ref):
        wait(ref, send_sem.at[item])

    KC, VC, Q, KN, VN, KAC, VAC, KAN, VAN, QA, QX, OB, OA, ST, OY = range(15)
    QS = 15
    AG = QS + ny

    barrier = pltpu.get_barrier_semaphore()

    def greet(d, _):
        pl.semaphore_signal(barrier, inc=1, device_id={"cp": d}, device_id_type=MESH)
        return 0

    raw = ((kcb, rkb, tkb), (vcb, rvb, tvb), (kca, rka, tka), (vca, rva, tva))
    for i, (src, dst, _) in enumerate(raw):
        copy(src, dst, load_sem.at[i])
    copy(xb, xs.at[pl.ds(0, tb), :], load_sem.at[4])
    copy(xa, xs.at[pl.ds(tb, ta), :], load_sem.at[4])

    q_steps, kv_steps = kv, kv // CORES

    def q_head(i):
        return lax.rem(mine + 1 + i, kv)

    def kv_pair(i):
        return lax.rem(y + 1 + i, ny)

    def load_q_cols(i, slot):
        copy(wq.at[:, pl.ds(pl.multiple_of(q_head(i) * width, width), width)], wbuf.at[slot], wsem.at[slot])

    def load_kv_cols(i, slot):
        cols = pl.ds(pl.multiple_of(kv_pair(i) * pair, pair), pair)
        copy(wk.at[:, cols], wbuf.at[slot, :, pl.ds(0, pair)], wsem.at[slot])
        copy(wv.at[:, cols], wbuf.at[slot, :, pl.ds(pair, pair)], wsem.at[slot])

    def load_cols(i):
        slot = lax.rem(i, SLOTS)

        @pl.when(i < kv_steps)
        def _():
            load_kv_cols(i, slot)

        @pl.when(jnp.logical_and(i >= kv_steps, i < kv_steps + q_steps))
        def _():
            load_q_cols(i - kv_steps, slot)

    for i in range(SLOTS - 1):
        load_cols(jnp.int32(i))
    lax.fori_loop(0, cp, greet, 0)
    for i, (_, dst, turned) in enumerate(raw):
        wait(dst, load_sem.at[i])
        turned[...] = jnp.transpose(dst[...], (1, 0, 2))
    pl.semaphore_wait(barrier, cp)

    def scatter(item, src, dst):
        def one(k, _):
            h = lax.rem(mine + k, kv)
            put(item, src.at[h], dst, peer(h))
            return 0

        lax.fori_loop(1, kv, one, 0)
        copy(src.at[mine], dst, recv_sem.at[item])

    c_rows = pl.ds(pl.multiple_of(c * cb, cb), cb)
    scatter(KC, tkb, kc.at[y, x, c_rows, :])
    scatter(VC, tvb, vc.at[y, x, c_rows, :])

    right = dev(y, lax.rem(x + 1, nx), c)
    left = dev(y, lax.rem(x + nx - 1, nx), c)
    x_left = lax.rem(x + nx - 1, nx)
    x_right = lax.rem(x + 1, nx)
    x_far = lax.rem(x + nx // 2, nx)
    lo, hi = pl.ds(0, ny // 2), pl.ds(ny // 2, ny // 2)

    def ag_sem(i, step, direction):
        return AG + i * 4 + step * 2 + direction

    def ring_first(i, buf):
        put(ag_sem(i, 0, 0), buf.at[:, x], buf.at[:, x], right)
        put(ag_sem(i, 0, 1), buf.at[:, x], buf.at[:, x], left)

    def ring_second(i, buf):
        wait_in(ag_sem(i, 0, 0), buf.at[:, x_left])
        put(ag_sem(i, 1, 0), buf.at[lo, x_left], buf.at[lo, x_left], right)
        wait_in(ag_sem(i, 0, 1), buf.at[:, x_right])
        put(ag_sem(i, 1, 1), buf.at[hi, x_right], buf.at[hi, x_right], left)

    def ring_last(i, buf):
        wait_in(ag_sem(i, 1, 0), buf.at[lo, x_far])
        wait_in(ag_sem(i, 1, 1), buf.at[hi, x_far])

    def ring_drain(i, buf):
        wait_out(ag_sem(i, 0, 0), buf.at[:, x])
        wait_out(ag_sem(i, 0, 1), buf.at[:, x])
        wait_out(ag_sem(i, 1, 0), buf.at[lo, x])
        wait_out(ag_sem(i, 1, 1), buf.at[hi, x])

    wait(xs, load_sem.at[4])
    b_rows, a_rows = pl.ds(0, tb), pl.ds(tb, ta)
    new_a = kv * ta
    col_a = pl.ds(pl.multiple_of(x * new_a, new_a), new_a)
    my_a = pl.ds(pl.multiple_of(x * new_a + mine * ta, ta), ta)

    def rope(t):
        t = t.astype(bf).astype(jnp.float32)
        return (t * cosf[...] + pltpu.roll(t, dim // 2, 1) * sinf[...]).astype(bf)

    def project(slot):
        return jnp.dot(xs[...], wbuf[slot], preferred_element_type=jnp.float32)

    def q_step(i, _):
        load_cols(kv_steps + i + SLOTS - 1)
        slot = lax.rem(kv_steps + i, SLOTS)
        wait(wbuf.at[slot], wsem.at[slot])
        h = q_head(i)
        lin = project(slot)
        for g in range(grp):
            cols = slice(g * dim, (g + 1) * dim)
            qsend[h, :, cols] = rope(lin[:, cols])
        give(QS + lax.rem(y - h // CORES + ny, ny), qsend.at[h, b_rows], qbuf.at[mine], peer(h))
        give(QA, qsend.at[h, a_rows], qabuf.at[my_a, :], peer(h))
        return 0

    def kv_step(i, _):
        load_cols(i + SLOTS - 1)
        slot = lax.rem(i, SLOTS)
        wait(wbuf.at[slot], wsem.at[slot])
        p = kv_pair(i)
        lin = project(slot)
        for g in range(CORES):
            cols = slice(g * dim, (g + 1) * dim)
            kvsend[p, :, cols] = rope(lin[:, cols])
        kvsend[p, :, pair:2 * pair] = lin[:, pair:2 * pair].astype(bf)
        for j, (nb, na) in enumerate(((nkb, nka), (nvb, nva))):
            for g in range(CORES):
                cols = pl.ds(j * pair + g * dim, dim)
                copy(kvsend.at[p, b_rows, cols], nb.at[p * CORES + g], out_sem.at[2 * j])
                copy(kvsend.at[p, a_rows, cols], na.at[p * CORES + g], out_sem.at[2 * j + 1])
        n_rows = pl.ds(pl.multiple_of(c * tb, tb), tb)
        s_rows = pl.ds(pl.multiple_of(mine * ta, ta), ta)
        for g in range(CORES):
            for j, (ib, db, ia, da) in enumerate(((KN, kn, KAN, kan), (VN, vn, VAN, van))):
                cols = pl.ds(j * pair + g * dim, dim)
                give(ib, kvsend.at[p, b_rows, cols], db.at[y, x, n_rows, :], dev(p, x, g))
                give(ia, kvsend.at[p, a_rows, cols], da.at[s_rows, :], dev(p, x, g))
        return 0

    lax.fori_loop(0, kv_steps, kv_step, 0)
    wait_in(KC, kc.at[:, x])
    ring_first(0, kc)
    wait_in(VC, vc.at[:, x])
    ring_first(1, vc)
    lax.fori_loop(0, q_steps - 1, q_step, 0)
    ring_second(0, kc)
    ring_second(1, vc)
    lax.fori_loop(q_steps - 1, q_steps, q_step, 0)
    wait_in(KN, kn.at[:, x])
    ring_first(2, kn)
    wait_in(VN, vn.at[:, x])
    ring_first(3, vn)
    scatter(KAC, tka, kac.at[mine])
    scatter(VAC, tva, vac.at[mine])

    s_refs, p_refs = (s0, s1, s2, s3), (p0, p1, p2, p3)
    blk = s0.shape[0]
    tiles = range(4)

    def scores(t, keys, queries):
        s = qk(keys, queries)
        s_refs[t][...] = s
        return fold(s, jnp.maximum)

    def highest(m, top8):
        m_new = jnp.maximum(m, jnp.max(top8, axis=0, keepdims=True))
        return m_new, jnp.exp2((m - m_new) * scale2)

    def expo(t, m, l8, top8):
        m_new, alpha = highest(m, top8)
        l8 = l8 * alpha
        for r in range(0, blk, 16):
            e = jnp.exp2((s_refs[t][pl.ds(r, 16), :] - m_new) * scale2)
            p_refs[t][pl.ds(r, 16), :] = e.astype(bf)
            l8 = l8 + fold(e, jnp.add)
        return m_new, l8, alpha

    def values(t, vt, alpha, acc_ref):
        acc_ref[...] = acc_ref[...] * alpha + jnp.dot(vt, p_refs[t][...], preferred_element_type=jnp.float32)

    def step(carry, before, now, k_after, q_after, acc_before, accs):
        m, l, top = list(carry[0:4]), list(carry[4:8]), list(carry[8:12])
        values(3, before, carry[12], acc_before)
        for t in tiles:
            m[t], l[t], alpha = expo(t, m[t], l[t], top[t])
            top[t] = scores(t, k_after, q_after(t))
            if t < 3:
                values(t, now, alpha, accs[t])
        return tuple(m + l + top) + (alpha,)

    neg, zero = jnp.full((1, rows), NEG, jnp.float32), jnp.zeros((8, rows), jnp.float32)
    one = jnp.ones((1, rows), jnp.float32)

    def total(l8):
        return jnp.sum(l8, axis=0, keepdims=True)

    def others(ref):
        return ref.at[pl.ds(0, (nx - 1) * new_a), :]

    def token_of_lane(shape):
        return lax.rem(lax.broadcasted_iota(jnp.int32, shape, 1), tq)

    def turn(first, end, dst, block):
        n = 2 if first % 4 or end % 4 else 4

        def some(i, _):
            for k in range(n):
                dst[n * i + k] = block(n * i + k).T
            return 0

        lax.fori_loop(first // n, end // n, some, 0)

    blocks = vtc.shape[0]
    per_col = blocks // nx
    part = ny // per_col
    acc[...] = jnp.zeros_like(acc)
    p3[...] = jnp.zeros_like(p3)

    def row_of(i):
        return lax.rem(y + ny - i, ny)

    def arrive_q(i):
        yy = row_of(i)
        wait_in(QS + (ny - i) % ny, qbuf.at[pl.ds(yy * CORES, CORES)])
        for t in tiles:
            u, half = yy * CORES + t // 2, t % 2
            for g in range(grp):
                q_all[4 * yy + t, pl.ds(g * tq, tq), :] = qbuf[u, pl.ds(half * tq, tq), pl.ds(g * dim, dim)]

    def cached(buf, j):
        i = j // per_col
        xx = jnp.where(i == 0, x, jnp.where(i == 1, x_left, jnp.where(i == 2, x_right, x_far)))
        return buf[pl.ds(lax.rem(j, per_col) * part, part), xx].reshape(blk, dim)

    def turn_c(first, end):
        turn(first, end, vtc, lambda j: cached(vc, j))

    near = blocks - per_col
    arrive_q(0)
    turn_c(0, near)

    def step_c(i, carry):
        yy, j = row_of(i // blocks), lax.rem(i, blocks)
        before, after = lax.max(i - 1, 0), lax.min(i + 1, ny * blocks - 1)
        y_before, y_after = row_of(before // blocks), row_of(after // blocks)
        start = j == 0
        m = tuple(jnp.where(start, NEG, v) for v in carry[0:4])
        l = tuple(jnp.where(start, 0.0, v) for v in carry[4:8])
        out = step(
            m + l + carry[8:], vtc[lax.rem(before, blocks)], vtc[j], cached(kc, lax.rem(after, blocks)),
            lambda t: q_all[4 * y_after + t], acc.at[4 * y_before + 3], [acc.at[4 * yy + t] for t in tiles])
        for t in tiles:
            m_all[4 * yy + t, 0:1, :] = out[t]
            l_all[4 * yy + t] = out[4 + t]
        return out

    tops = tuple(scores(t, cached(kc, jnp.int32(0)), q_all[4 * y + t]) for t in tiles)
    carry = (neg,) * 4 + (zero,) * 4 + tops + (one,)
    carry = lax.fori_loop(0, near - 1, step_c, carry)
    ring_last(0, kc)
    ring_last(1, vc)
    turn_c(near, blocks)
    carry = lax.fori_loop(near - 1, blocks - 1, step_c, carry)
    arrive_q(1)
    carry = lax.fori_loop(blocks - 1, 2 * blocks - 1, step_c, carry)
    arrive_q(2)
    carry = lax.fori_loop(2 * blocks - 1, 3 * blocks - 1, step_c, carry)
    arrive_q(3)
    ring_second(2, kn)
    ring_second(3, vn)
    wait_in(QA, qabuf.at[col_a, :])

    def pass_qa(k, _):
        put(QX, qabuf.at[col_a, :], qabuf.at[col_a, :], dev(y, lax.rem(x + k, nx), c))
        return 0

    lax.fori_loop(1, nx, pass_qa, 0)
    carry = lax.fori_loop(3 * blocks - 1, 4 * blocks, step_c, carry)
    values(3, vtc[blocks - 1], carry[12], acc.at[4 * row_of(ny - 1) + 3])

    ring_last(2, kn)
    ring_last(3, vn)
    turn(0, ny * nx, vtn, lambda j: vn[j // nx, lax.rem(j, nx)])

    def new_keys(j):
        return kn[j // nx, lax.rem(j, nx)]

    def row_n(i):
        return lax.rem(y + ny + jnp.where(c == 0, 1 + i, ny - 1 - i), ny)

    def rows_n(i, tops):
        yy, y_after = row_n(i), row_n(lax.min(i + 1, ny - 1))
        last = yy * nx + x
        accs = [acc.at[4 * yy + t] for t in tiles]
        p3[...] = jnp.zeros_like(p3)

        def step_n(j, carry):
            return step(carry, vtn[lax.max(j - 1, 0)], vtn[j], new_keys(j + 1), lambda t: q_all[4 * yy + t],
                        accs[3], accs)

        state = tuple(m_all[4 * yy + t, 0:1, :] for t in tiles) + tuple(l_all[4 * yy + t] for t in tiles)
        carry = lax.fori_loop(0, last, step_n, state + tuple(tops) + (one,))
        values(3, vtn[lax.max(last - 1, 0)], carry[12], accs[3])
        tops = []
        for t in tiles:
            seen = (t + 1) * tq
            tri = lax.broadcasted_iota(jnp.int32, (tq, rows), 0) <= token_of_lane((tq, rows))
            s = jnp.where(tri, s_refs[t][pl.ds(t * tq, tq), :], NEG)
            s_refs[t][pl.ds(t * tq, tq), :] = s
            top8 = fold(s, jnp.maximum)
            if t:
                top8 = jnp.maximum(top8, fold(s_refs[t][pl.ds(0, t * tq), :], jnp.maximum))
            m_new, alpha = highest(carry[t], top8)
            l8 = carry[4 + t] * alpha
            for r in range(0, seen, 16):
                e = jnp.exp2((s_refs[t][pl.ds(r, 16), :] - m_new) * scale2)
                p_refs[t][pl.ds(r, 16), :] = e.astype(bf)
                l8 = l8 + fold(e, jnp.add)
            tops.append(scores(t, new_keys(0), q_all[4 * y_after + t]))
            pv = jnp.dot(vtn[last, :, pl.ds(0, seen)], p_refs[t][pl.ds(0, seen), :], preferred_element_type=jnp.float32)
            o = (accs[t][...] * alpha + pv) * (1.0 / total(l8))
            for g in range(grp):
                obuf[yy * CORES + t // 2, pl.ds(t % 2 * tq, tq), pl.ds(g * dim, dim)] = (
                    o[:, g * tq:(g + 1) * tq].T.astype(bf))
        for cc in range(CORES):
            u = yy * CORES + cc
            give(OB, obuf.at[u], ob.at[:, pl.ds(pl.multiple_of(mine * width, width), width)], peer(u))
        return tuple(tops)

    tops = tuple(scores(t, new_keys(0), q_all[4 * row_n(0) + t]) for t in tiles)
    tops = lax.fori_loop(0, 1, rows_n, tops)

    wait_in(QX, others(qabuf))
    wait_in(KAC, kac)
    wait_in(VAC, vac)
    wait_in(KAN, kan)
    wait_in(VAN, van)
    turn(0, kv, vtac, lambda j: vac[j])
    vtan[...] = van[...].T
    for t in tiles:
        for g in range(grp):
            q_a[t, pl.ds(g * tq, tq), :] = qabuf[pl.ds(t * tq, tq), pl.ds(g * dim, dim)]
    acc_a[...] = jnp.zeros_like(acc_a)
    p3[...] = jnp.zeros_like(p3)
    accs_a = [acc_a.at[t] for t in tiles]

    def step_a(j, carry):
        return step(carry, vtac[lax.max(j - 1, 0)], vtac[j], kac[j + 1], lambda t: q_a[t], accs_a[3], accs_a)

    tops = tuple(scores(t, kac[0], q_a[t]) for t in tiles)
    carry = lax.fori_loop(0, kv - 1, step_a, (neg,) * 4 + (zero,) * 4 + tops + (one,))
    values(3, vtac[kv - 2], carry[12], accs_a[3])

    def token_a(r, xx):
        holder = dev(r // (CORES * ta), xx, lax.rem(r // ta, CORES))
        return holder * ta + lax.rem(r, ta)

    pos_k = token_a(lax.broadcasted_iota(jnp.int32, (new_a, rows), 0), x)
    place_q = token_of_lane((new_a, rows))
    row = lax.broadcasted_iota(jnp.int32, (dim, tq), 0)
    for t in tiles:
        m, l, alpha = expo(t, carry[t], carry[4 + t], carry[8 + t])
        values(t, vtac[kv - 1], alpha, accs_a[t])
        s = jnp.where(pos_k <= token_a(place_q, t), qk(kan[...], q_a[t]), NEG)
        m, l = soft_step(scale2, s, vtan[...], m, total(l), accs_a[t])
        stat = jnp.zeros((dim, tq), jnp.float32)
        for g in range(grp):
            cols = slice(g * tq, (g + 1) * tq)
            oastage[pl.ds(t * tq, tq), pl.ds(g * dim, dim)] = acc_a[t, :, cols].T
            stat = jnp.where(row == g, m[:, cols], stat)
            stat = jnp.where(row == grp + g, l[:, cols], stat)
        ststage[pl.ds(t * tq, tq), :] = stat.T

    def give_a(k, _):
        xx = lax.rem(x + k, nx)
        r = pl.ds(pl.multiple_of(xx * new_a, new_a), new_a)
        put(OA, oastage.at[r, :], oarecv.at[x], dev(y, xx, c))
        put(ST, ststage.at[r, :], strecv.at[x], dev(y, xx, c))
        return 0

    lax.fori_loop(1, nx, give_a, 0)
    copy(oastage.at[col_a, :], oarecv.at[x], recv_sem.at[OA])
    copy(ststage.at[col_a, :], strecv.at[x], recv_sem.at[ST])

    tops = tuple(scores(t, new_keys(0), q_all[4 * row_n(1) + t]) for t in tiles)
    tops = lax.fori_loop(1, ny - 1, rows_n, tops)

    wait_in(OA, oarecv)
    wait_in(ST, strecv)
    for g in range(grp):
        cols = pl.ds(g * dim, dim)
        ms = [strecv[i, :, g:g + 1] for i in range(nx)]
        top = functools.reduce(jnp.maximum, ms)
        num = jnp.zeros((new_a, dim), jnp.float32)
        den = jnp.zeros((new_a, 1), jnp.float32)
        for i in range(nx):
            w = jnp.exp2((ms[i] - top) * scale2)
            num = num + w * oarecv[i, :, cols]
            den = den + w * strecv[i, :, grp + g:grp + g + 1]
        odone[:, cols] = (num / den).astype(bf)

    def home_a(r, _):
        give(OY, odone.at[pl.ds(pl.multiple_of(r * ta, ta), ta), :],
             oa.at[:, pl.ds(pl.multiple_of(mine * width, width), width)], peer(r))
        return 0

    lax.fori_loop(0, kv, home_a, 0)
    lax.fori_loop(ny - 1, ny, rows_n, tops)

    wait_in(OB, ob)
    wait_in(OY, oa)
    for i, ref in enumerate((nkb, nka, nvb, nva)):
        wait(ref, out_sem.at[i])
    most = pl.ds(0, kv - 1)
    for item, ref in ((KC, tkb), (VC, tvb), (KAC, tka), (VAC, tva), (OB, obuf)):
        wait_out(item, ref.at[most])
    wait_out(QS, qbuf.at[pl.ds(0, CORES - 1)])
    for i in range(1, ny):
        wait_out(QS + i, qbuf.at[pl.ds(0, CORES)])
    for item, ref in ((KN, qbuf), (VN, qbuf)):
        wait_out(item, ref.at[most, :, pl.ds(0, dim)])
    for item, ref in ((KAN, kan), (VAN, van)):
        wait_out(item, ref.at[pl.ds(0, (kv - 1) * ta), :])
    wait_out(QA, qabuf.at[pl.ds(0, (kv - 1) * ta), :])
    wait_out(OY, odone.at[pl.ds(0, (kv - 1) * ta), :])
    wait_out(QX, others(qabuf))
    wait_out(OA, oarecv.at[pl.ds(0, nx - 1)])
    wait_out(ST, strecv.at[pl.ds(0, nx - 1)])
    ring_drain(0, kc)
    ring_drain(1, vc)
    ring_drain(2, kn)
    ring_drain(3, vn)


def attention(cp, xb, xa, cosf, sinf, wq, wk, wv, kcb, vcb, kca, vca):
    kv, dim = kcb.shape[1:]
    ny, nx = kv // CORES, cp // kv
    assert nx * CORES == kv and ny * nx * CORES == cp and ny == nx
    grp = wq.shape[1] // (kv * dim)
    tb, ta, cb, ca, model = xb.shape[0], xa.shape[0], kcb.shape[0], kca.shape[0], xb.shape[1]
    tq = tb // 2
    rows, width = grp * tq, grp * dim
    blk = CORES * tb
    assert blk == ca and (ny * CORES * cb) % (2 * blk) == 0 and (cp * ta) % (2 * tq) == 0
    assert width == 2 * CORES * dim and kv * ta == tq and nx == 4 and CORES == 2
    bf, f32 = jnp.bfloat16, jnp.float32
    vm = pltpu.VMEM
    scratch = [
        vm((tb + ta, model), bf),
        vm((SLOTS, model, width), bf),
        vm((kv, tb + ta, width), bf),
        vm((ny, tb + ta, width), bf),
        vm(kcb.shape, bf), vm(vcb.shape, bf), vm(kca.shape, bf), vm(vca.shape, bf),
        vm((kv, cb, dim), bf), vm((kv, cb, dim), bf), vm((kv, ca, dim), bf), vm((kv, ca, dim), bf),
        vm((kv, tb, width), bf),
        vm((ny, nx, CORES * cb, dim), bf),
        vm((ny, nx, CORES * cb, dim), bf),
        vm((ny, nx, blk, dim), bf),
        vm((ny, nx, blk, dim), bf),
        vm((cp * cb // blk, dim, blk), bf),
        vm((ny * nx, dim, blk), bf),
        vm((kv, tb, width), bf),
        vm((2 * kv, dim, rows), f32),
        vm((2 * kv, 8, rows), f32),
        vm((2 * kv, 8, rows), f32),
        vm((4, rows, dim), bf),
        vm((2 * kv, rows, dim), bf),
        vm((blk, rows), f32), vm((blk, rows), f32), vm((blk, rows), f32), vm((blk, rows), f32),
        vm((blk, rows), bf), vm((blk, rows), bf), vm((blk, rows), bf), vm((blk, rows), bf),
        vm((cp * ta, width), bf),
        vm((kv, ca, dim), bf),
        vm((kv, ca, dim), bf),
        vm((kv * ta, dim), bf),
        vm((kv * ta, dim), bf),
        vm((kv, dim, ca), bf),
        vm((dim, kv * ta), bf),
        vm((cp * ta, width), f32),
        vm((cp * ta, dim), f32),
        vm((nx, kv * ta, width), f32),
        vm((nx, kv * ta, dim), f32),
        vm((kv * ta, width), bf),
        vm((4, dim, rows), f32),
        pltpu.SemaphoreType.DMA((15 + ny + 16,)),
        pltpu.SemaphoreType.DMA((15 + ny + 16,)),
        pltpu.SemaphoreType.DMA((5,)),
        pltpu.SemaphoreType.DMA((SLOTS,)),
        pltpu.SemaphoreType.DMA((4,)),
    ]
    any_spec = pl.BlockSpec(memory_space=pl.ANY)
    vmem_spec = pl.BlockSpec(memory_space=pltpu.VMEM)
    shape = jax.ShapeDtypeStruct
    return pl.pallas_call(
        functools.partial(kernel, (ny, nx, kv, grp, dim)),
        out_shape=(shape((tb, kv * width), bf), shape((ta, kv * width), bf),
                   shape((kv, tb, dim), bf), shape((kv, tb, dim), bf),
                   shape((kv, ta, dim), bf), shape((kv, ta, dim), bf)),
        in_specs=[any_spec, any_spec, vmem_spec, vmem_spec] + [any_spec] * 7,
        out_specs=(any_spec,) * 6,
        scratch_shapes=scratch,
        compiler_params=pltpu.CompilerParams(
            collective_id=0, has_side_effects=True, vmem_limit_bytes=VMEM_LIMIT),
        name="attend",
    )(xb, xa, cosf, sinf, wq, wk, wv, kcb, vcb, kca, vca)


def out_kernel(ob, oa, w, kb, vb, ka, va, yb, ya, nkb, nvb, nka, nva, o, wbuf, ybuf, *rest):
    new, turned, (wsem, osem, nsem, ysem) = rest[:4], rest[4:8], rest[8:]
    tb, ta = ob.shape[0], oa.shape[0]
    cols = wbuf.shape[2]
    steps = w.shape[1] // cols
    b_rows, a_rows = pl.ds(0, tb), pl.ds(tb, ta)

    def copy(src, dst, sem):
        pltpu.make_async_copy(src, dst, sem).start()

    def wait(ref, sem):
        pltpu.make_async_copy(ref, ref, sem).wait()

    def span(i):
        return pl.ds(pl.multiple_of(i * cols, cols), cols)

    def load(i):
        copy(w.at[:, span(i)], wbuf.at[lax.rem(i, SLOTS)], wsem.at[lax.rem(i, SLOTS)])

    copy(ob, o.at[b_rows, :], osem)
    copy(oa, o.at[a_rows, :], osem)
    for i in range(min(SLOTS - 1, steps)):
        load(i)
    for i, (src, dst) in enumerate(zip((kb, vb, ka, va), new)):
        copy(src, dst, nsem.at[i])
    wait(o, osem)

    def step(i, _):
        @pl.when(i + SLOTS - 1 < steps)
        def _():
            load(i + SLOTS - 1)

        slot = lax.rem(i, SLOTS)
        wait(wbuf.at[slot], wsem.at[slot])
        ybuf[i] = jnp.dot(o[...], wbuf[slot], preferred_element_type=jnp.float32).astype(ybuf.dtype)
        copy(ybuf.at[i, b_rows, :], yb.at[:, span(i)], ysem.at[0])
        copy(ybuf.at[i, a_rows, :], ya.at[:, span(i)], ysem.at[1])
        return 0

    lax.fori_loop(0, steps, step, 0)
    for i, (src, dst, out) in enumerate(zip(new, turned, (nkb, nvb, nka, nva))):
        wait(src, nsem.at[i])
        dst[...] = jnp.transpose(src[...], (1, 0, 2))
        copy(dst, out, nsem.at[i])
    wait(yb, ysem.at[0])
    wait(ya, ysem.at[1])
    for i, out in enumerate((nkb, nvb, nka, nva)):
        wait(out, nsem.at[i])


def output_projection(ob, oa, w, *new):
    (tb, inner), ta, model = ob.shape, oa.shape[0], w.shape[1]
    cols = min(512, model)
    shape = jax.ShapeDtypeStruct
    bf, vm, dma = ob.dtype, pltpu.VMEM, pltpu.SemaphoreType.DMA
    turned = [(t.shape[1], t.shape[0], t.shape[2]) for t in new]
    any_spec = pl.BlockSpec(memory_space=pl.ANY)
    return pl.pallas_call(
        out_kernel,
        out_shape=[shape((tb, model), bf), shape((ta, model), bf)] + [shape(t, bf) for t in turned],
        in_specs=[any_spec] * 7,
        out_specs=[any_spec] * 6,
        scratch_shapes=[vm((tb + ta, inner), bf), vm((SLOTS, inner, cols), bf), vm((model // cols, tb + ta, cols), bf)]
        + [vm(t.shape, bf) for t in new] + [vm(t, bf) for t in turned] + [dma((SLOTS,)), dma, dma((4,)), dma((2,))],
        compiler_params=pltpu.CompilerParams(vmem_limit_bytes=VMEM_LIMIT),
        name="project_out",
    )(ob, oa, w, *new)


def solution(mesh):
    cp_size = mesh.shape["cp"]

    def local_step(x_a, kc_a, vc_a, x_b, kc_b, vc_b, w_q, w_k, w_v, w_o):
        ta, tb = x_a.shape[0], x_b.shape[0]
        kv, dim = kc_a.shape[1:]
        me = lax.axis_index("cp")
        pos_a = kc_a.shape[0] * cp_size + me * ta + jnp.arange(ta)
        pos_b = kc_b.shape[0] * cp_size + me * tb + jnp.arange(tb)
        cosf, sinf = rope_tables(jnp.concatenate([pos_b, pos_a]), dim)
        o_b, o_a, k_b, v_b, k_a, v_a = attention(cp_size, x_b, x_a, cosf, sinf, w_q, w_k, w_v, kc_b, vc_b, kc_a, vc_a)
        y_b, y_a, k_b, v_b, k_a, v_a = output_projection(o_b, o_a, w_o, k_b, v_b, k_a, v_a)
        return y_a, k_a, v_a, y_b, k_b, v_b

    row_spec = P(("dp", "cp"), None)
    kv_spec = P(("dp", "cp"), None, None)
    full_spec = P()
    return jax.shard_map(
        local_step, mesh=mesh,
        in_specs=(row_spec, kv_spec, kv_spec, row_spec, kv_spec, kv_spec, full_spec, full_spec, full_spec, full_spec),
        out_specs=(row_spec, kv_spec, kv_spec, row_spec, kv_spec, kv_spec), check_vma=False)
```
